1024 devices in a mesh: gx: 8 (over x, core), gy: 16 (over z), gz: 8 (over y).
Axes of the slice: x: 4, y: 8, z: 16, core: 2. Of those that a mesh axis runs over, the one named last changes fastest.
Arguments:
- density: float32 [64, 256, 1024], P('gx', 'gy', 'gz'), may hold values from 0.1 to 10
- x_faces: float32 [2, 256, 1024], P(None, 'gy', 'gz'), may hold values from -6 to 6
- y_faces: float32 [2, 64, 1024], P(None, 'gx', 'gz'), may hold values from -6 to 6
- z_faces: float32 [2, 64, 256], P(None, 'gx', 'gy'), may hold values from -6 to 6
Outputs:
- solution_field: float32 [64, 256, 1024], P('gx', 'gy', 'gz')
- residual: float32 [64, 256, 1024], P('gx', 'gy', 'gz')
The draws below stay inside these ranges and needn't reach their ends.
All inputs are finite; a program needn't handle non-finite values.
Results may differ from the reference program's by a relative error of at most 0.0003.
Values sent between devices are 32-bit elements; how exact they have to be, the bound alone decides.
No kernel may reach another device: no remote copies, remote signals or barrier semaphores. Data moves between devices by JAX's collectives and lax.ppermute only.
A program may use at most 32 MiB of HBM per device.

```python
import jax
import jax.numpy as jnp

ITERS = 2
LEVELS = 3
COARSE_SWEEPS = 3
NX = 64
NY = 256
NZ = 1024


def draw_density(key, part):
    rough_key = jax.random.fold_in(key, 11)
    x_frac = jnp.arange(NX, dtype=jnp.float32) / NX
    rough = jnp.exp(jax.random.uniform(rough_key, (NX, NY, NZ), jnp.float32, jnp.log(0.5), jnp.log(2.0)))
    profile = jnp.exp(jnp.log(3.0) * x_frac)[:, None, None]
    return (rough * profile).astype(jnp.float32)


def shard_levels(stream_key, dims, pieces, least, largest):
    def one(axis_at, blocks):
        heights = jax.random.uniform(jax.random.fold_in(jax.random.fold_in(stream_key, 6), axis_at), (blocks,), jnp.float32, least / len(pieces), largest / len(pieces))
        return jnp.repeat(jnp.exp(heights), dims[axis_at] // blocks).reshape((-1,) + (1,) * (len(dims) - axis_at - 1))

    level = one(*pieces[0])
    for cut in pieces[1:]:
        level = level * one(*cut)
    return level


def bell_draw(stream_key, dims, width, most, cuts=(), kind=jnp.bfloat16):
    gain = shard_levels(stream_key, dims, cuts, -0.22, 0.18) if cuts else 1.0
    array = jax.random.normal(stream_key, dims, jnp.float32) * width * gain
    return jnp.minimum(jnp.maximum(array, -most), most).astype(kind)


def setup_inputs(seed: int = 0) -> dict:
    key_list = jax.random.split(jax.random.key(seed), 5)
    density = draw_density(jax.random.fold_in(key_list[4], 71), 0)
    x_faces = bell_draw(key_list[1], (2, NY, NZ), 1.0, 6.0, ((1, 16), (2, 8)), jnp.float32)
    y_faces = bell_draw(key_list[2], (2, NX, NZ), 1.0, 6.0, ((1, 8), (2, 8)), jnp.float32)
    z_faces = bell_draw(key_list[3], (2, NX, NY), 1.0, 6.0, ((1, 8), (2, 16)), jnp.float32)
    return dict(density=density, x_faces=x_faces, y_faces=y_faces, z_faces=z_faces)


relax_rate = 1.0 / 9.0
coupling = 0.5


def beside_sum(padded):
    beside = padded[2:, 1:-1, 1:-1] + padded[:-2, 1:-1, 1:-1]
    beside = beside + padded[1:-1, 2:, 1:-1] + padded[1:-1, :-2, 1:-1]
    beside = beside + padded[1:-1, 1:-1, 2:] + padded[1:-1, 1:-1, :-2]
    return beside


def operate(field):
    return 6.0 * field - beside_sum(jnp.pad(field, 1))


def restrict(field):
    sx, sy, sz = field.shape
    return 0.5 * jnp.sum(field.reshape(sx // 2, 2, sy // 2, 2, sz // 2, 2), axis=(1, 3, 5))


def prolong(field):
    sx, sy, sz = field.shape
    spread = jnp.broadcast_to(field[:, None, :, None, :, None], (sx, 2, sy, 2, sz, 2))
    return spread.reshape(2 * sx, 2 * sy, 2 * sz)


def cycle(right_side, level_idx):
    approx = relax_rate * right_side
    if level_idx == LEVELS - 1:
        for sweep_idx in range(COARSE_SWEEPS - 1):
            approx = approx + relax_rate * (right_side - operate(approx))
        return approx
    defect = right_side - operate(approx)
    approx = approx + prolong(cycle(restrict(defect), level_idx + 1))
    return approx + relax_rate * (right_side - operate(approx))


def reference(density, x_faces, y_faces, z_faces):
    right_side = -coupling * density
    right_side = right_side.at[0].add(x_faces[0])
    right_side = right_side.at[-1].add(x_faces[1])
    right_side = right_side.at[:, 0].add(y_faces[0])
    right_side = right_side.at[:, -1].add(y_faces[1])
    right_side = right_side.at[:, :, 0].add(z_faces[0])
    right_side = right_side.at[:, :, -1].add(z_faces[1])
    solution_field = jnp.zeros_like(right_side)
    residual = right_side
    precond = cycle(residual, 0)
    direction = precond
    gamma_now = jnp.sum(residual * precond)
    for iteration in range(ITERS):
        image = operate(direction)
        step_size = gamma_now / jnp.sum(direction * image)
        solution_field = solution_field + step_size * direction
        residual = residual - step_size * image
        if iteration + 1 < ITERS:
            precond = cycle(residual, 0)
            gamma_next = jnp.sum(residual * precond)
            direction = precond + (gamma_next / gamma_now) * direction
            gamma_now = gamma_next
    return solution_field, residual
```

```python
import functools

import jax
import jax.numpy as jnp
from jax import lax
from jax.experimental import pallas as pl
from jax.experimental.pallas import tpu as pltpu
from jax.sharding import Mesh
from jax.sharding import PartitionSpec as P

AXES = ("gx_0", "gx_1", "gy", "gz")
GX = ("gx_0", "gx_1")
NX, NY, NZ = 64, 256, 1024
BX, BY, BZ = 8, 16, 128
CZ = 32
HY, HZ = 32, 32
ROWS, LANES = BY + 2 * HY, 128
relax = 1.0 / 9.0
coupling = 0.5
VMEM = pl.BlockSpec(memory_space=pltpu.VMEM)
SMEM = pl.BlockSpec(memory_space=pltpu.SMEM)


def roll(x, shift, axis):
    return pltpu.roll(x, shift % x.shape[axis], axis)


def lane_index(shape):
    return lax.broadcasted_iota(jnp.int32, shape, 1)


def row_index(shape):
    return lax.broadcasted_iota(jnp.int32, shape, 0)


def rhs_kernel(where_ref, density, xf, yf, zf, rhs, packed):
    gx, gy, gz = where_ref[0], where_ref[1], where_ref[2]
    rows, lanes = row_index((BY, BZ)), lane_index((BY, BZ))
    eye = row_index((BY, BY)) == lane_index((BY, BY))
    low_y = (rows == 0) & (gy == 0)
    high_y = (rows == BY - 1) & (gy == NY // BY - 1)
    low_z = (lanes == 0) & (gz == 0)
    high_z = (lanes == BZ - 1) & (gz == NZ // BZ - 1)

    def column(row):
        return jnp.sum(jnp.where(eye, row, 0.0), axis=1, keepdims=True)

    layers = []
    for x in range(BX):
        value = -coupling * density[x]
        if x == 0:
            value = value + jnp.where(gx == 0, xf[0], 0.0)
        if x == BX - 1:
            value = value + jnp.where(gx == NX // BX - 1, xf[1], 0.0)
        value = value + jnp.where(low_y, yf[0, x : x + 1, :], 0.0)
        value = value + jnp.where(high_y, yf[1, x : x + 1, :], 0.0)
        value = value + jnp.where(low_z, column(zf[0, x : x + 1, :]), 0.0)
        value = value + jnp.where(high_z, column(zf[1, x : x + 1, :]), 0.0)
        rhs[x] = value
        layers.append(value)
    for chunk in range(4):
        for quad in range(2):
            out = None
            for k in range(4):
                part = roll(layers[4 * quad + k], 32 * (k - chunk), 1)
                out = part if k == 0 else jnp.where(lanes >= 32 * k, part, out)
            packed[2 * chunk, quad] = out
            packed[2 * chunk + 1, quad] = out


def make_rhs(where, density, xf, yf, zf):
    return pl.pallas_call(
        rhs_kernel,
        out_shape=(
            jax.ShapeDtypeStruct((BX, BY, BZ), jnp.float32),
            jax.ShapeDtypeStruct((8, 2, BY, BZ), jnp.float32),
        ),
        in_specs=[SMEM, VMEM, VMEM, VMEM, VMEM],
        out_specs=(VMEM, VMEM),
    )(where, density, xf, yf, zf)


def join_kernel(where_ref, own, near, far, near2, far2, out):
    core = where_ref[3]
    out[:, 2 * BY : 3 * BY] = own[...]

    @pl.when(core == 0)
    def _():
        out[:, 0:BY] = far[...]
        out[:, BY : 2 * BY] = near[...]
        out[:, 3 * BY : 4 * BY] = near2[...]
        out[:, 4 * BY : 5 * BY] = far2[...]

    @pl.when(core == 1)
    def _():
        out[:, 0:BY] = far2[...]
        out[:, BY : 2 * BY] = near2[...]
        out[:, 3 * BY : 4 * BY] = near[...]
        out[:, 4 * BY : 5 * BY] = far[...]


def join(where, own, near, far, near2, far2):
    return pl.pallas_call(
        join_kernel,
        out_shape=jax.ShapeDtypeStruct((16, ROWS, 128), jnp.float32),
        in_specs=[SMEM] + [VMEM] * 5,
        out_specs=VMEM,
    )(where, own, near, far, near2, far2)


def around(x, step):
    return (roll(x, step, 0) + roll(x, -step, 0)) + (roll(x, step, 1) + roll(x, -step, 1))


def fold(x, step):
    rows, lanes = row_index(x.shape), lane_index(x.shape)
    x = x + jnp.where(rows & step == 0, roll(x, -step, 0), roll(x, step, 0))
    return x + jnp.where(lanes & step == 0, roll(x, -step, 1), roll(x, step, 1))


def third(x):
    return x * (1.0 / 3.0)


def cycle_in(src, mask, f1, f2, t2, e2, e1, lo, hi, lo2, hi2, n0, n1, n2):
    rows = slice(lo, hi)
    inner = slice(lo2, hi2)

    def down0(i, _):
        a, b = src[2 * i + 1, rows], src[2 * i + 2, rows]
        t = a + b
        s = third(t) + relax * ((t + src[2 * i, rows] + src[2 * i + 3, rows]) + around(t, 1))
        f1[i + 1, rows] = 0.5 * fold(s, 1) * mask[rows]
        return 0

    lax.fori_loop(0, NX // 2, down0, 0)

    def down1(i, _):
        t = f1[2 * i + 1, rows] + f1[2 * i + 2, rows]
        s = third(t) + relax * ((t + f1[2 * i, rows] + f1[2 * i + 3, rows]) + around(t, 2))
        f2[i + 1, rows] = 0.5 * fold(s, 2) * mask[rows]
        return 0

    lax.fori_loop(0, NX // 4, down1, 0)

    def sweep0(i, _):
        r = f2[i + 1, rows]
        s = (4.0 / 3.0) * r + relax * ((f2[i, rows] + f2[i + 2, rows]) + around(r, 4))
        t2[i + 1, rows] = relax * s * mask[rows]
        return 0

    lax.fori_loop(0, NX // 4, sweep0, 0)

    def sweep1(i, _):
        v = t2[i + 1, rows]
        s = third(v) + relax * (f2[i + 1, rows] + ((t2[i, rows] + t2[i + 2, rows]) + around(v, 4)))
        e2[i + 1, rows] = s * mask[rows]
        return 0

    lax.fori_loop(0, NX // 4, sweep1, 0)

    def up1(i, _):
        e = e2[i + 1, rows]
        before = relax * f1[2 * i, rows] + e2[i, rows]
        ra, rb = f1[2 * i + 1, rows], f1[2 * i + 2, rows]
        va, vb = relax * ra + e, relax * rb + e
        after = relax * f1[2 * i + 3, rows] + e2[i + 2, rows]
        m = mask[rows]
        e1[2 * i + 1, rows] = (third(va) + relax * (ra + ((before + vb) + around(va, 2)))) * m
        e1[2 * i + 2, rows] = (third(vb) + relax * (rb + ((va + after) + around(vb, 2)))) * m
        return 0

    lax.fori_loop(0, NX // 4, up1, 0)


def cycle_out(src, mask, e1, out, lo, hi):
    rows = slice(lo, hi)

    def up0(i, _):
        e = e1[i + 1, rows]
        before = relax * src[2 * i, rows] + e1[i, rows]
        ra, rb = src[2 * i + 1, rows], src[2 * i + 2, rows]
        va, vb = relax * ra + e, relax * rb + e
        after = relax * src[2 * i + 3, rows] + e1[i + 2, rows]
        m = mask[rows]
        out[2 * i + 1, rows] = (third(va) + relax * (ra + ((before + vb) + around(va, 1)))) * m
        out[2 * i + 2, rows] = (third(vb) + relax * (rb + ((va + after) + around(vb, 1)))) * m
        return 0

    lax.fori_loop(0, NX // 2, up0, 0)


def operate_on(src, i, rows):
    v = src[i + 1, rows]
    return 6.0 * v - ((src[i, rows] + src[i + 2, rows]) + around(v, 1))


def cycles_kernel(where_ref, own, got, swapped, out, r0, z0, q0, w, f1, f2, t2, e2, e1, mask):
    gx0, core, gy, gz = where_ref[4], where_ref[3], where_ref[1], where_ref[2]
    shape = (ROWS, LANES)
    rows, lanes = row_index(shape), lane_index(shape)
    y = gy * BY - HY + rows
    z = (gz * 4 + gx0) * CZ - HZ + lanes
    valid = (y >= 0) & (y < NY) & (z >= 0) & (z < NZ) & (lanes < CZ + 2 * HZ)
    mask[...] = jnp.where(valid, 1.0, 0.0)
    zero = jnp.zeros(shape, jnp.float32)
    for ref, count in ((r0, NX), (z0, NX), (q0, NX), (w, NX), (f1, NX // 2), (e1, NX // 2), (f2, NX // 4), (t2, NX // 4), (e2, NX // 4)):
        ref[0] = zero
        ref[count + 1] = zero

    def unpack(i, _):
        a, c, b = got[i], own[i], swapped[i]
        first = core == 0
        left, right = jnp.where(first, a, b), jnp.where(first, b, a)
        for k in range(4):
            value = jnp.where(lanes < 32, roll(left, -32 * k, 1), jnp.where(lanes < 64, roll(c, 32 - 32 * k, 1), roll(right, 64 - 32 * k, 1)))
            r0[4 * i + k + 1] = jnp.where(lanes < 96, value, 0.0)
        return 0

    lax.fori_loop(0, NX // 4, unpack, 0)
    cycle_in(r0, mask, f1, f2, t2, e2, e1, 0, 80, 8, 72, 0, 0, 0)
    cycle_out(r0, mask, e1, z0, 8, 72)

    mid = slice(16, 64)

    def image(i, _):
        q0[i + 1, mid] = operate_on(z0, i, mid) * mask[mid]
        return 0

    lax.fori_loop(0, NX, image, 0)
    cycle_in(q0, mask, f1, f2, t2, e2, e1, 16, 64, 24, 56, 0, 0, 0)
    cycle_out(q0, mask, e1, w, 24, 56)

    home = slice(HY, HY + BY)
    wide = slice(24, 56)
    hlanes = lane_index((BY, LANES))
    inside = (hlanes >= HZ) & (hlanes < HZ + CZ)

    def sums(i, acc):
        s = operate_on(w, i, wide)[8:24]
        r, zz, q, ww = r0[i + 1, home], z0[i + 1, home], q0[i + 1, home], w[i + 1, home]
        a0, a1, a2, a3, a4 = acc
        value = jnp.where(hlanes < 32, roll(zz, -32, 1), jnp.where(hlanes < 64, q, jnp.where(hlanes < 96, roll(ww, 32, 1), roll(s, 64, 1))))
        slab = i // BX

        @pl.when(slab % 2 == core)
        def _():
            out[slab // 2, pl.ds(pl.multiple_of((i % BX) * BY, BY), BY)] = value

        return a0 + r * zz, a1 + zz * q, a2 + r * ww, a3 + q * ww, a4 + ww * s

    init = jnp.zeros((BY, LANES), jnp.float32)
    acc = lax.fori_loop(0, NX, sums, (init,) * 5)
    out_rows, out_lanes = row_index((8, LANES)), lane_index((8, LANES))
    row = jnp.zeros((8, LANES), jnp.float32)
    for k, a in enumerate(acc):
        total = jnp.sum(jnp.where(inside, a, 0.0))
        row = jnp.where(out_lanes == k, total, row)
    for t in range(4):
        out[t, BX * BY : BX * BY + 8] = row


def cycles(where, own, got, swapped):
    def field(n):
        return pltpu.VMEM((n + 2, ROWS, LANES), jnp.float32)

    return pl.pallas_call(
        cycles_kernel,
        out_shape=jax.ShapeDtypeStruct((4, BX * BY + 8, LANES), jnp.float32),
        in_specs=[SMEM] + [VMEM] * 3,
        out_specs=VMEM,
        scratch_shapes=[field(NX)] * 4 + [field(NX // 2), field(NX // 4), field(NX // 4), field(NX // 4), field(NX // 2), pltpu.VMEM((ROWS, LANES), jnp.float32)],
        compiler_params=pltpu.CompilerParams(vmem_limit_bytes=48 * 1024 * 1024),
    )(where, own, got, swapped)


def finish_kernel(rhs, fields, sums, solution, residual):
    total = jnp.sum(sums[...], axis=0, keepdims=True)
    lanes = lane_index(total.shape)

    def pick(k):
        return jnp.sum(jnp.where(lanes == k, total, 0.0), axis=1, keepdims=True)

    rz, zq, rw, qw, ws = (pick(k) for k in range(5))
    step0 = rz / zq
    rz1 = rz - step0 * (rw + zq) + step0 * step0 * qw
    growth = rz1 / rz
    image1 = (zq - 2.0 * step0 * qw + step0 * step0 * ws) + 2.0 * growth * (zq - step0 * qw) + growth * growth * zq
    step1 = rz1 / image1
    on_z = step0 + step1 * (1.0 + growth)
    on_w = -step1 * step0
    wide = lane_index((BY, LANES))
    for x in range(BX):
        parts = [fields[c, x * BY : (x + 1) * BY] for c in range(4)]

        def field(f):
            value = None
            for c in range(4):
                part = roll(parts[c], 32 * (c - f), 1)
                value = part if c == 0 else jnp.where(wide >= 32 * c, part, value)
            return value

        z0, q0, w, s = (field(f) for f in range(4))
        solution[x] = on_z * z0 + on_w * w
        residual[x] = rhs[x] - (on_z * q0 + on_w * s)


def finish(rhs, fields, sums):
    shape = jax.ShapeDtypeStruct((BX, BY, BZ), jnp.float32)
    return pl.pallas_call(finish_kernel, out_shape=(shape, shape), in_specs=[VMEM] * 3, out_specs=(VMEM, VMEM))(rhs, fields, sums)


def both_ways(count, step):
    pairs = [(i, i + step) for i in range(count - step)]
    return pairs + [(count + b, count + a) for a, b in pairs]


def z_pairs():
    def number(core, block):
        return ((block % 4) * 2 + core) * 8 + block // 4

    up = [(i, i + 1) for i in range(31)]
    return [(number(0, a), number(0, b)) for a, b in up] + [(number(1, b), number(1, a)) for a, b in up]


SWAP = [(0, 1), (1, 0)]


def local(density, x_faces, y_faces, z_faces):
    where = jnp.stack([lax.axis_index(GX), lax.axis_index("gy"), lax.axis_index("gz"), lax.axis_index("gx_1"), lax.axis_index("gx_0")]).astype(jnp.int32)
    rhs, packed = make_rhs(where, density, x_faces, y_faces, z_faces)
    own = lax.all_to_all(packed, GX, 0, 0, tiled=True).reshape(16, BY, 128)
    near = lax.ppermute(own, ("gx_1", "gy"), both_ways(16, 1))
    far = lax.ppermute(own, ("gx_1", "gy"), both_ways(16, 2))
    near2 = lax.ppermute(near, "gx_1", SWAP)
    far2 = lax.ppermute(far, "gx_1", SWAP)
    joined = join(where, own, near, far, near2, far2)
    got = lax.ppermute(joined, ("gx_0", "gx_1", "gz"), z_pairs())
    swapped = lax.ppermute(got, "gx_1", SWAP)
    packed = cycles(where, joined, got, swapped)
    fields = lax.all_to_all(packed, "gx_0", 0, 0, tiled=True)
    sums = jnp.sum(fields[:, BX * BY, :], axis=0)
    sums = lax.all_to_all(jnp.broadcast_to(sums, (128, 1, 128)), ("gy", "gz"), 0, 0, tiled=True)
    return finish(rhs, fields, sums.reshape(128, 128))


def solution(mesh):
    torus = Mesh(mesh.devices.reshape(4, 2, mesh.shape["gy"], mesh.shape["gz"]), AXES)
    in_specs = (P(GX, "gy", "gz"), P(None, "gy", "gz"), P(None, GX, "gz"), P(None, GX, "gy"))
    out_specs = (P(GX, "gy", "gz"), P(GX, "gy", "gz"))
    return jax.shard_map(local, mesh=torus, in_specs=in_specs, out_specs=out_specs, check_vma=False)
```

```python
import functools

import jax
import jax.numpy as jnp
from jax import lax
from jax.experimental import pallas as pl
from jax.experimental.pallas import tpu as pltpu
from jax.sharding import Mesh
from jax.sharding import PartitionSpec as P

AXES = ("gx_0", "gx_1", "gy", "gz")
GX = ("gx_0", "gx_1")
NX, NY, NZ = 64, 256, 1024
BX, BY, BZ = 8, 16, 128
CZ = 32
HY, HZ = 32, 32
ROWS, LANES = BY + 2 * HY, 128
relax = 1.0 / 9.0
coupling = 0.5
VMEM = pl.BlockSpec(memory_space=pltpu.VMEM)
SMEM = pl.BlockSpec(memory_space=pltpu.SMEM)


def roll(x, shift, axis):
    return pltpu.roll(x, shift % x.shape[axis], axis)


def lane_index(shape):
    return lax.broadcasted_iota(jnp.int32, shape, 1)


def row_index(shape):
    return lax.broadcasted_iota(jnp.int32, shape, 0)


PLANES = (0, 2, 1, 3)


def rhs_kernel(where_ref, density, xf, yf, zf, rhs, packed, scratch):
    gx, gy, gz = where_ref[0], where_ref[1], where_ref[2]
    rows, lanes = row_index((BY, BZ)), lane_index((BY, BZ))
    eye = row_index((BY, BY)) == lane_index((BY, BY))
    low_y = (rows == 0) & (gy == 0)
    high_y = (rows == BY - 1) & (gy == NY // BY - 1)
    low_z = (lanes == 0) & (gz == 0)
    high_z = (lanes == BZ - 1) & (gz == NZ // BZ - 1)

    def column(row):
        return jnp.sum(jnp.where(eye, row, 0.0), axis=1, keepdims=True)

    layers = []
    for x in range(BX):
        value = -coupling * density[x]
        if x == 0:
            value = value + jnp.where(gx == 0, xf[0], 0.0)
        if x == BX - 1:
            value = value + jnp.where(gx == NX // BX - 1, xf[1], 0.0)
        value = value + jnp.where(low_y, yf[0, x : x + 1, :], 0.0)
        value = value + jnp.where(high_y, yf[1, x : x + 1, :], 0.0)
        value = value + jnp.where(low_z, column(zf[0, x : x + 1, :]), 0.0)
        value = value + jnp.where(high_z, column(zf[1, x : x + 1, :]), 0.0)
        rhs[x] = value
        layers.append(value)
    for chunk in range(4):
        for quad in range(2):
            out = None
            for k in range(4):
                part = roll(layers[4 * quad + k], 32 * (k - chunk), 1)
                out = part if k == 0 else jnp.where(lanes >= 32 * k, part, out)
            scratch[chunk, quad] = out
    for chunk in range(4):
        for quad in range(2):
            for at, plane in enumerate(PLANES):
                part = scratch[chunk, quad, pl.ds(plane, 4, stride=4), :]
                packed[2 * chunk, quad, 4 * at : 4 * at + 4] = part
                packed[2 * chunk + 1, quad, 4 * at : 4 * at + 4] = part


def make_rhs(where, density, xf, yf, zf):
    return pl.pallas_call(
        rhs_kernel,
        out_shape=(
            jax.ShapeDtypeStruct((BX, BY, BZ), jnp.float32),
            jax.ShapeDtypeStruct((8, 2, BY, BZ), jnp.float32),
        ),
        in_specs=[SMEM, VMEM, VMEM, VMEM, VMEM],
        out_specs=(VMEM, VMEM),
        scratch_shapes=[pltpu.VMEM((4, 2, BY, BZ), jnp.float32)],
    )(where, density, xf, yf, zf)


def join_kernel(where_ref, own, near, far, near2, far2, out):
    core = where_ref[3]

    def place(blocks):
        def layer(i, _):
            for at in range(4):
                for b, block in enumerate(blocks):
                    out[i, 20 * at + 4 * b : 20 * at + 4 * b + 4] = block[i, 4 * at : 4 * at + 4]
            return 0

        lax.fori_loop(0, NX // 4, layer, 0, unroll=4)

    @pl.when(core == 0)
    def _():
        place((far, near, own, near2, far2))

    @pl.when(core == 1)
    def _():
        place((far2, near2, own, near, far))


def join(where, own, near, far, near2, far2):
    return pl.pallas_call(
        join_kernel,
        out_shape=jax.ShapeDtypeStruct((16, ROWS, 128), jnp.float32),
        in_specs=[SMEM] + [VMEM] * 5,
        out_specs=VMEM,
    )(where, own, near, far, near2, far2)


WHOLE = (0, 8, 12)
MIDDLE = (4, 12)
HOME = (6,)


def sides(x, step):
    return roll(x, step, 1) + roll(x, -step, 1)


def third(x):
    return x * (1.0 / 3.0)


def even(ref, x, half, j):
    return ref[x, 0, pl.ds(20 * half + j, 8)]


def odd(ref, x, half, j):
    return ref[x, 1, pl.ds(20 + 20 * half + j, 8)]


def below(ref, x, half, j):
    return ref[x, 1, pl.ds(20 * half + j, 8)]


def above(ref, x, half, j):
    return ref[x, 0, pl.ds(20 + 20 * half + j, 8)]


def put0(ref, x, parity, half, j, value):
    if parity == 0:
        if half == 0:
            ref[x, 0, pl.ds(39 + j, 8)] = value
        ref[x, 0, pl.ds(20 * half + j, 8)] = value
    else:
        if half == 1:
            if j == 12:
                ref[x, 1, pl.ds(13, 7)] = value[0:7]
            else:
                ref[x, 1, pl.ds(1 + j, 8)] = value
        ref[x, 1, pl.ds(20 + 20 * half + j, 8)] = value


def put1(ref, x, half, j, value):
    if half == 0:
        ref[x, pl.ds(59 + j, 8)] = value
    elif j == 12:
        ref[x, pl.ds(13, 7)] = value[0:7]
    else:
        ref[x, pl.ds(1 + j, 8)] = value
    ref[x, pl.ds(20 + 20 * half + j, 8)] = value


def chunks(count, size, body):
    lax.fori_loop(0, count // size, lambda i, _: body(i * size) or 0, 0)


def cycle_down(src, mask, fold, f1, f2, tiles):
    def level1(first):
        for j in tiles:
            m = mask[pl.ds(j, 8)]
            for half in range(2):
                cells = [even(src, 2 * first + k, half, j) + odd(src, 2 * first + k, half, j) for k in range(10)]
                for i in range(4):
                    before, a, b, after = cells[2 * i : 2 * i + 4]
                    u = a + b
                    y = [below(src, 2 * first + 2 * i + k, half, j) + above(src, 2 * first + 2 * i + k, half, j) for k in (1, 2)]
                    s = third(u) + relax * (((u + u) + (before + after)) + ((y[0] + y[1]) + sides(u, 1)))
                    put1(f1, first + i + 1, half, j, fold(s, 1) * m)

    chunks(NX // 2, 4, level1)

    def level2(first):
        for j in tiles:
            m = mask[pl.ds(j, 8)]
            cells = [f1[2 * first + k, pl.ds(20 + j, 8)] + f1[2 * first + k, pl.ds(40 + j, 8)] for k in range(10)]
            for i in range(4):
                before, a, b, after = cells[2 * i : 2 * i + 4]
                u = a + b
                y = [f1[2 * first + 2 * i + k, pl.ds(j, 8)] + f1[2 * first + 2 * i + k, pl.ds(60 + j, 8)] for k in (1, 2)]
                s = third(u) + relax * (((u + u) + (before + after)) + ((y[0] + y[1]) + sides(u, 2)))
                f2[first + i + 1, pl.ds(8 + j, 8)] = fold(s, 2) * m

    chunks(NX // 4, 4, level2)


def cycle_coarse(mask, f2, t2, e2, tiles, last):
    def around(ref, x, j):
        return (ref[x - 1, pl.ds(8 + j, 8)] + ref[x + 1, pl.ds(8 + j, 8)]) + (ref[x, pl.ds(7 + j, 8)] + ref[x, pl.ds(9 + j, 8)])

    def sweep1(first):
        for j in tiles:
            m = mask[pl.ds(j, 8)]
            for i in range(1, 9):
                r = f2[first + i, pl.ds(8 + j, 8)]
                s = (4.0 / 3.0) * r + relax * (around(f2, first + i, j) + sides(r, 4))
                t2[first + i, pl.ds(8 + j, 8)] = (relax * s) * m

    chunks(NX // 4, 8, sweep1)

    def sweep2(first):
        for j in last:
            m = mask[pl.ds(j, 8)]
            for i in range(1, 9):
                v = t2[first + i, pl.ds(8 + j, 8)]
                s = third(v) + relax * (f2[first + i, pl.ds(8 + j, 8)] + (around(t2, first + i, j) + sides(v, 4)))
                e2[first + i, pl.ds(8 + j, 8)] = s * m

    chunks(NX // 4, 8, sweep2)


def cycle_up(src, mask, f1, e2, v1, e1, v0, out, tiles, last):
    def correct1(first):
        for j in tiles:
            for i in range(4):
                e = e2[first + i + 1, pl.ds(8 + j, 8)]
                for half in range(2):
                    for k in (1, 2):
                        x = 2 * first + 2 * i + k
                        put1(v1, x, half, j, relax * f1[x, pl.ds(20 + 20 * half + j, 8)] + e)

    chunks(NX // 4, 4, correct1)

    def smooth1(first):
        for j in tiles:
            m = mask[pl.ds(j, 8)]
            for half in range(2):
                at = pl.ds(20 + 20 * half + j, 8)
                for i in range(1, 9):
                    x = first + i
                    v = v1[x, at]
                    y = v1[x, pl.ds(20 * half + j, 8)] + v1[x, pl.ds(40 + 20 * half + j, 8)]
                    s = third(v) + relax * ((f1[x, at] + (v1[x - 1, at] + v1[x + 1, at])) + (y + sides(v, 2)))
                    e1[x, pl.ds(20 * half + j, 8)] = s * m

    chunks(NX // 2, 8, smooth1)

    def correct0(first):
        for j in tiles:
            for i in range(1, 5):
                for half in range(2):
                    e = e1[first + i, pl.ds(20 * half + j, 8)]
                    for k in (-1, 0):
                        x = 2 * first + 2 * i + k
                        put0(v0, x, 0, half, j, relax * even(src, x, half, j) + e)
                        put0(v0, x, 1, half, j, relax * odd(src, x, half, j) + e)

    chunks(NX // 2, 4, correct0)

    def smooth0(first):
        for j in last:
            m = mask[pl.ds(j, 8)]
            for half in range(2):
                evens = [even(v0, first + k, half, j) for k in range(10)]
                odds = [odd(v0, first + k, half, j) for k in range(10)]
                for i in range(1, 9):
                    x = first + i
                    v, o = evens[i], odds[i]
                    s = third(v) + relax * ((even(src, x, half, j) + (evens[i - 1] + evens[i + 1])) + ((below(v0, x, half, j) + o) + sides(v, 1)))
                    put0(out, x, 0, half, j, s * m)
                    s = third(o) + relax * ((odd(src, x, half, j) + (odds[i - 1] + odds[i + 1])) + ((above(v0, x, half, j) + v) + sides(o, 1)))
                    put0(out, x, 1, half, j, s * m)

    chunks(NX, 8, smooth0)


def images(src, first, half, j, count):
    evens = [even(src, first + k, half, j) for k in range(count + 2)]
    odds = [odd(src, first + k, half, j) for k in range(count + 2)]
    result = []
    for i in range(1, count + 1):
        v, o = evens[i], odds[i]
        e = 6.0 * v - ((evens[i - 1] + evens[i + 1]) + ((below(src, first + i, half, j) + o) + sides(v, 1)))
        d = 6.0 * o - ((odds[i - 1] + odds[i + 1]) + ((above(src, first + i, half, j) + v) + sides(o, 1)))
        result.append((v, o, e, d))
    return result


def cycles_kernel(where_ref, own, got, swapped, out, r0, z0, q0, w, v0, f1, v1, e1, f2, t2, e2, mask):
    gx0, core, gy, gz = where_ref[4], where_ref[3], where_ref[1], where_ref[2]
    rows, lanes = row_index((24, LANES)), lane_index((24, LANES))
    y = gy * BY - HY + 4 * rows
    z = (gz * 4 + gx0) * CZ - HZ + lanes
    mask[...] = jnp.where((y >= 0) & (y < NY) & (z >= 0) & (z < NZ), 1.0, 0.0)
    for ref, count in ((r0, NX), (z0, NX), (q0, NX), (w, NX), (v0, NX), (f1, NX // 2), (v1, NX // 2), (f2, NX // 4), (t2, NX // 4)):
        ref[0] = jnp.zeros(ref.shape[1:], jnp.float32)
        ref[count + 1] = jnp.zeros(ref.shape[1:], jnp.float32)
    nothing = jnp.zeros((1, LANES), jnp.float32)

    def edges(i, _):
        for ref in (r0, v0):
            ref[i, 0, 59:60] = nothing
            ref[i, 1, 0:1] = nothing
        return 0

    lax.fori_loop(1, NX + 1, edges, 0, unroll=8)

    def edges1(i, _):
        for ref in (f1, v1):
            ref[i, 79:80] = nothing
            ref[i, 0:1] = nothing
        return 0

    lax.fori_loop(1, NX // 2 + 1, edges1, 0, unroll=8)

    def edges2(i, _):
        for ref in (f2, t2):
            ref[i, 7:8] = nothing
            ref[i, 28:29] = nothing
        return 0

    lax.fori_loop(1, NX // 4 + 1, edges2, 0, unroll=8)
    lanes = lane_index((8, LANES))

    def unpack(left, right):
        def body(first):
            for i in range(2):
                for parity in range(2):
                    for half in range(2):
                        for j in WHOLE:
                            at = pl.ds(20 * (2 * parity + half) + j, 8)
                            a, c, b = left[first + i, at], own[first + i, at], right[first + i, at]
                            for k in range(4):
                                value = jnp.where(lanes < 32, roll(a, -32 * k, 1), jnp.where(lanes < 64, roll(c, 32 - 32 * k, 1), roll(b, 64 - 32 * k, 1)))
                                put0(r0, 4 * (first + i) + k + 1, parity, half, j, value)

        chunks(NX // 4, 2, body)

    @pl.when(core == 0)
    def _():
        unpack(got, swapped)

    @pl.when(core == 1)
    def _():
        unpack(swapped, got)

    low = {step: lanes & step == 0 for step in (1, 2)}

    def fold(x, step):
        return 0.5 * (x + jnp.where(low[step], roll(x, -step, 1), roll(x, step, 1)))

    cycle_down(r0, mask, fold, f1, f2, WHOLE)
    cycle_coarse(mask, f2, t2, e2, WHOLE, WHOLE)
    cycle_up(r0, mask, f1, e2, v1, e1, v0, z0, WHOLE, MIDDLE)

    def image(first):
        for j in MIDDLE:
            m = mask[pl.ds(j, 8)]
            for half in range(2):
                for i, (_, _, e, d) in enumerate(images(z0, first, half, j, 8)):
                    put0(q0, first + i + 1, 0, half, j, e * m)
                    put0(q0, first + i + 1, 1, half, j, d * m)

    chunks(NX, 8, image)
    cycle_down(q0, mask, fold, f1, f2, MIDDLE)
    cycle_coarse(mask, f2, t2, e2, MIDDLE, HOME)
    cycle_up(q0, mask, f1, e2, v1, e1, v0, w, HOME, HOME)

    inside = (lanes >= HZ) & (lanes < HZ + CZ) & (row_index((8, LANES)) < 4)

    def sums(i, acc):
        acc = list(acc)
        for half in range(2):
            for k, (we, wo, se, so) in enumerate(images(w, 8 * i, half, 8, 8)):
                x = 8 * i + k + 1
                for get, ww, s in ((even, we, se), (odd, wo, so)):
                    r, zz, q = get(r0, x, half, 8), get(z0, x, half, 8), get(q0, x, half, 8)
                    for n, term in enumerate((r * zz, zz * q, r * ww, q * ww, ww * s)):
                        acc[n] = acc[n] + term
                at = 20 * half + 8
                v0[x, 0, pl.ds(at, 8)] = se
                v0[x, 1, pl.ds(20 + at, 8)] = so
        return tuple(acc)

    acc = lax.fori_loop(0, NX // 8, sums, (jnp.zeros((8, LANES), jnp.float32),) * 5)

    def send(t, _):
        for k in range(BX):
            x = BX * (2 * t + core) + k + 1
            for at in range(4):
                parity, half = at // 2, at % 2
                rows = pl.ds(20 * parity + 20 * half + 8, 4)
                zz, q, ww, s = (ref[x, parity, rows] for ref in (z0, q0, w, v0))
                wide = lanes[0:4]
                out[t, pl.ds(k * BY + 4 * at, 4)] = jnp.where(
                    wide < 32, roll(zz, -32, 1), jnp.where(wide < 64, q, jnp.where(wide < 96, roll(ww, 32, 1), roll(s, 64, 1)))
                )
        return 0

    lax.fori_loop(0, 4, send, 0)
    row = jnp.zeros((8, LANES), jnp.float32)
    for k, a in enumerate(acc):
        row = jnp.where(lanes == k, jnp.sum(jnp.where(inside, a, 0.0)), row)
    for t in range(4):
        out[t, BX * BY : BX * BY + 8] = row


def cycles(where, own, got, swapped):
    fine = pltpu.VMEM((NX + 2, 2, 64, LANES), jnp.float32)
    level1 = pltpu.VMEM((NX // 2 + 2, 80, LANES), jnp.float32)
    level2 = pltpu.VMEM((NX // 4 + 2, 40, LANES), jnp.float32)
    return pl.pallas_call(
        cycles_kernel,
        out_shape=jax.ShapeDtypeStruct((4, BX * BY + 8, LANES), jnp.float32),
        in_specs=[SMEM] + [VMEM] * 3,
        out_specs=VMEM,
        scratch_shapes=[fine] * 5 + [level1, level1, pltpu.VMEM((NX // 2 + 2, 40, LANES), jnp.float32)] + [level2] * 3 + [pltpu.VMEM((24, LANES), jnp.float32)],
        compiler_params=pltpu.CompilerParams(vmem_limit_bytes=48 * 1024 * 1024),
    )(where, own, got, swapped)


def finish_kernel(rhs, fields, sums, solution, residual):
    total = jnp.sum(sums[...], axis=0, keepdims=True)
    lanes = lane_index(total.shape)

    def pick(k):
        return jnp.sum(jnp.where(lanes == k, total, 0.0), axis=1, keepdims=True)

    rz, zq, rw, qw, ws = (pick(k) for k in range(5))
    step0 = rz / zq
    rz1 = rz - step0 * (rw + zq) + step0 * step0 * qw
    growth = rz1 / rz
    image1 = (zq - 2.0 * step0 * qw + step0 * step0 * ws) + 2.0 * growth * (zq - step0 * qw) + growth * growth * zq
    step1 = rz1 / image1
    on_z = step0 + step1 * (1.0 + growth)
    on_w = -step1 * step0
    wide = lane_index((BY, LANES))
    for x in range(BX):
        parts = [fields[c, x * BY : (x + 1) * BY] for c in range(4)]

        def field(f):
            value = None
            for c in range(4):
                part = roll(parts[c], 32 * (c - f), 1)
                value = part if c == 0 else jnp.where(wide >= 32 * c, part, value)
            return value

        z0, q0, w, s = (field(f) for f in range(4))
        u = on_z * z0 + on_w * w
        v = on_z * q0 + on_w * s
        for at, plane in enumerate(PLANES):
            rows = pl.ds(plane, 4, stride=4)
            solution[x, rows, :] = u[4 * at : 4 * at + 4]
            residual[x, rows, :] = rhs[x, rows, :] - v[4 * at : 4 * at + 4]


def finish(rhs, fields, sums):
    shape = jax.ShapeDtypeStruct((BX, BY, BZ), jnp.float32)
    return pl.pallas_call(finish_kernel, out_shape=(shape, shape), in_specs=[VMEM] * 3, out_specs=(VMEM, VMEM))(rhs, fields, sums)


def both_ways(count, step):
    pairs = [(i, i + step) for i in range(count - step)]
    return pairs + [(count + b, count + a) for a, b in pairs]


def z_pairs():
    def number(core, block):
        return ((block % 4) * 2 + core) * 8 + block // 4

    up = [(i, i + 1) for i in range(31)]
    return [(number(0, a), number(0, b)) for a, b in up] + [(number(1, b), number(1, a)) for a, b in up]


SWAP = [(0, 1), (1, 0)]


def local(density, x_faces, y_faces, z_faces):
    where = jnp.stack([lax.axis_index(GX), lax.axis_index("gy"), lax.axis_index("gz"), lax.axis_index("gx_1"), lax.axis_index("gx_0")]).astype(jnp.int32)
    rhs, packed = make_rhs(where, density, x_faces, y_faces, z_faces)
    own = lax.all_to_all(packed, GX, 0, 0, tiled=True).reshape(16, BY, 128)
    near = lax.ppermute(own, ("gx_1", "gy"), both_ways(16, 1))
    far = lax.ppermute(own, ("gx_1", "gy"), both_ways(16, 2))
    near2 = lax.ppermute(near, "gx_1", SWAP)
    far2 = lax.ppermute(far, "gx_1", SWAP)
    joined = join(where, own, near, far, near2, far2)
    got = lax.ppermute(joined, ("gx_0", "gx_1", "gz"), z_pairs())
    swapped = lax.ppermute(got, "gx_1", SWAP)
    packed = cycles(where, joined, got, swapped)
    fields = lax.all_to_all(packed, "gx_0", 0, 0, tiled=True)
    sums = jnp.sum(fields[:, BX * BY, :], axis=0)
    sums = lax.all_to_all(jnp.broadcast_to(sums, (128, 1, 128)), ("gy", "gz"), 0, 0, tiled=True)
    return finish(rhs, fields, sums.reshape(128, 128))


def solution(mesh):
    torus = Mesh(mesh.devices.reshape(4, 2, mesh.shape["gy"], mesh.shape["gz"]), AXES)
    in_specs = (P(GX, "gy", "gz"), P(None, "gy", "gz"), P(None, GX, "gz"), P(None, GX, "gy"))
    out_specs = (P(GX, "gy", "gz"), P(GX, "gy", "gz"))
    return jax.shard_map(local, mesh=torus, in_specs=in_specs, out_specs=out_specs, check_vma=False)
```

```python
import functools

import jax
import jax.numpy as jnp
from jax import lax
from jax.experimental import pallas as pl
from jax.experimental.pallas import tpu as pltpu
from jax.sharding import Mesh
from jax.sharding import PartitionSpec as P

AXES = ("gx_0", "gx_1", "gy", "gz")
GX = ("gx_0", "gx_1")
NX, NY, NZ = 64, 256, 1024
BX, BY, BZ = 8, 16, 128
CZ = 32
HY, HZ = 32, 32
ROWS, LANES = BY + 2 * HY, 128
relax = 1.0 / 9.0
coupling = 0.5
VMEM = pl.BlockSpec(memory_space=pltpu.VMEM)
HBM = pl.BlockSpec(memory_space=pltpu.MemorySpace.HBM)


def roll(x, shift, axis):
    return pltpu.roll(x, shift % x.shape[axis], axis)


def place():
    return tuple(lax.axis_index(axis) for axis in AXES)


def small(**more):
    return pltpu.CompilerParams(vmem_limit_bytes=4 * 1024 * 1024, **more)


def lane_index(shape):
    return lax.broadcasted_iota(jnp.int32, shape, 1)


def row_index(shape):
    return lax.broadcasted_iota(jnp.int32, shape, 0)


PLANES = (0, 2, 1, 3)


def rhs_kernel(density_in, xf_in, yf_in, zf_in, rhs, packed, scratch, density, xf, yf, zf, arrived):
    copies = [pltpu.make_async_copy(a, b, arrived.at[i]) for i, (a, b) in enumerate(((density_in, density), (xf_in, xf), (yf_in, yf), (zf_in, zf)))]
    for copy in copies:
        copy.start()
    gx0, core, gy, gz = place()
    gx = 2 * gx0 + core
    rows, lanes = row_index((BY, BZ)), lane_index((BY, BZ))
    eye = row_index((BY, BY)) == lane_index((BY, BY))
    low_y = (rows == 0) & (gy == 0)
    high_y = (rows == BY - 1) & (gy == NY // BY - 1)
    low_z = (lanes == 0) & (gz == 0)
    high_z = (lanes == BZ - 1) & (gz == NZ // BZ - 1)

    def column(row):
        return jnp.sum(jnp.where(eye, row, 0.0), axis=1, keepdims=True)

    for copy in copies:
        copy.wait()
    layers = []
    for x in range(BX):
        value = -coupling * density[x]
        if x == 0:
            value = value + jnp.where(gx == 0, xf[0], 0.0)
        if x == BX - 1:
            value = value + jnp.where(gx == NX // BX - 1, xf[1], 0.0)
        value = value + jnp.where(low_y, yf[0, x : x + 1, :], 0.0)
        value = value + jnp.where(high_y, yf[1, x : x + 1, :], 0.0)
        value = value + jnp.where(low_z, column(zf[0, x : x + 1, :]), 0.0)
        value = value + jnp.where(high_z, column(zf[1, x : x + 1, :]), 0.0)
        rhs[x] = value
        layers.append(value)
    for chunk in range(4):
        for quad in range(2):
            out = None
            for k in range(4):
                part = roll(layers[4 * quad + k], 32 * (k - chunk), 1)
                out = part if k == 0 else jnp.where(lanes >= 32 * k, part, out)
            scratch[chunk, quad] = out
    for chunk in range(4):
        for quad in range(2):
            for at, plane in enumerate(PLANES):
                part = scratch[chunk, quad, pl.ds(plane, 4, stride=4), :]
                packed[2 * chunk, quad, 4 * at : 4 * at + 4] = part
                packed[2 * chunk + 1, quad, 4 * at : 4 * at + 4] = part


def make_rhs(density, xf, yf, zf):
    return pl.pallas_call(
        rhs_kernel,
        out_shape=(
            jax.ShapeDtypeStruct((BX, BY, BZ), jnp.float32),
            jax.ShapeDtypeStruct((8, 2, BY, BZ), jnp.float32),
        ),
        in_specs=[HBM] * 4,
        out_specs=(VMEM, VMEM),
        scratch_shapes=[pltpu.VMEM((4, 2, BY, BZ), jnp.float32)]
        + [pltpu.VMEM(a.shape, a.dtype) for a in (density, xf, yf, zf)]
        + [pltpu.SemaphoreType.DMA((4,))],
        compiler_params=small(),
    )(density, xf, yf, zf)


WHOLE = (0, 8, 12)
MIDDLE = (4, 12)
HOME = (6,)


def sides(x, step):
    return roll(x, step, 1) + roll(x, -step, 1)


def third(x):
    return x * (1.0 / 3.0)


def even(ref, x, half, j):
    return ref[x, 0, pl.ds(20 * half + j, 8)]


def odd(ref, x, half, j):
    return ref[x, 1, pl.ds(20 + 20 * half + j, 8)]


def below(ref, x, half, j):
    return ref[x, 1, pl.ds(20 * half + j, 8)]


def above(ref, x, half, j):
    return ref[x, 0, pl.ds(20 + 20 * half + j, 8)]


def put0(ref, x, parity, half, j, value):
    if parity == 0:
        if half == 0:
            ref[x, 0, pl.ds(39 + j, 8)] = value
        ref[x, 0, pl.ds(20 * half + j, 8)] = value
    else:
        if half == 1:
            if j == 12:
                ref[x, 1, pl.ds(13, 7)] = value[0:7]
            else:
                ref[x, 1, pl.ds(1 + j, 8)] = value
        ref[x, 1, pl.ds(20 + 20 * half + j, 8)] = value


def put1(ref, x, half, j, value):
    if half == 0:
        ref[x, pl.ds(59 + j, 8)] = value
    elif j == 12:
        ref[x, pl.ds(13, 7)] = value[0:7]
    else:
        ref[x, pl.ds(1 + j, 8)] = value
    ref[x, pl.ds(20 + 20 * half + j, 8)] = value


def chunks(count, size, body):
    lax.fori_loop(0, count // size, lambda i, _: body(i * size) or 0, 0)


def cycle_down(src, mask, fold, f1, f2, tiles):
    def level1(first):
        for j in tiles:
            m = mask[pl.ds(j, 8)]
            for half in range(2):
                cells = [even(src, 2 * first + k, half, j) + odd(src, 2 * first + k, half, j) for k in range(10)]
                for i in range(4):
                    before, a, b, after = cells[2 * i : 2 * i + 4]
                    u = a + b
                    y = [below(src, 2 * first + 2 * i + k, half, j) + above(src, 2 * first + 2 * i + k, half, j) for k in (1, 2)]
                    s = third(u) + relax * (((u + u) + (before + after)) + ((y[0] + y[1]) + sides(u, 1)))
                    put1(f1, first + i + 1, half, j, fold(s, 1) * m)

    chunks(NX // 2, 4, level1)

    def level2(first):
        for j in tiles:
            m = mask[pl.ds(j, 8)]
            cells = [f1[2 * first + k, pl.ds(20 + j, 8)] + f1[2 * first + k, pl.ds(40 + j, 8)] for k in range(10)]
            for i in range(4):
                before, a, b, after = cells[2 * i : 2 * i + 4]
                u = a + b
                y = [f1[2 * first + 2 * i + k, pl.ds(j, 8)] + f1[2 * first + 2 * i + k, pl.ds(60 + j, 8)] for k in (1, 2)]
                s = third(u) + relax * (((u + u) + (before + after)) + ((y[0] + y[1]) + sides(u, 2)))
                f2[first + i + 1, pl.ds(8 + j, 8)] = fold(s, 2) * m

    chunks(NX // 4, 4, level2)


def cycle_coarse(mask, f2, t2, e2, tiles, last):
    def around(ref, x, j):
        return (ref[x - 1, pl.ds(8 + j, 8)] + ref[x + 1, pl.ds(8 + j, 8)]) + (ref[x, pl.ds(7 + j, 8)] + ref[x, pl.ds(9 + j, 8)])

    def sweep1(first):
        for j in tiles:
            m = mask[pl.ds(j, 8)]
            for i in range(1, 9):
                r = f2[first + i, pl.ds(8 + j, 8)]
                s = (4.0 / 3.0) * r + relax * (around(f2, first + i, j) + sides(r, 4))
                t2[first + i, pl.ds(8 + j, 8)] = (relax * s) * m

    chunks(NX // 4, 8, sweep1)

    def sweep2(first):
        for j in last:
            m = mask[pl.ds(j, 8)]
            for i in range(1, 9):
                v = t2[first + i, pl.ds(8 + j, 8)]
                s = third(v) + relax * (f2[first + i, pl.ds(8 + j, 8)] + (around(t2, first + i, j) + sides(v, 4)))
                e2[first + i, pl.ds(8 + j, 8)] = s * m

    chunks(NX // 4, 8, sweep2)


def cycle_up(src, mask, f1, e2, v1, e1, v0, out, tiles, last):
    def correct1(first):
        for j in tiles:
            for i in range(4):
                e = e2[first + i + 1, pl.ds(8 + j, 8)]
                for half in range(2):
                    for k in (1, 2):
                        x = 2 * first + 2 * i + k
                        put1(v1, x, half, j, relax * f1[x, pl.ds(20 + 20 * half + j, 8)] + e)

    chunks(NX // 4, 4, correct1)

    def smooth1(first):
        for j in tiles:
            m = mask[pl.ds(j, 8)]
            for half in range(2):
                at = pl.ds(20 + 20 * half + j, 8)
                for i in range(1, 9):
                    x = first + i
                    v = v1[x, at]
                    y = v1[x, pl.ds(20 * half + j, 8)] + v1[x, pl.ds(40 + 20 * half + j, 8)]
                    s = third(v) + relax * ((f1[x, at] + (v1[x - 1, at] + v1[x + 1, at])) + (y + sides(v, 2)))
                    e1[x, pl.ds(20 * half + j, 8)] = s * m

    chunks(NX // 2, 8, smooth1)

    def correct0(first):
        for j in tiles:
            for i in range(1, 5):
                for half in range(2):
                    e = e1[first + i, pl.ds(20 * half + j, 8)]
                    for k in (-1, 0):
                        x = 2 * first + 2 * i + k
                        put0(v0, x, 0, half, j, relax * even(src, x, half, j) + e)
                        put0(v0, x, 1, half, j, relax * odd(src, x, half, j) + e)

    chunks(NX // 2, 4, correct0)

    def smooth0(first):
        for j in last:
            m = mask[pl.ds(j, 8)]
            for half in range(2):
                evens = [even(v0, first + k, half, j) for k in range(10)]
                odds = [odd(v0, first + k, half, j) for k in range(10)]
                for i in range(1, 9):
                    x = first + i
                    v, o = evens[i], odds[i]
                    s = third(v) + relax * ((even(src, x, half, j) + (evens[i - 1] + evens[i + 1])) + ((below(v0, x, half, j) + o) + sides(v, 1)))
                    put0(out, x, 0, half, j, s * m)
                    s = third(o) + relax * ((odd(src, x, half, j) + (odds[i - 1] + odds[i + 1])) + ((above(v0, x, half, j) + v) + sides(o, 1)))
                    put0(out, x, 1, half, j, s * m)

    chunks(NX, 8, smooth0)


def images(src, first, half, j, count):
    evens = [even(src, first + k, half, j) for k in range(count + 2)]
    odds = [odd(src, first + k, half, j) for k in range(count + 2)]
    result = []
    for i in range(1, count + 1):
        v, o = evens[i], odds[i]
        e = 6.0 * v - ((evens[i - 1] + evens[i + 1]) + ((below(src, first + i, half, j) + o) + sides(v, 1)))
        d = 6.0 * o - ((odds[i - 1] + odds[i + 1]) + ((above(src, first + i, half, j) + v) + sides(o, 1)))
        result.append((v, o, e, d))
    return result


def cycles_kernel(own, side, side2, rows_, rows2, up, up2, down, down2, out, r0, z0, q0, w, v0, f1, v1, e1, f2, t2, e2, mask):
    gx0, core, gy, gz = place()
    rows, lanes = row_index((24, LANES)), lane_index((24, LANES))
    y = gy * BY - HY + 4 * rows
    z = (gz * 4 + gx0) * CZ - HZ + lanes
    mask[...] = jnp.where((y >= 0) & (y < NY) & (z >= 0) & (z < NZ), 1.0, 0.0)
    for ref, count in ((r0, NX), (z0, NX), (q0, NX), (w, NX), (v0, NX), (f1, NX // 2), (v1, NX // 2), (f2, NX // 4), (t2, NX // 4)):
        ref[0] = jnp.zeros(ref.shape[1:], jnp.float32)
        ref[count + 1] = jnp.zeros(ref.shape[1:], jnp.float32)
    nothing = jnp.zeros((1, LANES), jnp.float32)

    def edges(i, _):
        for ref in (r0, v0):
            ref[i, 0, 59:60] = nothing
            ref[i, 1, 0:1] = nothing
        return 0

    lax.fori_loop(1, NX + 1, edges, 0, unroll=8)

    def edges1(i, _):
        for ref in (f1, v1):
            ref[i, 79:80] = nothing
            ref[i, 0:1] = nothing
        return 0

    lax.fori_loop(1, NX // 2 + 1, edges1, 0, unroll=8)

    def edges2(i, _):
        for ref in (f2, t2):
            ref[i, 7:8] = nothing
            ref[i, 28:29] = nothing
        return 0

    lax.fori_loop(1, NX // 4 + 1, edges2, 0, unroll=8)
    lanes = lane_index((8, LANES))

    def unpack(low_side, high_side, low_rows, high_rows, low_up, high_up, low_down, high_down):
        blocks = (
            (low_up, low_rows, low_down, 1),
            (low_up, low_rows, low_down, 0),
            (low_side, own, high_side, None),
            (high_up, high_rows, high_down, 0),
            (high_up, high_rows, high_down, 1),
        )

        def body(i, _):
            for b, (left, middle, right, pair) in enumerate(blocks):
                for parity in range(2):
                    at = pl.ds(8 * parity, 8)
                    a, c, d = ((ref[i, at] if pair is None else ref[pair, i, at]) for ref in (left, middle, right))
                    for k in range(4):
                        value = jnp.where(lanes < 32, roll(a, -32 * k, 1), jnp.where(lanes < 64, roll(c, 32 - 32 * k, 1), roll(d, 64 - 32 * k, 1)))
                        x = 4 * i + k + 1
                        if parity == 0:
                            if b > 0:
                                r0[x, 0, 39 + 4 * b : 43 + 4 * b] = value[0:4]
                            else:
                                r0[x, 0, 40:43] = value[1:4]
                            r0[x, 0, 4 * b : 4 * b + 4] = value[0:4]
                            r0[x, 0, 20 + 4 * b : 24 + 4 * b] = value[4:8]
                        else:
                            if b < 4:
                                r0[x, 1, 1 + 4 * b : 5 + 4 * b] = value[4:8]
                            else:
                                r0[x, 1, 17:20] = value[4:7]
                            r0[x, 1, 20 + 4 * b : 24 + 4 * b] = value[0:4]
                            r0[x, 1, 40 + 4 * b : 44 + 4 * b] = value[4:8]
            return 0

        lax.fori_loop(0, NX // 4, body, 0)

    @pl.when(core == 0)
    def _():
        unpack(side, side2, rows_, rows2, up, up2, down, down2)

    @pl.when(core == 1)
    def _():
        unpack(side2, side, rows2, rows_, up2, up, down2, down)

    low = {step: lanes & step == 0 for step in (1, 2)}

    def fold(x, step):
        return 0.5 * (x + jnp.where(low[step], roll(x, -step, 1), roll(x, step, 1)))

    cycle_down(r0, mask, fold, f1, f2, WHOLE)
    cycle_coarse(mask, f2, t2, e2, WHOLE, WHOLE)
    cycle_up(r0, mask, f1, e2, v1, e1, v0, z0, WHOLE, MIDDLE)

    def image(first):
        for j in MIDDLE:
            m = mask[pl.ds(j, 8)]
            for half in range(2):
                for i, (_, _, e, d) in enumerate(images(z0, first, half, j, 8)):
                    put0(q0, first + i + 1, 0, half, j, e * m)
                    put0(q0, first + i + 1, 1, half, j, d * m)

    chunks(NX, 8, image)
    cycle_down(q0, mask, fold, f1, f2, MIDDLE)
    cycle_coarse(mask, f2, t2, e2, MIDDLE, HOME)
    cycle_up(q0, mask, f1, e2, v1, e1, v0, w, HOME, HOME)

    inside = (lanes >= HZ) & (lanes < HZ + CZ) & (row_index((8, LANES)) < 4)

    def sums(i, acc):
        acc = list(acc)
        for half in range(2):
            for k, (we, wo, se, so) in enumerate(images(w, 8 * i, half, 8, 8)):
                x = 8 * i + k + 1
                for get, ww, s in ((even, we, se), (odd, wo, so)):
                    r, zz, q = get(r0, x, half, 8), get(z0, x, half, 8), get(q0, x, half, 8)
                    for n, term in enumerate((r * zz, zz * q, r * ww, q * ww, ww * s)):
                        acc[n] = acc[n] + term
                at = 20 * half + 8
                v0[x, 0, pl.ds(at, 8)] = se
                v0[x, 1, pl.ds(20 + at, 8)] = so
        return tuple(acc)

    acc = lax.fori_loop(0, NX // 8, sums, (jnp.zeros((8, LANES), jnp.float32),) * 5)

    def send(t, _):
        for k in range(BX):
            x = BX * (2 * t + core) + k + 1
            for at in range(4):
                parity, half = at // 2, at % 2
                rows = pl.ds(20 * parity + 20 * half + 8, 4)
                zz, q, ww, s = (ref[x, parity, rows] for ref in (z0, q0, w, v0))
                wide = lanes[0:4]
                out[t, pl.ds(k * BY + 4 * at, 4)] = jnp.where(
                    wide < 32, roll(zz, -32, 1), jnp.where(wide < 64, q, jnp.where(wide < 96, roll(ww, 32, 1), roll(s, 64, 1)))
                )
        return 0

    lax.fori_loop(0, 4, send, 0)
    row = jnp.zeros((8, LANES), jnp.float32)
    for k, a in enumerate(acc):
        row = jnp.where(lanes == k, jnp.sum(jnp.where(inside, a, 0.0)), row)
    for t in range(4):
        out[t, BX * BY : BX * BY + 8] = row


def cycles(*blocks):
    fine = pltpu.VMEM((NX + 2, 2, 64, LANES), jnp.float32)
    level1 = pltpu.VMEM((NX // 2 + 2, 80, LANES), jnp.float32)
    level2 = pltpu.VMEM((NX // 4 + 2, 40, LANES), jnp.float32)
    return pl.pallas_call(
        cycles_kernel,
        out_shape=jax.ShapeDtypeStruct((4, BX * BY + 8, LANES), jnp.float32),
        in_specs=[VMEM] * 9,
        out_specs=VMEM,
        scratch_shapes=[fine] * 5 + [level1, level1, pltpu.VMEM((NX // 2 + 2, 40, LANES), jnp.float32)] + [level2] * 3 + [pltpu.VMEM((24, LANES), jnp.float32)],
        compiler_params=pltpu.CompilerParams(vmem_limit_bytes=30 * 1024 * 1024),
    )(*blocks)


def finish_kernel(rhs, fields, sums, solution, residual):
    total = jnp.sum(sums[...], axis=0, keepdims=True)
    lanes = lane_index(total.shape)

    def pick(k):
        return jnp.sum(jnp.where(lanes == k, total, 0.0), axis=1, keepdims=True)

    rz, zq, rw, qw, ws = (pick(k) for k in range(5))
    step0 = rz / zq
    rz1 = rz - step0 * (rw + zq) + step0 * step0 * qw
    growth = rz1 / rz
    image1 = (zq - 2.0 * step0 * qw + step0 * step0 * ws) + 2.0 * growth * (zq - step0 * qw) + growth * growth * zq
    step1 = rz1 / image1
    on_z = step0 + step1 * (1.0 + growth)
    on_w = -step1 * step0
    wide = lane_index((BY, LANES))
    for x in range(BX):
        parts = [fields[c, x * BY : (x + 1) * BY] for c in range(4)]

        def field(f):
            value = None
            for c in range(4):
                part = roll(parts[c], 32 * (c - f), 1)
                value = part if c == 0 else jnp.where(wide >= 32 * c, part, value)
            return value

        z0, q0, w, s = (field(f) for f in range(4))
        u = on_z * z0 + on_w * w
        v = on_z * q0 + on_w * s
        for at, plane in enumerate(PLANES):
            rows = pl.ds(plane, 4, stride=4)
            solution[x, rows, :] = u[4 * at : 4 * at + 4]
            residual[x, rows, :] = rhs[x, rows, :] - v[4 * at : 4 * at + 4]


def finish(rhs, fields, sums):
    shape = jax.ShapeDtypeStruct((BX, BY, BZ), jnp.float32)
    return pl.pallas_call(finish_kernel, out_shape=(shape, shape), in_specs=[VMEM] * 3, out_specs=(VMEM, VMEM), compiler_params=small())(rhs, fields, sums)


def both_ways(count, step):
    pairs = [(i, i + step) for i in range(count - step)]
    return pairs + [(count + b, count + a) for a, b in pairs]


def z_pairs(steps):
    def number(core, block):
        return ((block % 4) * 2 + core) * 8 + block // 4

    return [(number(core, a), number(core, a + step)) for core, step in enumerate(steps) for a in range(32) if 0 <= a + step < 32]


SWAP = [(0, 1), (1, 0)]
Z_AXES = ("gx_0", "gx_1", "gz")


def local(density, x_faces, y_faces, z_faces):
    rhs, packed = make_rhs(density, x_faces, y_faces, z_faces)
    own = lax.all_to_all(packed, GX, 0, 0, tiled=True).reshape(16, BY, 128)
    near = lax.ppermute(own, ("gx_1", "gy"), both_ways(16, 1))
    far = lax.ppermute(own, ("gx_1", "gy"), both_ways(16, 2))
    side = lax.ppermute(own, Z_AXES, z_pairs((1, -1)))
    rows = jnp.stack([near, far])
    up = lax.ppermute(rows, Z_AXES, z_pairs((1, 1)))
    down = lax.ppermute(rows, Z_AXES, z_pairs((-1, -1)))
    swapped = [lax.ppermute(each, "gx_1", SWAP) for each in (side, rows, up, down)]
    packed = cycles(own, side, swapped[0], rows, swapped[1], up, swapped[2], down, swapped[3])
    fields = lax.all_to_all(packed, "gx_0", 0, 0, tiled=True)
    sums = jnp.sum(fields[:, BX * BY, :], axis=0)
    sums = lax.all_to_all(jnp.broadcast_to(sums, (128, 1, 128)), ("gy", "gz"), 0, 0, tiled=True)
    return finish(rhs, fields, sums.reshape(128, 128))


def solution(mesh):
    torus = Mesh(mesh.devices.reshape(4, 2, mesh.shape["gy"], mesh.shape["gz"]), AXES)
    in_specs = (P(GX, "gy", "gz"), P(None, "gy", "gz"), P(None, GX, "gz"), P(None, GX, "gy"))
    out_specs = (P(GX, "gy", "gz"), P(GX, "gy", "gz"))
    return jax.shard_map(local, mesh=torus, in_specs=in_specs, out_specs=out_specs, check_vma=False)
```

```python
import functools

import jax
import jax.numpy as jnp
from jax import lax
from jax.experimental import pallas as pl
from jax.experimental.pallas import tpu as pltpu
from jax.sharding import Mesh
from jax.sharding import PartitionSpec as P

AXES = ("gx_0", "gx_1", "gy", "gz")
GX = ("gx_0", "gx_1")
NX, NY, NZ = 64, 256, 1024
BX, BY, BZ = 8, 16, 128
CZ = 32
HY, HZ = 32, 32
ROWS, LANES = BY + 2 * HY, 128
relax = 1.0 / 9.0
coupling = 0.5
VMEM = pl.BlockSpec(memory_space=pltpu.VMEM)
HBM = pl.BlockSpec(memory_space=pltpu.MemorySpace.HBM)


def roll(x, shift, axis):
    return pltpu.roll(x, shift % x.shape[axis], axis)


def place():
    return tuple(lax.axis_index(axis) for axis in AXES)


def small(**more):
    return pltpu.CompilerParams(vmem_limit_bytes=4 * 1024 * 1024, **more)


def lane_index(shape):
    return lax.broadcasted_iota(jnp.int32, shape, 1)


def row_index(shape):
    return lax.broadcasted_iota(jnp.int32, shape, 0)


PLANES = (0, 2, 1, 3)


def rhs_kernel(density_in, xf_in, yf_in, zf_in, rhs, packed, scratch, density, xf, yf, zf, arrived):
    copies = [pltpu.make_async_copy(a, b, arrived.at[i]) for i, (a, b) in enumerate(((density_in, density), (xf_in, xf), (yf_in, yf), (zf_in, zf)))]
    for copy in copies:
        copy.start()
    gx0, core, gy, gz = place()
    gx = 2 * gx0 + core
    rows, lanes = row_index((BY, BZ)), lane_index((BY, BZ))
    eye = row_index((BY, BY)) == lane_index((BY, BY))
    low_y = (rows == 0) & (gy == 0)
    high_y = (rows == BY - 1) & (gy == NY // BY - 1)
    low_z = (lanes == 0) & (gz == 0)
    high_z = (lanes == BZ - 1) & (gz == NZ // BZ - 1)

    def column(row):
        return jnp.sum(jnp.where(eye, row, 0.0), axis=1, keepdims=True)

    for copy in copies:
        copy.wait()
    layers = []
    for x in range(BX):
        value = -coupling * density[x]
        if x == 0:
            value = value + jnp.where(gx == 0, xf[0], 0.0)
        if x == BX - 1:
            value = value + jnp.where(gx == NX // BX - 1, xf[1], 0.0)
        value = value + jnp.where(low_y, yf[0, x : x + 1, :], 0.0)
        value = value + jnp.where(high_y, yf[1, x : x + 1, :], 0.0)
        value = value + jnp.where(low_z, column(zf[0, x : x + 1, :]), 0.0)
        value = value + jnp.where(high_z, column(zf[1, x : x + 1, :]), 0.0)
        rhs[x] = value
        layers.append(value)
    for chunk in range(4):
        for quad in range(2):
            out = None
            for k in range(4):
                part = roll(layers[4 * quad + k], 32 * (k - chunk), 1)
                out = part if k == 0 else jnp.where(lanes >= 32 * k, part, out)
            scratch[chunk, quad] = out
    for chunk in range(4):
        for quad in range(2):
            for at, plane in enumerate(PLANES):
                part = scratch[chunk, quad, pl.ds(plane, 4, stride=4), :]
                packed[2 * chunk, quad, 4 * at : 4 * at + 4] = part
                packed[2 * chunk + 1, quad, 4 * at : 4 * at + 4] = part


def make_rhs(density, xf, yf, zf):
    return pl.pallas_call(
        rhs_kernel,
        out_shape=(
            jax.ShapeDtypeStruct((BX, BY, BZ), jnp.float32),
            jax.ShapeDtypeStruct((8, 2, BY, BZ), jnp.float32),
        ),
        in_specs=[HBM] * 4,
        out_specs=(VMEM, VMEM),
        scratch_shapes=[pltpu.VMEM((4, 2, BY, BZ), jnp.float32)]
        + [pltpu.VMEM(a.shape, a.dtype) for a in (density, xf, yf, zf)]
        + [pltpu.SemaphoreType.DMA((4,))],
        compiler_params=pltpu.CompilerParams(vmem_limit_bytes=60 * 1024 * 1024),
    )(density, xf, yf, zf)


WHOLE = (0, 8, 12)
MIDDLE = (4, 12)
HOME = (6,)


def sides(x, step):
    return roll(x, step, 1) + roll(x, -step, 1)


def third(x):
    return x * (1.0 / 3.0)


def even(ref, x, half, j):
    return ref[x, 0, pl.ds(20 * half + j, 8)]


def odd(ref, x, half, j):
    return ref[x, 1, pl.ds(20 + 20 * half + j, 8)]


def below(ref, x, half, j):
    return ref[x, 1, pl.ds(20 * half + j, 8)]


def above(ref, x, half, j):
    return ref[x, 0, pl.ds(20 + 20 * half + j, 8)]


def put0(ref, x, parity, half, j, value):
    if parity == 0:
        if half == 0:
            ref[x, 0, pl.ds(39 + j, 8)] = value
        ref[x, 0, pl.ds(20 * half + j, 8)] = value
    else:
        if half == 1:
            if j == 12:
                ref[x, 1, pl.ds(13, 7)] = value[0:7]
            else:
                ref[x, 1, pl.ds(1 + j, 8)] = value
        ref[x, 1, pl.ds(20 + 20 * half + j, 8)] = value


def put1(ref, x, half, j, value):
    if half == 0:
        ref[x, pl.ds(59 + j, 8)] = value
    elif j == 12:
        ref[x, pl.ds(13, 7)] = value[0:7]
    else:
        ref[x, pl.ds(1 + j, 8)] = value
    ref[x, pl.ds(20 + 20 * half + j, 8)] = value


def chunks(count, size, body):
    lax.fori_loop(0, count // size, lambda i, _: body(i * size) or 0, 0)


def cycle_down(src, mask, fold, f1, f2, tiles):
    def level1(first):
        for j in tiles:
            m = mask[pl.ds(j, 8)]
            for half in range(2):
                cells = [even(src, 2 * first + k, half, j) + odd(src, 2 * first + k, half, j) for k in range(10)]
                for i in range(4):
                    before, a, b, after = cells[2 * i : 2 * i + 4]
                    u = a + b
                    y = [below(src, 2 * first + 2 * i + k, half, j) + above(src, 2 * first + 2 * i + k, half, j) for k in (1, 2)]
                    s = third(u) + relax * (((u + u) + (before + after)) + ((y[0] + y[1]) + sides(u, 1)))
                    put1(f1, first + i + 1, half, j, fold(s, 1) * m)

    chunks(NX // 2, 4, level1)

    def level2(first):
        for j in tiles:
            m = mask[pl.ds(j, 8)]
            cells = [f1[2 * first + k, pl.ds(20 + j, 8)] + f1[2 * first + k, pl.ds(40 + j, 8)] for k in range(10)]
            for i in range(4):
                before, a, b, after = cells[2 * i : 2 * i + 4]
                u = a + b
                y = [f1[2 * first + 2 * i + k, pl.ds(j, 8)] + f1[2 * first + 2 * i + k, pl.ds(60 + j, 8)] for k in (1, 2)]
                s = third(u) + relax * (((u + u) + (before + after)) + ((y[0] + y[1]) + sides(u, 2)))
                f2[first + i + 1, pl.ds(8 + j, 8)] = fold(s, 2) * m

    chunks(NX // 4, 4, level2)


def cycle_coarse(mask, f2, t2, e2, tiles, last):
    def around(ref, x, j):
        return (ref[x - 1, pl.ds(8 + j, 8)] + ref[x + 1, pl.ds(8 + j, 8)]) + (ref[x, pl.ds(7 + j, 8)] + ref[x, pl.ds(9 + j, 8)])

    def sweep1(first):
        for j in tiles:
            m = mask[pl.ds(j, 8)]
            for i in range(1, 9):
                r = f2[first + i, pl.ds(8 + j, 8)]
                s = (4.0 / 3.0) * r + relax * (around(f2, first + i, j) + sides(r, 4))
                t2[first + i, pl.ds(8 + j, 8)] = (relax * s) * m

    chunks(NX // 4, 8, sweep1)

    def sweep2(first):
        for j in last:
            m = mask[pl.ds(j, 8)]
            for i in range(1, 9):
                v = t2[first + i, pl.ds(8 + j, 8)]
                s = third(v) + relax * (f2[first + i, pl.ds(8 + j, 8)] + (around(t2, first + i, j) + sides(v, 4)))
                e2[first + i, pl.ds(8 + j, 8)] = s * m

    chunks(NX // 4, 8, sweep2)


def cycle_up(src, mask, f1, e2, v1, e1, v0, out, tiles, last):
    def correct1(first):
        for j in tiles:
            for i in range(4):
                e = e2[first + i + 1, pl.ds(8 + j, 8)]
                for half in range(2):
                    for k in (1, 2):
                        x = 2 * first + 2 * i + k
                        put1(v1, x, half, j, relax * f1[x, pl.ds(20 + 20 * half + j, 8)] + e)

    chunks(NX // 4, 4, correct1)

    def smooth1(first):
        for j in tiles:
            m = mask[pl.ds(j, 8)]
            for half in range(2):
                at = pl.ds(20 + 20 * half + j, 8)
                for i in range(1, 9):
                    x = first + i
                    v = v1[x, at]
                    y = v1[x, pl.ds(20 * half + j, 8)] + v1[x, pl.ds(40 + 20 * half + j, 8)]
                    s = third(v) + relax * ((f1[x, at] + (v1[x - 1, at] + v1[x + 1, at])) + (y + sides(v, 2)))
                    e1[x, pl.ds(20 * half + j, 8)] = s * m

    chunks(NX // 2, 8, smooth1)

    def correct0(first):
        for j in tiles:
            for i in range(1, 5):
                for half in range(2):
                    e = e1[first + i, pl.ds(20 * half + j, 8)]
                    for k in (-1, 0):
                        x = 2 * first + 2 * i + k
                        put0(v0, x, 0, half, j, relax * even(src, x, half, j) + e)
                        put0(v0, x, 1, half, j, relax * odd(src, x, half, j) + e)

    chunks(NX // 2, 4, correct0)

    def smooth0(first):
        for j in last:
            m = mask[pl.ds(j, 8)]
            for half in range(2):
                evens = [even(v0, first + k, half, j) for k in range(10)]
                odds = [odd(v0, first + k, half, j) for k in range(10)]
                for i in range(1, 9):
                    x = first + i
                    v, o = evens[i], odds[i]
                    s = third(v) + relax * ((even(src, x, half, j) + (evens[i - 1] + evens[i + 1])) + ((below(v0, x, half, j) + o) + sides(v, 1)))
                    put0(out, x, 0, half, j, s * m)
                    s = third(o) + relax * ((odd(src, x, half, j) + (odds[i - 1] + odds[i + 1])) + ((above(v0, x, half, j) + v) + sides(o, 1)))
                    put0(out, x, 1, half, j, s * m)

    chunks(NX, 8, smooth0)


def images(src, first, half, j, count):
    evens = [even(src, first + k, half, j) for k in range(count + 2)]
    odds = [odd(src, first + k, half, j) for k in range(count + 2)]
    result = []
    for i in range(1, count + 1):
        v, o = evens[i], odds[i]
        e = 6.0 * v - ((evens[i - 1] + evens[i + 1]) + ((below(src, first + i, half, j) + o) + sides(v, 1)))
        d = 6.0 * o - ((odds[i - 1] + odds[i + 1]) + ((above(src, first + i, half, j) + v) + sides(o, 1)))
        result.append((v, o, e, d))
    return result


def cycles_kernel(own, beside, rows_, up, down, out, r0, z0, q0, w, v0, f1, v1, e1, f2, t2, e2, mask):
    gx0, core, gy, gz = place()
    rows, lanes = row_index((24, LANES)), lane_index((24, LANES))
    y = gy * BY - HY + 4 * rows
    z = (gz * 4 + gx0) * CZ - HZ + lanes
    mask[...] = jnp.where((y >= 0) & (y < NY) & (z >= 0) & (z < NZ), 1.0, 0.0)
    for ref, count in ((r0, NX), (z0, NX), (q0, NX), (w, NX), (v0, NX), (f1, NX // 2), (v1, NX // 2), (f2, NX // 4), (t2, NX // 4)):
        ref[0] = jnp.zeros(ref.shape[1:], jnp.float32)
        ref[count + 1] = jnp.zeros(ref.shape[1:], jnp.float32)
    nothing = jnp.zeros((1, LANES), jnp.float32)

    def edges(i, _):
        for ref in (r0, v0):
            ref[i, 0, 59:60] = nothing
            ref[i, 1, 0:1] = nothing
        return 0

    lax.fori_loop(1, NX + 1, edges, 0, unroll=8)

    def edges1(i, _):
        for ref in (f1, v1):
            ref[i, 79:80] = nothing
            ref[i, 0:1] = nothing
        return 0

    lax.fori_loop(1, NX // 2 + 1, edges1, 0, unroll=8)

    def edges2(i, _):
        for ref in (f2, t2):
            ref[i, 7:8] = nothing
            ref[i, 28:29] = nothing
        return 0

    lax.fori_loop(1, NX // 4 + 1, edges2, 0, unroll=8)
    lanes = lane_index((8, LANES))

    def unpack():
        blocks = [(up, rows_, down, at) for at in ((0, 1), (0, 0), None, (1, 0), (1, 1))]

        def body(i, _):
            for b, (left, middle, right, which) in enumerate(blocks):
                for parity in range(2):
                    at = pl.ds(8 * parity, 8)
                    if which is None:
                        a, c, d = beside[0, i, at], own[i, at], beside[1, i, at]
                    else:
                        a, c, d = (ref[which + (i, at)] for ref in (left, middle, right))
                    for k in range(4):
                        value = jnp.where(lanes < 32, roll(a, -32 * k, 1), jnp.where(lanes < 64, roll(c, 32 - 32 * k, 1), roll(d, 64 - 32 * k, 1)))
                        x = 4 * i + k + 1
                        if parity == 0:
                            if b > 0:
                                r0[x, 0, 39 + 4 * b : 43 + 4 * b] = value[0:4]
                            else:
                                r0[x, 0, 40:43] = value[1:4]
                            r0[x, 0, 4 * b : 4 * b + 4] = value[0:4]
                            r0[x, 0, 20 + 4 * b : 24 + 4 * b] = value[4:8]
                        else:
                            if b < 4:
                                r0[x, 1, 1 + 4 * b : 5 + 4 * b] = value[4:8]
                            else:
                                r0[x, 1, 17:20] = value[4:7]
                            r0[x, 1, 20 + 4 * b : 24 + 4 * b] = value[0:4]
                            r0[x, 1, 40 + 4 * b : 44 + 4 * b] = value[4:8]
            return 0

        lax.fori_loop(0, NX // 4, body, 0)

    unpack()
    low = {step: lanes & step == 0 for step in (1, 2)}

    def fold(x, step):
        return 0.5 * (x + jnp.where(low[step], roll(x, -step, 1), roll(x, step, 1)))

    cycle_down(r0, mask, fold, f1, f2, WHOLE)
    cycle_coarse(mask, f2, t2, e2, WHOLE, WHOLE)
    cycle_up(r0, mask, f1, e2, v1, e1, v0, z0, WHOLE, MIDDLE)

    def image(first):
        for j in MIDDLE:
            m = mask[pl.ds(j, 8)]
            for half in range(2):
                for i, (_, _, e, d) in enumerate(images(z0, first, half, j, 8)):
                    put0(q0, first + i + 1, 0, half, j, e * m)
                    put0(q0, first + i + 1, 1, half, j, d * m)

    chunks(NX, 8, image)
    cycle_down(q0, mask, fold, f1, f2, MIDDLE)
    cycle_coarse(mask, f2, t2, e2, MIDDLE, HOME)
    cycle_up(q0, mask, f1, e2, v1, e1, v0, w, HOME, HOME)

    inside = (lanes >= HZ) & (lanes < HZ + CZ) & (row_index((8, LANES)) < 4)

    def sums(i, acc):
        acc = list(acc)
        for half in range(2):
            for k, (we, wo, se, so) in enumerate(images(w, 8 * i, half, 8, 8)):
                x = 8 * i + k + 1
                for get, ww, s in ((even, we, se), (odd, wo, so)):
                    r, zz, q = get(r0, x, half, 8), get(z0, x, half, 8), get(q0, x, half, 8)
                    for n, term in enumerate((r * zz, zz * q, r * ww, q * ww, ww * s)):
                        acc[n] = acc[n] + term
                at = 20 * half + 8
                v0[x, 0, pl.ds(at, 8)] = se
                v0[x, 1, pl.ds(20 + at, 8)] = so
        return tuple(acc)

    acc = lax.fori_loop(0, NX // 8, sums, (jnp.zeros((8, LANES), jnp.float32),) * 5)

    def send(t, _):
        for k in range(BX):
            x = BX * (2 * t + core) + k + 1
            for at in range(4):
                parity, half = at // 2, at % 2
                rows = pl.ds(20 * parity + 20 * half + 8, 4)
                zz, q, ww, s = (ref[x, parity, rows] for ref in (z0, q0, w, v0))
                wide = lanes[0:4]
                out[t, pl.ds(k * BY + 4 * at, 4)] = jnp.where(
                    wide < 32, roll(zz, -32, 1), jnp.where(wide < 64, q, jnp.where(wide < 96, roll(ww, 32, 1), roll(s, 64, 1)))
                )
        return 0

    lax.fori_loop(0, 4, send, 0)
    row = jnp.zeros((8, LANES), jnp.float32)
    for k, a in enumerate(acc):
        row = jnp.where(lanes == k, jnp.sum(jnp.where(inside, a, 0.0)), row)
    for t in range(4):
        out[t, BX * BY : BX * BY + 8] = row


def cycles(*blocks):
    fine = pltpu.VMEM((NX + 2, 2, 64, LANES), jnp.float32)
    level1 = pltpu.VMEM((NX // 2 + 2, 80, LANES), jnp.float32)
    level2 = pltpu.VMEM((NX // 4 + 2, 40, LANES), jnp.float32)
    return pl.pallas_call(
        cycles_kernel,
        out_shape=jax.ShapeDtypeStruct((4, BX * BY + 8, LANES), jnp.float32),
        in_specs=[VMEM] * 5,
        out_specs=VMEM,
        scratch_shapes=[fine] * 5 + [level1, level1, pltpu.VMEM((NX // 2 + 2, 40, LANES), jnp.float32)] + [level2] * 3 + [pltpu.VMEM((24, LANES), jnp.float32)],
        compiler_params=pltpu.CompilerParams(vmem_limit_bytes=30 * 1024 * 1024),
    )(*blocks)


def finish_kernel(rhs, fields, sums, solution, residual):
    total = jnp.sum(sums[...], axis=0, keepdims=True)
    lanes = lane_index(total.shape)

    def pick(k):
        return jnp.sum(jnp.where(lanes == k, total, 0.0), axis=1, keepdims=True)

    rz, zq, rw, qw, ws = (pick(k) for k in range(5))
    step0 = rz / zq
    rz1 = rz - step0 * (rw + zq) + step0 * step0 * qw
    growth = rz1 / rz
    image1 = (zq - 2.0 * step0 * qw + step0 * step0 * ws) + 2.0 * growth * (zq - step0 * qw) + growth * growth * zq
    step1 = rz1 / image1
    on_z = step0 + step1 * (1.0 + growth)
    on_w = -step1 * step0
    wide = lane_index((BY, LANES))
    for x in range(BX):
        parts = [fields[c, x * BY : (x + 1) * BY] for c in range(4)]

        def field(f):
            value = None
            for c in range(4):
                part = roll(parts[c], 32 * (c - f), 1)
                value = part if c == 0 else jnp.where(wide >= 32 * c, part, value)
            return value

        z0, q0, w, s = (field(f) for f in range(4))
        u = on_z * z0 + on_w * w
        v = on_z * q0 + on_w * s
        for at, plane in enumerate(PLANES):
            rows = pl.ds(plane, 4, stride=4)
            solution[x, rows, :] = u[4 * at : 4 * at + 4]
            residual[x, rows, :] = rhs[x, rows, :] - v[4 * at : 4 * at + 4]


def finish(rhs, fields, sums):
    shape = jax.ShapeDtypeStruct((BX, BY, BZ), jnp.float32)
    return pl.pallas_call(finish_kernel, out_shape=(shape, shape), in_specs=[VMEM] * 3, out_specs=(VMEM, VMEM), compiler_params=small())(rhs, fields, sums)


def both_ways(count, step):
    pairs = [(i, i + step) for i in range(count - step)]
    return pairs + [(count + b, count + a) for a, b in pairs]


def z_pairs(steps):
    def number(core, block):
        return ((block % 4) * 2 + core) * 8 + block // 4

    return [(number(core, a), number(core, a + step)) for core, step in enumerate(steps) for a in range(32) if 0 <= a + step < 32]


Z_AXES = ("gx_0", "gx_1", "gz")


def local(density, x_faces, y_faces, z_faces):
    rhs, packed = make_rhs(density, x_faces, y_faces, z_faces)
    own = lax.all_to_all(packed, GX, 0, 0, tiled=True).reshape(16, BY, 128)
    near = lax.ppermute(own, ("gx_1", "gy"), both_ways(16, 1))
    far = lax.ppermute(own, ("gx_1", "gy"), both_ways(16, 2))
    side = lax.ppermute(own, Z_AXES, z_pairs((1, -1)))
    rows = jnp.stack([near, far])
    up = lax.ppermute(rows, Z_AXES, z_pairs((1, 1)))
    down = lax.ppermute(rows, Z_AXES, z_pairs((-1, -1)))
    packed = cycles(own, *(lax.all_gather(each, "gx_1") for each in (side, rows, up, down)))
    fields = lax.all_to_all(packed, "gx_0", 0, 0, tiled=True)
    sums = jnp.sum(fields[:, BX * BY, :], axis=0)
    sums = lax.all_to_all(jnp.broadcast_to(sums, (128, 1, 128)), ("gy", "gz"), 0, 0, tiled=True)
    return finish(rhs, fields, sums.reshape(128, 128))


def solution(mesh):
    torus = Mesh(mesh.devices.reshape(4, 2, mesh.shape["gy"], mesh.shape["gz"]), AXES)
    in_specs = (P(GX, "gy", "gz"), P(None, "gy", "gz"), P(None, GX, "gz"), P(None, GX, "gy"))
    out_specs = (P(GX, "gy", "gz"), P(GX, "gy", "gz"))
    return jax.shard_map(local, mesh=torus, in_specs=in_specs, out_specs=out_specs, check_vma=False)
```

```python
import functools

import jax
import jax.numpy as jnp
from jax import lax
from jax.experimental import pallas as pl
from jax.experimental.pallas import tpu as pltpu
from jax.sharding import Mesh
from jax.sharding import PartitionSpec as P

AXES = ("gx_0", "gx_1", "gy", "gz")
GX = ("gx_0", "gx_1")
NX, NY, NZ = 64, 256, 1024
BX, BY, BZ = 8, 16, 128
CZ = 32
HY, HZ = 32, 32
ROWS, LANES = BY + 2 * HY, 128
relax = 1.0 / 9.0
coupling = 0.5
VMEM = pl.BlockSpec(memory_space=pltpu.VMEM)
HBM = pl.BlockSpec(memory_space=pltpu.MemorySpace.HBM)


def roll(x, shift, axis):
    return pltpu.roll(x, shift % x.shape[axis], axis)


def place():
    return tuple(lax.axis_index(axis) for axis in AXES)


def small(**more):
    return pltpu.CompilerParams(vmem_limit_bytes=4 * 1024 * 1024, **more)


def lane_index(shape):
    return lax.broadcasted_iota(jnp.int32, shape, 1)


def row_index(shape):
    return lax.broadcasted_iota(jnp.int32, shape, 0)


def rhs_kernel(density_in, xf_in, yf_in, zf_in, rhs, packed, scratch, density, xf, yf, zf, arrived):
    copies = [pltpu.make_async_copy(a, b, arrived.at[i]) for i, (a, b) in enumerate(((density_in, density), (xf_in, xf), (yf_in, yf), (zf_in, zf)))]
    for copy in copies:
        copy.start()
    gx0, core, gy, gz = place()
    gx = 2 * gx0 + core
    rows, lanes = row_index((BY, BZ)), lane_index((BY, BZ))
    eye = row_index((BY, BY)) == lane_index((BY, BY))
    low_y = (rows == 0) & (gy == 0)
    high_y = (rows == BY - 1) & (gy == NY // BY - 1)
    low_z = (lanes == 0) & (gz == 0)
    high_z = (lanes == BZ - 1) & (gz == NZ // BZ - 1)

    def column(row):
        return jnp.sum(jnp.where(eye, row, 0.0), axis=1, keepdims=True)

    for copy in copies:
        copy.wait()
    layers = []
    for x in range(BX):
        value = -coupling * density[x]
        if x == 0:
            value = value + jnp.where(gx == 0, xf[0], 0.0)
        if x == BX - 1:
            value = value + jnp.where(gx == NX // BX - 1, xf[1], 0.0)
        value = value + jnp.where(low_y, yf[0, x : x + 1, :], 0.0)
        value = value + jnp.where(high_y, yf[1, x : x + 1, :], 0.0)
        value = value + jnp.where(low_z, column(zf[0, x : x + 1, :]), 0.0)
        value = value + jnp.where(high_z, column(zf[1, x : x + 1, :]), 0.0)
        rhs[x] = value
        layers.append(value)
    for chunk in range(4):
        for quad in range(2):
            out = None
            for k in range(4):
                part = roll(layers[4 * quad + k], 32 * (k - chunk), 1)
                out = part if k == 0 else jnp.where(lanes >= 32 * k, part, out)
            scratch[chunk, quad] = out
    for chunk in range(4):
        for quad in range(2):
            for odd in range(2):
                part = scratch[chunk, quad, pl.ds(odd, 8, stride=2), :]
                packed[2 * chunk, quad, 8 * odd : 8 * odd + 8] = part
                packed[2 * chunk + 1, quad, 8 * odd : 8 * odd + 8] = part


def make_rhs(density, xf, yf, zf):
    return pl.pallas_call(
        rhs_kernel,
        out_shape=(
            jax.ShapeDtypeStruct((BX, BY, BZ), jnp.float32),
            jax.ShapeDtypeStruct((8, 2, BY, BZ), jnp.float32),
        ),
        in_specs=[HBM] * 4,
        out_specs=(VMEM, VMEM),
        scratch_shapes=[pltpu.VMEM((4, 2, BY, BZ), jnp.float32)]
        + [pltpu.VMEM(a.shape, a.dtype) for a in (density, xf, yf, zf)]
        + [pltpu.SemaphoreType.DMA((4,))],
        compiler_params=pltpu.CompilerParams(vmem_limit_bytes=60 * 1024 * 1024),
    )(density, xf, yf, zf)


def at(row, step=0):
    return pl.ds(8 + row + step, 8)


def every_other(row, step=0):
    return pl.ds(8 + 2 * row + step, 8, stride=2)


def sides(x, step):
    return roll(x, step, 1) + roll(x, -step, 1)


def third(x):
    return x * (1.0 / 3.0)


def chunks(count, size, body):
    size, unroll = size if isinstance(size, tuple) else (size, 1)
    if size == count:
        body(0)
    elif size * unroll == count:
        for i in range(unroll):
            body(i * size)
    else:
        lax.fori_loop(0, count // size, lambda i, _: body(i * size) or 0, 0, unroll=unroll)


def cycle_down(src, mask, mask2, fold, sum1, part1, f1, f2, rows1, rows2, size, nb):
    def gather(first, size=size):
        for r in rows1:
            layers = [2 * first + k for k in range(2 * size + 2)]
            cells = [src[x, 0, at(r)] + src[x, 1, at(r)] for x in layers]
            beyond = [src[x, 1, at(r, -1)] + src[x, 0, at(r, 1)] for x in layers[1:-1]]
            for i in range(size):
                before, a, b, after = cells[2 * i : 2 * i + 4]
                u = a + b
                y = beyond[2 * i] + beyond[2 * i + 1]
                sum1[first + i + 1, at(r)] = u
                part1[first + i + 1, at(r)] = third(u) + relax * (((u + u) + (before + after)) + y)

    chunks(NX // 2, size, gather)

    def across(first):
        for r in rows1:
            for x in [first + k for k in range(1, 32 + 1)]:
                f1[x, at(r)] = part1[x, at(r)] + relax * sides(sum1[x, at(r)], 1)

    chunks(NX // 2, 32, across)

    def level1(first):
        for r in rows1:
            m = mask[at(r)]
            for x in [first + k for k in range(1, 16 + 1)]:
                f1[x, at(r)] = fold(f1[x, at(r)], 1) * m

    chunks(NX // 2, 16, level1)

    def level2(first):
        for r in rows2:
            m = mask2[at(r)]
            layers = [2 * first + k for k in range(2 * nb + 2)]
            cells = [f1[x, every_other(r), :] + f1[x, every_other(r, 1), :] for x in layers]
            beyond = [f1[x, every_other(r, -1), :] + f1[x, every_other(r, 2), :] for x in layers[1:-1]]
            for i in range(nb):
                before, a, b, after = cells[2 * i : 2 * i + 4]
                u = a + b
                y = beyond[2 * i] + beyond[2 * i + 1]
                s = third(u) + relax * (((u + u) + (before + after)) + (y + sides(u, 2)))
                f2[first + i + 1, at(r)] = fold(s, 2) * m

    chunks(NX // 4, nb, level2)


def cycle_coarse(mask2, f2, t2, e2, rows, last):
    def around(ref, x, r):
        return (ref[x - 1, at(r)] + ref[x + 1, at(r)]) + (ref[x, at(r, -1)] + ref[x, at(r, 1)])

    def sweep1(first):
        for r in rows:
            m = mask2[at(r)]
            for x in range(1, 9):
                v = f2[first + x, at(r)]
                s = (4.0 / 3.0) * v + relax * (around(f2, first + x, r) + sides(v, 4))
                t2[first + x, at(r)] = (relax * s) * m

    chunks(NX // 4, 8, sweep1)

    def sweep2(first):
        for r in last:
            m = mask2[at(r)]
            for x in range(1, 9):
                v = t2[first + x, at(r)]
                s = (third(v) + relax * (f2[first + x, at(r)] + (around(t2, first + x, r) + sides(v, 4)))) * m
                e2[first + x, every_other(r), :] = s
                e2[first + x, every_other(r, 1), :] = s

    chunks(NX // 4, 8, sweep2)


def cycle_up(src, mask, f1, e2, v1, e1, v0, out, rows1, last1, rows0, last0, nd, ne):
    def correct1(first):
        for r in rows1:
            for i in range(4):
                e = e2[first + i + 1, at(r)]
                for k in (1, 2):
                    x = 2 * first + 2 * i + k
                    v1[x, at(r)] = relax * f1[x, at(r)] + e

    chunks(NX // 4, 4, correct1)

    def smooth1(first):
        for r in last1:
            m = mask[at(r)]
            for x in [first + k for k in range(1, nd + 1)]:
                v = v1[x, at(r)]
                y = v1[x, at(r, -1)] + v1[x, at(r, 1)]
                s = third(v) + relax * ((f1[x, at(r)] + (v1[x - 1, at(r)] + v1[x + 1, at(r)])) + (y + sides(v, 2)))
                e1[x, at(r)] = s * m

    chunks(NX // 2, nd, smooth1)

    def correct0(first):
        for odd in range(2):
            for r in rows0[odd]:
                for i in range(1, 5):
                    e = e1[first + i, at(r)]
                    for k in (-1, 0):
                        x = 2 * first + 2 * i + k
                        v0[x, odd, at(r)] = relax * src[x, odd, at(r)] + e

    chunks(NX // 2, 4, correct0)

    def smooth0(first):
        for odd in range(2):
            for r in last0[odd]:
                m = mask[at(r)]
                layers = [v0[first + k, odd, at(r)] for k in range(ne + 2)]
                for k in range(1, ne + 1):
                    x = first + k
                    v = layers[k]
                    y = v0[x, 1 - odd, at(r, odd - 1)] + v0[x, 1 - odd, at(r, odd)]
                    s = third(v) + relax * ((src[x, odd, at(r)] + (layers[k - 1] + layers[k + 1])) + (y + sides(v, 1)))
                    out[x, odd, at(r)] = s * m

    chunks(NX, ne, smooth0)


def images(src, first, odd, r, count):
    layers = [src[first + k, odd, at(r)] for k in range(count + 2)]
    result = []
    for k in range(1, count + 1):
        v = layers[k]
        y = src[first + k, 1 - odd, at(r, odd - 1)] + src[first + k, 1 - odd, at(r, odd)]
        result.append((v, 6.0 * v - ((layers[k - 1] + layers[k + 1]) + (y + sides(v, 1)))))
    return result


def cycles_kernel(own, beside, rows_, up, down, out, r0, z0, q0, w, v0, f1, v1, e1, e2, f2, t2, mask, mask2):
    gx0, core, gy, gz = place()

    def inside(count, height):
        rows, lanes = row_index((count, LANES)) - 8, lane_index((count, LANES))
        y = gy * BY - HY + height * rows
        z = (gz * 4 + gx0) * CZ - HZ + lanes
        return jnp.where((y >= 0) & (y < NY) & (z >= 0) & (z < NZ), 1.0, 0.0)

    mask[...] = inside(56, 2)
    mask2[...] = inside(40, 4)
    for ref, count in ((r0, NX), (z0, NX), (q0, NX), (w, NX), (v0, NX), (f1, NX // 2), (v1, NX // 2), (f2, NX // 4), (t2, NX // 4)):
        ref[0] = jnp.zeros(ref.shape[1:], jnp.float32)
        ref[count + 1] = jnp.zeros(ref.shape[1:], jnp.float32)
    lanes = lane_index((8, LANES))
    blocks = [(up, rows_, down, which) for which in ((0, 1), (0, 0), None, (1, 0), (1, 1))]

    def unpack(i, _):
        for b, (left, middle, right, which) in enumerate(blocks):
            for odd in range(2):
                part = pl.ds(8 * odd, 8)
                if which is None:
                    a, c, d = beside[0, i, part], own[i, part], beside[1, i, part]
                else:
                    a, c, d = (ref[which + (i, part)] for ref in (left, middle, right))
                for k in range(4):
                    value = jnp.where(lanes < 32, roll(a, -32 * k, 1), jnp.where(lanes < 64, roll(c, 32 - 32 * k, 1), roll(d, 64 - 32 * k, 1)))
                    r0[4 * i + k + 1, odd, at(8 * b)] = value
        return 0

    lax.fori_loop(0, NX // 4, unpack, 0, unroll=16)
    low = {step: lanes & step == 0 for step in (1, 2)}

    def fold(x, step):
        return 0.5 * (x + jnp.where(low[step], roll(x, -step, 1), roll(x, step, 1)))

    middle = (8, 16, 24)
    cycle_down(r0, mask, mask2, fold, v1, e1, f1, f2, (0, 8, 16, 24, 32), (0, 8, 12), 4, 8)
    cycle_coarse(mask2, f2, t2, e2, (0, 8, 12), (1, 9))
    cycle_up(r0, mask, f1, e2, v1, e1, v0, z0, (6, 14, 22, 26), (7, 15, 23, 25), ((8, 16, 24, 25), (7, 15, 23, 24)), (middle, middle), 32, 64)

    def image(first):
        for odd in range(2):
            for r in middle:
                m = mask[at(r)]
                for k, (_, value) in enumerate(images(z0, first, odd, r, 64)):
                    q0[first + k + 1, odd, at(r)] = value * m

    chunks(NX, 64, image)
    cycle_down(q0, mask, mask2, fold, v1, e1, f1, f2, middle, (5, 7), 8, 16)
    cycle_coarse(mask2, f2, t2, e2, (6,), (6,))
    cycle_up(q0, mask, f1, e2, v1, e1, v0, w, (14, 18), (15, 17), ((15, 17), (15, 17)), ((16, 17), (15, 16)), 32, 64)

    def sums(i, acc):
        acc = list(acc)
        for odd in range(2):
            for k, (ww, s) in enumerate(images(w, 64 * i, odd, 16, 64)):
                x = 64 * i + k + 1
                r, zz, q = r0[x, odd, at(16)], z0[x, odd, at(16)], q0[x, odd, at(16)]
                for n, term in enumerate((r * zz, zz * q, r * ww, q * ww, ww * s)):
                    acc[n] = acc[n] + term
                v0[x, odd, at(16)] = s
        return tuple(acc)

    acc = lax.fori_loop(0, NX // 64, sums, (jnp.zeros((8, LANES), jnp.float32),) * 5)

    def send(t, _):
        for k in range(BX):
            x = BX * (2 * t + core) + k + 1
            for odd in range(2):
                zz, q, ww, s = (ref[x, odd, at(16)] for ref in (z0, q0, w, v0))
                out[t, pl.ds(k * BY + 8 * odd, 8)] = jnp.where(
                    lanes < 32, roll(zz, -32, 1), jnp.where(lanes < 64, q, jnp.where(lanes < 96, roll(ww, 32, 1), roll(s, 64, 1)))
                )
        return 0

    lax.fori_loop(0, 4, send, 0, unroll=4)
    home = (lanes >= HZ) & (lanes < HZ + CZ)
    row = jnp.zeros((8, LANES), jnp.float32)
    for k, a in enumerate(acc):
        row = jnp.where(lanes == k, jnp.sum(jnp.where(home, a, 0.0)), row)
    for t in range(4):
        out[t, BX * BY : BX * BY + 8] = row


def cycles(*blocks):
    fine = pltpu.VMEM((NX + 2, 2, 56, LANES), jnp.float32)
    level1 = pltpu.VMEM((NX // 2 + 2, 56, LANES), jnp.float32)
    level2 = pltpu.VMEM((NX // 4 + 2, 40, LANES), jnp.float32)
    return pl.pallas_call(
        cycles_kernel,
        out_shape=jax.ShapeDtypeStruct((4, BX * BY + 8, LANES), jnp.float32),
        in_specs=[VMEM] * 5,
        out_specs=VMEM,
        scratch_shapes=[fine] * 5
        + [level1] * 3
        + [pltpu.VMEM((NX // 4 + 2, 56, LANES), jnp.float32), level2, level2, pltpu.VMEM((56, LANES), jnp.float32), pltpu.VMEM((40, LANES), jnp.float32)],
        compiler_params=pltpu.CompilerParams(vmem_limit_bytes=30 * 1024 * 1024),
    )(*blocks)


def finish_kernel(rhs, fields, sums, solution, residual):
    total = jnp.sum(sums[...], axis=0, keepdims=True)
    lanes = lane_index(total.shape)

    def pick(k):
        return jnp.sum(jnp.where(lanes == k, total, 0.0), axis=1, keepdims=True)

    rz, zq, rw, qw, ws = (pick(k) for k in range(5))
    step0 = rz / zq
    rz1 = rz - step0 * (rw + zq) + step0 * step0 * qw
    growth = rz1 / rz
    image1 = (zq - 2.0 * step0 * qw + step0 * step0 * ws) + 2.0 * growth * (zq - step0 * qw) + growth * growth * zq
    step1 = rz1 / image1
    on_z = step0 + step1 * (1.0 + growth)
    on_w = -step1 * step0
    wide = lane_index((BY, LANES))
    for x in range(BX):
        parts = [fields[c, x * BY : (x + 1) * BY] for c in range(4)]

        def field(f):
            value = None
            for c in range(4):
                part = roll(parts[c], 32 * (c - f), 1)
                value = part if c == 0 else jnp.where(wide >= 32 * c, part, value)
            return value

        z0, q0, w, s = (field(f) for f in range(4))
        u = on_z * z0 + on_w * w
        v = on_z * q0 + on_w * s
        for odd in range(2):
            rows = pl.ds(odd, 8, stride=2)
            solution[x, rows, :] = u[8 * odd : 8 * odd + 8]
            residual[x, rows, :] = rhs[x, rows, :] - v[8 * odd : 8 * odd + 8]


def finish(rhs, fields, sums):
    shape = jax.ShapeDtypeStruct((BX, BY, BZ), jnp.float32)
    return pl.pallas_call(finish_kernel, out_shape=(shape, shape), in_specs=[VMEM] * 3, out_specs=(VMEM, VMEM), compiler_params=small())(rhs, fields, sums)


def both_ways(count, step):
    pairs = [(i, i + step) for i in range(count - step)]
    return pairs + [(count + b, count + a) for a, b in pairs]


def z_pairs(steps):
    def number(core, block):
        return ((block % 4) * 2 + core) * 8 + block // 4

    return [(number(core, a), number(core, a + step)) for core, step in enumerate(steps) for a in range(32) if 0 <= a + step < 32]


Z_AXES = ("gx_0", "gx_1", "gz")


def local(density, x_faces, y_faces, z_faces):
    rhs, packed = make_rhs(density, x_faces, y_faces, z_faces)
    own = lax.all_to_all(packed, GX, 0, 0, tiled=True).reshape(16, BY, 128)
    near = lax.ppermute(own, ("gx_1", "gy"), both_ways(16, 1))
    far = lax.ppermute(own, ("gx_1", "gy"), both_ways(16, 2))
    side = lax.ppermute(own, Z_AXES, z_pairs((1, -1)))
    rows = jnp.stack([near, far])
    up = lax.ppermute(rows, Z_AXES, z_pairs((1, 1)))
    down = lax.ppermute(rows, Z_AXES, z_pairs((-1, -1)))
    packed = cycles(own, *(lax.all_gather(each, "gx_1") for each in (side, rows, up, down)))
    fields = lax.all_to_all(packed, "gx_0", 0, 0, tiled=True)
    sums = jnp.sum(fields[:, BX * BY, :], axis=0)
    sums = lax.all_to_all(jnp.broadcast_to(sums, (128, 1, 128)), ("gy", "gz"), 0, 0, tiled=True)
    return finish(rhs, fields, sums.reshape(128, 128))


def solution(mesh):
    torus = Mesh(mesh.devices.reshape(4, 2, mesh.shape["gy"], mesh.shape["gz"]), AXES)
    in_specs = (P(GX, "gy", "gz"), P(None, "gy", "gz"), P(None, GX, "gz"), P(None, GX, "gy"))
    out_specs = (P(GX, "gy", "gz"), P(GX, "gy", "gz"))
    return jax.shard_map(local, mesh=torus, in_specs=in_specs, out_specs=out_specs, check_vma=False)
```

```python
import jax
import jax.numpy as jnp
from jax import lax
from jax.experimental import pallas as pl
from jax.experimental.pallas import tpu as pltpu
from jax.sharding import Mesh
from jax.sharding import PartitionSpec as P


AXES = ("gx_0", "gx_1", "gy", "gz")
GX = ("gx_0", "gx_1")
NX, NY, NZ = 64, 256, 1024
BX, BY, BZ = 8, 16, 128
CZ = 32
HY, HZ = 32, 32
LANES = 128
relax = 1.0 / 9.0
coupling = 0.5
VMEM = pl.BlockSpec(memory_space=pltpu.VMEM)
HBM = pl.BlockSpec(memory_space=pltpu.MemorySpace.HBM)


def roll(x, shift, axis):
    return pltpu.roll(x, shift % x.shape[axis], axis)


def place():
    return tuple(lax.axis_index(axis) for axis in AXES)


def z_block(gx0, gz):
    return jnp.where(gz % 2 == 0, gx0, 3 - gx0)


def small(**more):
    return pltpu.CompilerParams(vmem_limit_bytes=4 * 1024 * 1024, **more)


def lane_index(shape):
    return lax.broadcasted_iota(jnp.int32, shape, 1)


def row_index(shape):
    return lax.broadcasted_iota(jnp.int32, shape, 0)


def rhs_kernel(density_in, xf_in, yf_in, zf_in, rhs, packed, scratch, density, xf, yf, zf, arrived):
    copies = [pltpu.make_async_copy(a, b, arrived.at[i]) for i, (a, b) in enumerate(((density_in, density), (xf_in, xf), (yf_in, yf), (zf_in, zf)))]
    for copy in copies:
        copy.start()
    gx0, core, gy, gz = place()
    gx = 2 * gx0 + core
    rows, lanes = row_index((BY, BZ)), lane_index((BY, BZ))
    eye = row_index((BY, BY)) == lane_index((BY, BY))
    low_y = (rows == 0) & (gy == 0)
    high_y = (rows == BY - 1) & (gy == NY // BY - 1)
    low_z = (lanes == 0) & (gz == 0)
    high_z = (lanes == BZ - 1) & (gz == NZ // BZ - 1)

    def column(row):
        return jnp.sum(jnp.where(eye, row, 0.0), axis=1, keepdims=True)

    for copy in copies:
        copy.wait()
    layers = []
    for x in range(BX):
        value = -coupling * density[x]
        if x == 0:
            value = value + jnp.where(gx == 0, xf[0], 0.0)
        if x == BX - 1:
            value = value + jnp.where(gx == NX // BX - 1, xf[1], 0.0)
        value = value + jnp.where(low_y, yf[0, x : x + 1, :], 0.0)
        value = value + jnp.where(high_y, yf[1, x : x + 1, :], 0.0)
        value = value + jnp.where(low_z, column(zf[0, x : x + 1, :]), 0.0)
        value = value + jnp.where(high_z, column(zf[1, x : x + 1, :]), 0.0)
        rhs[x] = value
        layers.append(value)
    for chunk in range(4):
        for quad in range(2):
            out = None
            for k in range(4):
                part = roll(layers[4 * quad + k], 32 * (k - chunk), 1)
                out = part if k == 0 else jnp.where(lanes >= 32 * k, part, out)
            scratch[chunk, quad] = out
    for chip in range(4):
        chunk = z_block(chip, gz)
        for quad in range(2):
            for odd in range(2):
                part = scratch[chunk, quad, pl.ds(odd, 8, stride=2), :]
                packed[2 * chip, quad, 8 * odd : 8 * odd + 8] = part
                packed[2 * chip + 1, quad, 8 * odd : 8 * odd + 8] = part


def make_rhs(density, xf, yf, zf):
    return pl.pallas_call(
        rhs_kernel,
        out_shape=(
            jax.ShapeDtypeStruct((BX, BY, BZ), jnp.float32),
            jax.ShapeDtypeStruct((8, 2, BY, BZ), jnp.float32),
        ),
        in_specs=[HBM] * 4,
        out_specs=(VMEM, VMEM),
        scratch_shapes=[pltpu.VMEM((4, 2, BY, BZ), jnp.float32)]
        + [pltpu.VMEM(a.shape, a.dtype) for a in (density, xf, yf, zf)]
        + [pltpu.SemaphoreType.DMA((4,))],
        compiler_params=pltpu.CompilerParams(vmem_limit_bytes=60 * 1024 * 1024),
    )(density, xf, yf, zf)


def join_kernel(*refs):
    out = refs[-1]
    for b, ref in enumerate(refs[:-1]):
        for i in range(16):
            out[i, BY * b : BY * b + BY] = ref[i]


def join(*blocks):
    return pl.pallas_call(
        join_kernel,
        out_shape=jax.ShapeDtypeStruct((16, 4 * BY, 128), jnp.float32),
        in_specs=[VMEM] * 4,
        out_specs=VMEM,
        compiler_params=small(),
    )(*blocks)


def at(row, step=0):
    return pl.ds(8 + row + step, 8)


def every_other(row, step=0):
    return pl.ds(8 + 2 * row + step, 8, stride=2)


def sides(x, step):
    return roll(x, step, 1) + roll(x, -step, 1)


def third(x):
    return x * (1.0 / 3.0)


def chunks(count, size, body):
    size, unroll = size if isinstance(size, tuple) else (size, 1)
    if size == count:
        body(0)
    elif size * unroll == count:
        for i in range(unroll):
            body(i * size)
    else:
        lax.fori_loop(0, count // size, lambda i, _: body(i * size) or 0, 0, unroll=unroll)


def cycle_down(src, mask, mask2, fold, sum1, part1, f1, f2, rows1, rows2, size, nb):
    def gather(first, size=size):
        for r in rows1:
            layers = [2 * first + k for k in range(2 * size + 2)]
            cells = [src[x, 0, at(r)] + src[x, 1, at(r)] for x in layers]
            beyond = [src[x, 1, at(r, -1)] + src[x, 0, at(r, 1)] for x in layers[1:-1]]
            for i in range(size):
                before, a, b, after = cells[2 * i : 2 * i + 4]
                u = a + b
                y = beyond[2 * i] + beyond[2 * i + 1]
                sum1[first + i + 1, at(r)] = u
                part1[first + i + 1, at(r)] = third(u) + relax * (((u + u) + (before + after)) + y)

    chunks(NX // 2, size, gather)

    def across(first):
        for r in rows1:
            for x in [first + k for k in range(1, 32 + 1)]:
                f1[x, at(r)] = part1[x, at(r)] + relax * sides(sum1[x, at(r)], 1)

    chunks(NX // 2, 32, across)

    def level1(first):
        for r in rows1:
            m = mask[at(r)]
            for x in [first + k for k in range(1, 16 + 1)]:
                f1[x, at(r)] = fold(f1[x, at(r)], 1) * m

    chunks(NX // 2, 16, level1)

    def level2(first):
        for r in rows2:
            m = mask2[at(r)]
            layers = [2 * first + k for k in range(2 * nb + 2)]
            cells = [f1[x, every_other(r), :] + f1[x, every_other(r, 1), :] for x in layers]
            beyond = [f1[x, every_other(r, -1), :] + f1[x, every_other(r, 2), :] for x in layers[1:-1]]
            for i in range(nb):
                before, a, b, after = cells[2 * i : 2 * i + 4]
                u = a + b
                y = beyond[2 * i] + beyond[2 * i + 1]
                s = third(u) + relax * (((u + u) + (before + after)) + (y + sides(u, 2)))
                f2[first + i + 1, at(r)] = fold(s, 2) * m

    chunks(NX // 4, nb, level2)


def cycle_coarse(mask2, f2, t2, e2, rows, last):
    def around(ref, x, r):
        return (ref[x - 1, at(r)] + ref[x + 1, at(r)]) + (ref[x, at(r, -1)] + ref[x, at(r, 1)])

    def sweep1(first):
        for r in rows:
            m = mask2[at(r)]
            for x in range(1, 9):
                v = f2[first + x, at(r)]
                s = (4.0 / 3.0) * v + relax * (around(f2, first + x, r) + sides(v, 4))
                t2[first + x, at(r)] = (relax * s) * m

    chunks(NX // 4, 8, sweep1)

    def sweep2(first):
        for r in last:
            m = mask2[at(r)]
            for x in range(1, 9):
                v = t2[first + x, at(r)]
                s = (third(v) + relax * (f2[first + x, at(r)] + (around(t2, first + x, r) + sides(v, 4)))) * m
                e2[first + x, every_other(r), :] = s
                e2[first + x, every_other(r, 1), :] = s

    chunks(NX // 4, 8, sweep2)


def cycle_up(src, mask, f1, e2, v1, e1, v0, out, rows1, last1, rows0, last0, nd, ne):
    def correct1(first):
        for r in rows1:
            for i in range(4):
                e = e2[first + i + 1, at(r)]
                for k in (1, 2):
                    x = 2 * first + 2 * i + k
                    v1[x, at(r)] = relax * f1[x, at(r)] + e

    chunks(NX // 4, 4, correct1)

    def smooth1(first):
        for r in last1:
            m = mask[at(r)]
            for x in [first + k for k in range(1, nd + 1)]:
                v = v1[x, at(r)]
                y = v1[x, at(r, -1)] + v1[x, at(r, 1)]
                s = third(v) + relax * ((f1[x, at(r)] + (v1[x - 1, at(r)] + v1[x + 1, at(r)])) + (y + sides(v, 2)))
                e1[x, at(r)] = s * m

    chunks(NX // 2, nd, smooth1)

    def correct0(first):
        for odd in range(2):
            for r in rows0[odd]:
                for i in range(1, 5):
                    e = e1[first + i, at(r)]
                    for k in (-1, 0):
                        x = 2 * first + 2 * i + k
                        v0[x, odd, at(r)] = relax * src[x, odd, at(r)] + e

    chunks(NX // 2, 4, correct0)

    def smooth0(first):
        for odd in range(2):
            for r in last0[odd]:
                m = mask[at(r)]
                layers = [v0[first + k, odd, at(r)] for k in range(ne + 2)]
                for k in range(1, ne + 1):
                    x = first + k
                    v = layers[k]
                    y = v0[x, 1 - odd, at(r, odd - 1)] + v0[x, 1 - odd, at(r, odd)]
                    s = third(v) + relax * ((src[x, odd, at(r)] + (layers[k - 1] + layers[k + 1])) + (y + sides(v, 1)))
                    out[x, odd, at(r)] = s * m

    chunks(NX, ne, smooth0)


def images(src, first, odd, r, count):
    layers = [src[first + k, odd, at(r)] for k in range(count + 2)]
    result = []
    for k in range(1, count + 1):
        v = layers[k]
        y = src[first + k, 1 - odd, at(r, odd - 1)] + src[first + k, 1 - odd, at(r, odd)]
        result.append((v, 6.0 * v - ((layers[k - 1] + layers[k + 1]) + (y + sides(v, 1)))))
    return result


def cycles_kernel(own, left, right, rows_, up, down, out, other, r0, z0, q0, w, v0, f1, v1, e1, e2, f2, t2, mask, mask2):
    gx0, _, gy, gz = place()

    def inside(count, height):
        rows, lanes = row_index((count, LANES)) - 8, lane_index((count, LANES))
        y = gy * BY - HY + height * rows
        z = (gz * 4 + z_block(gx0, gz)) * CZ - HZ + lanes
        return jnp.where((y >= 0) & (y < NY) & (z >= 0) & (z < NZ), 1.0, 0.0)

    mask[...] = inside(56, 2)
    mask2[...] = inside(40, 4)
    for ref, count in ((r0, NX), (z0, NX), (q0, NX), (w, NX), (v0, NX), (f1, NX // 2), (v1, NX // 2), (f2, NX // 4), (t2, NX // 4)):
        ref[0] = jnp.zeros(ref.shape[1:], jnp.float32)
        ref[count + 1] = jnp.zeros(ref.shape[1:], jnp.float32)
    lanes = lane_index((8, LANES))
    y_blocks = [tuple(ref.at[:, pl.ds(BY * b, BY)] for ref in (up, rows_, down)) for b in range(4)]
    y_blocks.insert(2, (left, own, right))

    def unpack(i, _):
        for b, sources in enumerate(y_blocks):
            for odd in range(2):
                a, c, d = (ref[i, pl.ds(8 * odd, 8)] for ref in sources)
                for k in range(4):
                    value = jnp.where(lanes < 32, roll(a, -32 * k, 1), jnp.where(lanes < 64, roll(c, 32 - 32 * k, 1), roll(d, 64 - 32 * k, 1)))
                    r0[4 * i + k + 1, odd, at(8 * b)] = value
        return 0

    lax.fori_loop(0, NX // 4, unpack, 0, unroll=16)
    low = {step: lanes & step == 0 for step in (1, 2)}

    def fold(x, step):
        return 0.5 * (x + jnp.where(low[step], roll(x, -step, 1), roll(x, step, 1)))

    middle = (8, 16, 24)
    cycle_down(r0, mask, mask2, fold, v1, e1, f1, f2, (0, 8, 16, 24, 32), (0, 8, 12), 4, 8)
    cycle_coarse(mask2, f2, t2, e2, (0, 8, 12), (1, 9))
    cycle_up(r0, mask, f1, e2, v1, e1, v0, z0, (6, 14, 22, 26), (7, 15, 23, 25), ((8, 16, 24, 25), (7, 15, 23, 24)), (middle, middle), 32, 64)

    def image(first):
        for odd in range(2):
            for r in middle:
                m = mask[at(r)]
                for k, (_, value) in enumerate(images(z0, first, odd, r, 64)):
                    q0[first + k + 1, odd, at(r)] = value * m

    chunks(NX, 64, image)
    cycle_down(q0, mask, mask2, fold, v1, e1, f1, f2, middle, (5, 7), 8, 16)
    cycle_coarse(mask2, f2, t2, e2, (6,), (6,))
    cycle_up(q0, mask, f1, e2, v1, e1, v0, w, (14, 18), (15, 17), ((15, 17), (15, 17)), ((16, 17), (15, 16)), 32, 64)

    def sums(i, acc):
        acc = list(acc)
        for odd in range(2):
            for k, (ww, s) in enumerate(images(w, 64 * i, odd, 16, 64)):
                x = 64 * i + k + 1
                r, zz, q = r0[x, odd, at(16)], z0[x, odd, at(16)], q0[x, odd, at(16)]
                for n, term in enumerate((r * zz, zz * q, r * ww, q * ww, ww * s)):
                    acc[n] = acc[n] + term
                v0[x, odd, at(16)] = s
        return tuple(acc)

    acc = lax.fori_loop(0, NX // 64, sums, (jnp.zeros((8, LANES), jnp.float32),) * 5)

    for odd_slab, ref in enumerate((other, out)):
        for t in range(4):
            for k in range(BX):
                x = BX * (2 * t + odd_slab) + k + 1
                for odd in range(2):
                    zz, q, ww, s = (field[x, odd, at(16)] for field in (z0, q0, w, v0))
                    ref[t, pl.ds(k * BY + 8 * odd, 8)] = jnp.where(
                        lanes < 32, roll(zz, -32, 1), jnp.where(lanes < 64, q, jnp.where(lanes < 96, roll(ww, 32, 1), roll(s, 64, 1)))
                    )
    home = (lanes >= HZ) & (lanes < HZ + CZ)
    row = jnp.zeros((8, LANES), jnp.float32)
    for k, a in enumerate(acc):
        row = jnp.where(lanes == k, jnp.sum(jnp.where(home, a, 0.0)), row)
    for t in range(4):
        out[t, BX * BY : BX * BY + 8] = row
        other[t, BX * BY : BX * BY + 8] = row


def cycles(*blocks):
    fine = pltpu.VMEM((NX + 2, 2, 56, LANES), jnp.float32)
    level1 = pltpu.VMEM((NX // 2 + 2, 56, LANES), jnp.float32)
    level2 = pltpu.VMEM((NX // 4 + 2, 40, LANES), jnp.float32)
    return pl.pallas_call(
        cycles_kernel,
        out_shape=(jax.ShapeDtypeStruct((4, BX * BY + 8, LANES), jnp.float32),) * 2,
        in_specs=[VMEM] * 6,
        out_specs=(VMEM, VMEM),
        scratch_shapes=[fine] * 5
        + [level1] * 3
        + [pltpu.VMEM((NX // 4 + 2, 56, LANES), jnp.float32), level2, level2, pltpu.VMEM((56, LANES), jnp.float32), pltpu.VMEM((40, LANES), jnp.float32)],
        compiler_params=pltpu.CompilerParams(vmem_limit_bytes=30 * 1024 * 1024),
    )(*blocks)


def finish_kernel(rhs, fields, sums, solution, residual):
    total = jnp.sum(sums[...], axis=0, keepdims=True)
    lanes = lane_index(total.shape)

    def pick(k):
        return jnp.sum(jnp.where(lanes == k, total, 0.0), axis=1, keepdims=True)

    rz, zq, rw, qw, ws = (pick(k) for k in range(5))
    step0 = rz / zq
    rz1 = rz - step0 * (rw + zq) + step0 * step0 * qw
    growth = rz1 / rz
    image1 = (zq - 2.0 * step0 * qw + step0 * step0 * ws) + 2.0 * growth * (zq - step0 * qw) + growth * growth * zq
    step1 = rz1 / image1
    on_z = step0 + step1 * (1.0 + growth)
    on_w = -step1 * step0
    wide = lane_index((BY, LANES))
    gz = lax.axis_index("gz")
    for x in range(BX):
        parts = [fields[z_block(c, gz), x * BY : (x + 1) * BY] for c in range(4)]

        def field(f):
            value = None
            for c in range(4):
                part = roll(parts[c], 32 * (c - f), 1)
                value = part if c == 0 else jnp.where(wide >= 32 * c, part, value)
            return value

        z0, q0, w, s = (field(f) for f in range(4))
        u = on_z * z0 + on_w * w
        v = on_z * q0 + on_w * s
        for odd in range(2):
            rows = pl.ds(odd, 8, stride=2)
            solution[x, rows, :] = u[8 * odd : 8 * odd + 8]
            residual[x, rows, :] = rhs[x, rows, :] - v[8 * odd : 8 * odd + 8]


def finish(rhs, fields, sums):
    shape = jax.ShapeDtypeStruct((BX, BY, BZ), jnp.float32)
    return pl.pallas_call(finish_kernel, out_shape=(shape, shape), in_specs=[VMEM] * 3, out_specs=(VMEM, VMEM), compiler_params=small())(rhs, fields, sums)


def y_pairs(step):
    return [(16 + a, a + step) for a in range(16) if 0 <= a + step < 16]


def z_pairs(step):
    def number(core, block):
        gz, at = block // 4, block % 4
        return ((at if gz % 2 == 0 else 3 - at) * 2 + core) * 8 + gz

    return [(number(0, a), number(1, a + step)) for a in range(32) if 0 <= a + step < 32]


Z_AXES = ("gx_0", "gx_1", "gz")


def local(density, x_faces, y_faces, z_faces):
    rhs, packed = make_rhs(density, x_faces, y_faces, z_faces)
    own = lax.all_to_all(packed, GX, 0, 0, tiled=True).reshape(16, BY, 128)
    moved = []
    for step in (1, -1, 2, -2):
        moved.append(lax.ppermute(own, ("gx_1", "gy"), y_pairs(step)))
    left = lax.ppermute(own, Z_AXES, z_pairs(1))
    right = lax.ppermute(own, Z_AXES, z_pairs(-1))
    rows = join(moved[2], moved[0], moved[1], moved[3])
    up = lax.ppermute(rows, Z_AXES, z_pairs(1))
    down = lax.ppermute(rows, Z_AXES, z_pairs(-1))
    rows = lax.ppermute(rows, "gx_1", [(0, 1)])
    packed, other = cycles(own, left, right, rows, up, down)
    other = lax.ppermute(other, "gx_1", [(1, 0)])
    packed = jnp.where(lax.axis_index("gx_1") == 0, other, packed)
    fields = lax.all_to_all(packed, "gx_0", 0, 0, tiled=True)
    sums = jnp.sum(fields[:, BX * BY, :], axis=0)
    sums = lax.all_to_all(jnp.broadcast_to(sums, (128, 1, 128)), ("gy", "gz"), 0, 0, tiled=True)
    return finish(rhs, fields, sums.reshape(128, 128))


def solution(mesh):
    torus = Mesh(mesh.devices.reshape(4, 2, mesh.shape["gy"], mesh.shape["gz"]), AXES)
    in_specs = (P(GX, "gy", "gz"), P(None, "gy", "gz"), P(None, GX, "gz"), P(None, GX, "gy"))
    out_specs = (P(GX, "gy", "gz"), P(GX, "gy", "gz"))
    return jax.shard_map(local, mesh=torus, in_specs=in_specs, out_specs=out_specs, check_vma=False)
```

```python
import jax
import jax.numpy as jnp
from jax import lax
from jax.experimental import pallas as pl
from jax.experimental.pallas import tpu as pltpu
from jax.sharding import Mesh
from jax.sharding import PartitionSpec as P


AXES = ("gx_0", "gx_1", "gy", "gz")
GX = ("gx_0", "gx_1")
NX, NY, NZ = 64, 256, 1024
BX, BY, BZ = 8, 16, 128
CZ = 32
HY, HZ = 32, 32
LANES = 128
relax = 1.0 / 9.0
coupling = 0.5
VMEM = pl.BlockSpec(memory_space=pltpu.VMEM)
HBM = pl.BlockSpec(memory_space=pltpu.MemorySpace.HBM)


def roll(x, shift, axis):
    return pltpu.roll(x, shift % x.shape[axis], axis)


def place():
    return tuple(lax.axis_index(axis) for axis in AXES)


def z_block(gx0, gz):
    return jnp.where(gz % 2 == 0, gx0, 3 - gx0)


def small(**more):
    return pltpu.CompilerParams(vmem_limit_bytes=4 * 1024 * 1024, **more)


def lane_index(shape):
    return lax.broadcasted_iota(jnp.int32, shape, 1)


def row_index(shape):
    return lax.broadcasted_iota(jnp.int32, shape, 0)


def rhs_kernel(density_in, xf_in, yf_in, zf_in, rhs, packed, scratch, density, xf, yf, zf, arrived):
    copies = [pltpu.make_async_copy(a, b, arrived.at[i]) for i, (a, b) in enumerate(((density_in, density), (xf_in, xf), (yf_in, yf), (zf_in, zf)))]
    for copy in copies:
        copy.start()
    gx0, core, gy, gz = place()
    gx = 2 * gx0 + core
    rows, lanes = row_index((BY, BZ)), lane_index((BY, BZ))
    eye = row_index((BY, BY)) == lane_index((BY, BY))
    low_y = (rows == 0) & (gy == 0)
    high_y = (rows == BY - 1) & (gy == NY // BY - 1)
    low_z = (lanes == 0) & (gz == 0)
    high_z = (lanes == BZ - 1) & (gz == NZ // BZ - 1)

    def column(row):
        return jnp.sum(jnp.where(eye, row, 0.0), axis=1, keepdims=True)

    for copy in copies:
        copy.wait()
    layers = []
    for x in range(BX):
        value = -coupling * density[x]
        if x == 0:
            value = value + jnp.where(gx == 0, xf[0], 0.0)
        if x == BX - 1:
            value = value + jnp.where(gx == NX // BX - 1, xf[1], 0.0)
        value = value + jnp.where(low_y, yf[0, x : x + 1, :], 0.0)
        value = value + jnp.where(high_y, yf[1, x : x + 1, :], 0.0)
        value = value + jnp.where(low_z, column(zf[0, x : x + 1, :]), 0.0)
        value = value + jnp.where(high_z, column(zf[1, x : x + 1, :]), 0.0)
        rhs[x] = value
        layers.append(value)
    for chunk in range(4):
        for quad in range(2):
            out = None
            for k in range(4):
                part = roll(layers[4 * quad + k], 32 * (k - chunk), 1)
                out = part if k == 0 else jnp.where(lanes >= 32 * k, part, out)
            scratch[chunk, quad] = out
    for chip in range(4):
        chunk = z_block(chip, gz)
        for quad in range(2):
            for odd in range(2):
                part = scratch[chunk, quad, pl.ds(odd, 8, stride=2), :]
                packed[2 * chip, quad, 8 * odd : 8 * odd + 8] = part
                packed[2 * chip + 1, quad, 8 * odd : 8 * odd + 8] = part


def make_rhs(density, xf, yf, zf):
    return pl.pallas_call(
        rhs_kernel,
        out_shape=(
            jax.ShapeDtypeStruct((BX, BY, BZ), jnp.float32),
            jax.ShapeDtypeStruct((8, 2, BY, BZ), jnp.float32),
        ),
        in_specs=[HBM] * 4,
        out_specs=(VMEM, VMEM),
        scratch_shapes=[pltpu.VMEM((4, 2, BY, BZ), jnp.float32)]
        + [pltpu.VMEM(a.shape, a.dtype) for a in (density, xf, yf, zf)]
        + [pltpu.SemaphoreType.DMA((4,))],
        compiler_params=pltpu.CompilerParams(vmem_limit_bytes=60 * 1024 * 1024),
    )(density, xf, yf, zf)


def join_kernel(*refs):
    out = refs[-1]
    for b, ref in enumerate(refs[:-1]):
        for i in range(16):
            out[i, BY * b : BY * b + BY] = ref[i]


def join(*blocks):
    return pl.pallas_call(
        join_kernel,
        out_shape=jax.ShapeDtypeStruct((16, 4 * BY, 128), jnp.float32),
        in_specs=[VMEM] * 4,
        out_specs=VMEM,
        compiler_params=small(),
    )(*blocks)


def at(row, step=0):
    return pl.ds(8 + row + step, 8)


def every_other(row, step=0):
    return pl.ds(8 + 2 * row + step, 8, stride=2)


def sides(x, step):
    return roll(x, step, 1) + roll(x, -step, 1)


def third(x):
    return x * (1.0 / 3.0)


def chunks(count, size, body):
    size, unroll = size if isinstance(size, tuple) else (size, 1)
    if size == count:
        body(0)
    elif size * unroll == count:
        for i in range(unroll):
            body(i * size)
    else:
        lax.fori_loop(0, count // size, lambda i, _: body(i * size) or 0, 0, unroll=unroll)


def cycle_down(src, mask, mask2, fold, sum1, part1, f1, f2, rows1, rows2, size, nb):
    def gather(first, size=size):
        for r in rows1:
            layers = [2 * first + k for k in range(2 * size + 2)]
            cells = [src[x, 0, at(r)] + src[x, 1, at(r)] for x in layers]
            beyond = [src[x, 1, at(r, -1)] + src[x, 0, at(r, 1)] for x in layers[1:-1]]
            for i in range(size):
                before, a, b, after = cells[2 * i : 2 * i + 4]
                u = a + b
                y = beyond[2 * i] + beyond[2 * i + 1]
                sum1[first + i + 1, at(r)] = u
                part1[first + i + 1, at(r)] = third(u) + relax * (((u + u) + (before + after)) + y)

    chunks(NX // 2, size, gather)

    def across(first):
        for r in rows1:
            for x in [first + k for k in range(1, 32 + 1)]:
                f1[x, at(r)] = part1[x, at(r)] + relax * sides(sum1[x, at(r)], 1)

    chunks(NX // 2, 32, across)

    def level1(first):
        for r in rows1:
            m = mask[at(r)]
            for x in [first + k for k in range(1, 16 + 1)]:
                f1[x, at(r)] = fold(f1[x, at(r)], 1) * m

    chunks(NX // 2, 16, level1)

    def level2(first):
        for r in rows2:
            m = mask2[at(r)]
            layers = [2 * first + k for k in range(2 * nb + 2)]
            cells = [f1[x, every_other(r), :] + f1[x, every_other(r, 1), :] for x in layers]
            beyond = [f1[x, every_other(r, -1), :] + f1[x, every_other(r, 2), :] for x in layers[1:-1]]
            for i in range(nb):
                before, a, b, after = cells[2 * i : 2 * i + 4]
                u = a + b
                y = beyond[2 * i] + beyond[2 * i + 1]
                s = third(u) + relax * (((u + u) + (before + after)) + (y + sides(u, 2)))
                f2[first + i + 1, at(r)] = fold(s, 2) * m

    chunks(NX // 4, nb, level2)


def cycle_coarse(mask2, f2, t2, e2, rows, last):
    def around(ref, x, r):
        return (ref[x - 1, at(r)] + ref[x + 1, at(r)]) + (ref[x, at(r, -1)] + ref[x, at(r, 1)])

    def sweep1(first):
        for r in rows:
            m = mask2[at(r)]
            for x in range(1, 9):
                v = f2[first + x, at(r)]
                s = (4.0 / 3.0) * v + relax * (around(f2, first + x, r) + sides(v, 4))
                t2[first + x, at(r)] = (relax * s) * m

    chunks(NX // 4, 8, sweep1)

    def sweep2(first):
        for r in last:
            m = mask2[at(r)]
            for x in range(1, 9):
                v = t2[first + x, at(r)]
                s = (third(v) + relax * (f2[first + x, at(r)] + (around(t2, first + x, r) + sides(v, 4)))) * m
                e2[first + x, every_other(r), :] = s
                e2[first + x, every_other(r, 1), :] = s

    chunks(NX // 4, 8, sweep2)


def cycle_up(src, mask, f1, e2, v1, e1, v0, out, rows1, last1, rows0, last0, nd, ne):
    def correct1(first):
        for r in rows1:
            for i in range(4):
                e = e2[first + i + 1, at(r)]
                for k in (1, 2):
                    x = 2 * first + 2 * i + k
                    v1[x, at(r)] = relax * f1[x, at(r)] + e

    chunks(NX // 4, 4, correct1)

    def smooth1(first):
        for r in last1:
            m = mask[at(r)]
            for x in [first + k for k in range(1, nd + 1)]:
                v = v1[x, at(r)]
                y = v1[x, at(r, -1)] + v1[x, at(r, 1)]
                s = third(v) + relax * ((f1[x, at(r)] + (v1[x - 1, at(r)] + v1[x + 1, at(r)])) + (y + sides(v, 2)))
                e1[x, at(r)] = s * m

    chunks(NX // 2, nd, smooth1)

    def correct0(first):
        for odd in range(2):
            for r in rows0[odd]:
                for i in range(1, 5):
                    e = e1[first + i, at(r)]
                    for k in (-1, 0):
                        x = 2 * first + 2 * i + k
                        v0[x, odd, at(r)] = relax * src[x, odd, at(r)] + e

    chunks(NX // 2, 4, correct0)

    def smooth0(first):
        for odd in range(2):
            for r in last0[odd]:
                m = mask[at(r)]
                layers = [v0[first + k, odd, at(r)] for k in range(ne + 2)]
                for k in range(1, ne + 1):
                    x = first + k
                    v = layers[k]
                    y = v0[x, 1 - odd, at(r, odd - 1)] + v0[x, 1 - odd, at(r, odd)]
                    s = third(v) + relax * ((src[x, odd, at(r)] + (layers[k - 1] + layers[k + 1])) + (y + sides(v, 1)))
                    out[x, odd, at(r)] = s * m

    chunks(NX, ne, smooth0)


def images(src, first, odd, r, count):
    layers = [src[first + k, odd, at(r)] for k in range(count + 2)]
    result = []
    for k in range(1, count + 1):
        v = layers[k]
        y = src[first + k, 1 - odd, at(r, odd - 1)] + src[first + k, 1 - odd, at(r, odd)]
        result.append((v, 6.0 * v - ((layers[k - 1] + layers[k + 1]) + (y + sides(v, 1)))))
    return result


def cycles_kernel(*refs):
    pl.when(lax.axis_index("gx_1") == 0)(lambda: cycles_on_core(*refs))


def cycles_on_core(own, left, right, rows_, up, down, out, other, r0, z0, q0, w, v0, f1, v1, e1, e2, f2, t2, mask, mask2):
    gx0, _, gy, gz = place()

    def inside(count, height):
        rows, lanes = row_index((count, LANES)) - 8, lane_index((count, LANES))
        y = gy * BY - HY + height * rows
        z = (gz * 4 + z_block(gx0, gz)) * CZ - HZ + lanes
        return jnp.where((y >= 0) & (y < NY) & (z >= 0) & (z < NZ), 1.0, 0.0)

    mask[...] = inside(56, 2)
    mask2[...] = inside(40, 4)
    for ref, count in ((r0, NX), (z0, NX), (q0, NX), (w, NX), (v0, NX), (f1, NX // 2), (v1, NX // 2), (f2, NX // 4), (t2, NX // 4)):
        ref[0] = jnp.zeros(ref.shape[1:], jnp.float32)
        ref[count + 1] = jnp.zeros(ref.shape[1:], jnp.float32)
    lanes = lane_index((8, LANES))
    y_blocks = [tuple(ref.at[:, pl.ds(BY * b, BY)] for ref in (up, rows_, down)) for b in range(4)]
    y_blocks.insert(2, (left, own, right))

    def unpack(i, _):
        for b, sources in enumerate(y_blocks):
            for odd in range(2):
                a, c, d = (ref[i, pl.ds(8 * odd, 8)] for ref in sources)
                for k in range(4):
                    value = jnp.where(lanes < 32, roll(a, -32 * k, 1), jnp.where(lanes < 64, roll(c, 32 - 32 * k, 1), roll(d, 64 - 32 * k, 1)))
                    r0[4 * i + k + 1, odd, at(8 * b)] = value
        return 0

    lax.fori_loop(0, NX // 4, unpack, 0, unroll=16)
    low = {step: lanes & step == 0 for step in (1, 2)}

    def fold(x, step):
        return 0.5 * (x + jnp.where(low[step], roll(x, -step, 1), roll(x, step, 1)))

    middle = (8, 16, 24)
    cycle_down(r0, mask, mask2, fold, v1, e1, f1, f2, (0, 8, 16, 24, 32), (0, 8, 12), 4, 8)
    cycle_coarse(mask2, f2, t2, e2, (0, 8, 12), (1, 9))
    cycle_up(r0, mask, f1, e2, v1, e1, v0, z0, (6, 14, 22, 26), (7, 15, 23, 25), ((8, 16, 24, 25), (7, 15, 23, 24)), (middle, middle), 32, 64)

    def image(first):
        for odd in range(2):
            for r in middle:
                m = mask[at(r)]
                for k, (_, value) in enumerate(images(z0, first, odd, r, 64)):
                    q0[first + k + 1, odd, at(r)] = value * m

    chunks(NX, 64, image)
    cycle_down(q0, mask, mask2, fold, v1, e1, f1, f2, middle, (5, 7), 8, 16)
    cycle_coarse(mask2, f2, t2, e2, (6,), (6,))
    cycle_up(q0, mask, f1, e2, v1, e1, v0, w, (14, 18), (15, 17), ((15, 17), (15, 17)), ((16, 17), (15, 16)), 32, 64)

    def sums(i, acc):
        acc = list(acc)
        for odd in range(2):
            for k, (ww, s) in enumerate(images(w, 64 * i, odd, 16, 64)):
                x = 64 * i + k + 1
                r, zz, q = r0[x, odd, at(16)], z0[x, odd, at(16)], q0[x, odd, at(16)]
                for n, term in enumerate((r * zz, zz * q, r * ww, q * ww, ww * s)):
                    acc[n] = acc[n] + term
                v0[x, odd, at(16)] = s
        return tuple(acc)

    acc = lax.fori_loop(0, NX // 64, sums, (jnp.zeros((8, LANES), jnp.float32),) * 5)

    for odd_slab, ref in enumerate((out, other)):
        for t in range(4):
            for k in range(BX):
                x = BX * (2 * t + odd_slab) + k + 1
                for odd in range(2):
                    zz, q, ww, s = (field[x, odd, at(16)] for field in (z0, q0, w, v0))
                    ref[t, pl.ds(k * BY + 8 * odd, 8)] = jnp.where(
                        lanes < 32, roll(zz, -32, 1), jnp.where(lanes < 64, q, jnp.where(lanes < 96, roll(ww, 32, 1), roll(s, 64, 1)))
                    )
    home = (lanes >= HZ) & (lanes < HZ + CZ)
    row = jnp.zeros((8, LANES), jnp.float32)
    for k, a in enumerate(acc):
        row = jnp.where(lanes == k, jnp.sum(jnp.where(home, a, 0.0)), row)
    for t in range(4):
        out[t, BX * BY : BX * BY + 8] = row
        other[t, BX * BY : BX * BY + 8] = row


def cycles(*blocks):
    fine = pltpu.VMEM((NX + 2, 2, 56, LANES), jnp.float32)
    level1 = pltpu.VMEM((NX // 2 + 2, 56, LANES), jnp.float32)
    level2 = pltpu.VMEM((NX // 4 + 2, 40, LANES), jnp.float32)
    return pl.pallas_call(
        cycles_kernel,
        out_shape=(jax.ShapeDtypeStruct((4, BX * BY + 8, LANES), jnp.float32),) * 2,
        in_specs=[VMEM] * 6,
        out_specs=(VMEM, VMEM),
        scratch_shapes=[fine] * 5
        + [level1] * 3
        + [pltpu.VMEM((NX // 4 + 2, 56, LANES), jnp.float32), level2, level2, pltpu.VMEM((56, LANES), jnp.float32), pltpu.VMEM((40, LANES), jnp.float32)],
        compiler_params=pltpu.CompilerParams(vmem_limit_bytes=30 * 1024 * 1024),
    )(*blocks)


def finish_kernel(rhs, fields, sums, solution, residual):
    total = jnp.sum(sums[...], axis=0, keepdims=True)
    lanes = lane_index(total.shape)

    def pick(k):
        return jnp.sum(jnp.where(lanes == k, total, 0.0), axis=1, keepdims=True)

    rz, zq, rw, qw, ws = (pick(k) for k in range(5))
    step0 = rz / zq
    rz1 = rz - step0 * (rw + zq) + step0 * step0 * qw
    growth = rz1 / rz
    image1 = (zq - 2.0 * step0 * qw + step0 * step0 * ws) + 2.0 * growth * (zq - step0 * qw) + growth * growth * zq
    step1 = rz1 / image1
    on_z = step0 + step1 * (1.0 + growth)
    on_w = -step1 * step0
    wide = lane_index((BY, LANES))
    gz = lax.axis_index("gz")
    for x in range(BX):
        parts = [fields[z_block(c, gz), x * BY : (x + 1) * BY] for c in range(4)]

        def field(f):
            value = None
            for c in range(4):
                part = roll(parts[c], 32 * (c - f), 1)
                value = part if c == 0 else jnp.where(wide >= 32 * c, part, value)
            return value

        z0, q0, w, s = (field(f) for f in range(4))
        u = on_z * z0 + on_w * w
        v = on_z * q0 + on_w * s
        for odd in range(2):
            rows = pl.ds(odd, 8, stride=2)
            solution[x, rows, :] = u[8 * odd : 8 * odd + 8]
            residual[x, rows, :] = rhs[x, rows, :] - v[8 * odd : 8 * odd + 8]


def finish(rhs, fields, sums):
    shape = jax.ShapeDtypeStruct((BX, BY, BZ), jnp.float32)
    return pl.pallas_call(finish_kernel, out_shape=(shape, shape), in_specs=[VMEM] * 3, out_specs=(VMEM, VMEM), compiler_params=small())(rhs, fields, sums)


def y_pairs(step):
    return [(a, 16 + a + step) for a in range(16) if 0 <= a + step < 16]


def z_pairs(step):
    def number(core, block):
        gz, at = block // 4, block % 4
        return ((at if gz % 2 == 0 else 3 - at) * 2 + core) * 8 + gz

    return [(number(1, a), number(0, a + step)) for a in range(32) if 0 <= a + step < 32]


Z_AXES = ("gx_0", "gx_1", "gz")


def local(density, x_faces, y_faces, z_faces):
    rhs, packed = make_rhs(density, x_faces, y_faces, z_faces)
    own = lax.all_to_all(packed, GX, 0, 0, tiled=True).reshape(16, BY, 128)
    moved = []
    for step in (2, -2, 1, -1):
        moved.append(lax.ppermute(own, ("gx_1", "gy"), y_pairs(step)))
    left = lax.ppermute(own, Z_AXES, z_pairs(1))
    right = lax.ppermute(own, Z_AXES, z_pairs(-1))
    rows = join(moved[0], moved[2], moved[3], moved[1])
    up = lax.ppermute(rows, Z_AXES, z_pairs(1))
    down = lax.ppermute(rows, Z_AXES, z_pairs(-1))
    rows = lax.ppermute(rows, "gx_1", [(1, 0)])
    packed, other = cycles(own, left, right, rows, up, down)
    other = lax.ppermute(other, "gx_1", [(0, 1)])
    packed = jnp.where(lax.axis_index("gx_1") == 1, other, packed)
    fields = lax.all_to_all(packed, "gx_0", 0, 0, tiled=True)
    sums = jnp.sum(fields[:, BX * BY, :], axis=0)
    sums = lax.all_to_all(jnp.broadcast_to(sums, (128, 1, 128)), ("gy", "gz"), 0, 0, tiled=True)
    return finish(rhs, fields, sums.reshape(128, 128))


def solution(mesh):
    torus = Mesh(mesh.devices.reshape(4, 2, mesh.shape["gy"], mesh.shape["gz"]), AXES)
    in_specs = (P(GX, "gy", "gz"), P(None, "gy", "gz"), P(None, GX, "gz"), P(None, GX, "gy"))
    out_specs = (P(GX, "gy", "gz"), P(GX, "gy", "gz"))
    return jax.shard_map(local, mesh=torus, in_specs=in_specs, out_specs=out_specs, check_vma=False)
```

```python
import jax
import jax.numpy as jnp
from jax import lax
from jax.experimental import pallas as pl
from jax.experimental.pallas import tpu as pltpu
from jax.sharding import Mesh
from jax.sharding import PartitionSpec as P


AXES = ("gx_0", "gx_1", "gy", "gz")
GX = ("gx_0", "gx_1")
NX, NY, NZ = 64, 256, 1024
BX, BY, BZ = 8, 16, 128
CZ = 32
HY, HZ = 32, 32
LANES = 128
relax = 1.0 / 9.0
coupling = 0.5
VMEM = pl.BlockSpec(memory_space=pltpu.VMEM)
HBM = pl.BlockSpec(memory_space=pltpu.MemorySpace.HBM)


def roll(x, shift, axis):
    return pltpu.roll(x, shift % x.shape[axis], axis)


def place():
    return tuple(lax.axis_index(axis) for axis in AXES)


def z_block(gx0, gz):
    return jnp.where(gz % 2 == 0, gx0, 3 - gx0)


def small(**more):
    return pltpu.CompilerParams(vmem_limit_bytes=4 * 1024 * 1024, **more)


def lane_index(shape):
    return lax.broadcasted_iota(jnp.int32, shape, 1)


def row_index(shape):
    return lax.broadcasted_iota(jnp.int32, shape, 0)


def rhs_kernel(density_in, xf_in, yf_in, zf_in, rhs, packed, scratch, density, xf, yf, zf, arrived):
    copies = [pltpu.make_async_copy(a, b, arrived.at[i]) for i, (a, b) in enumerate(((density_in, density), (xf_in, xf), (yf_in, yf), (zf_in, zf)))]
    for copy in copies:
        copy.start()
    gx0, core, gy, gz = place()
    gx = 2 * gx0 + core
    rows, lanes = row_index((BY, BZ)), lane_index((BY, BZ))
    eye = row_index((BY, BY)) == lane_index((BY, BY))
    low_y = (rows == 0) & (gy == 0)
    high_y = (rows == BY - 1) & (gy == NY // BY - 1)
    low_z = (lanes == 0) & (gz == 0)
    high_z = (lanes == BZ - 1) & (gz == NZ // BZ - 1)

    def column(row):
        return jnp.sum(jnp.where(eye, row, 0.0), axis=1, keepdims=True)

    for copy in copies:
        copy.wait()
    layers = []
    for x in range(BX):
        value = -coupling * density[x]
        if x == 0:
            value = value + jnp.where(gx == 0, xf[0], 0.0)
        if x == BX - 1:
            value = value + jnp.where(gx == NX // BX - 1, xf[1], 0.0)
        value = value + jnp.where(low_y, yf[0, x : x + 1, :], 0.0)
        value = value + jnp.where(high_y, yf[1, x : x + 1, :], 0.0)
        value = value + jnp.where(low_z, column(zf[0, x : x + 1, :]), 0.0)
        value = value + jnp.where(high_z, column(zf[1, x : x + 1, :]), 0.0)
        rhs[x] = value
        layers.append(value)
    for chunk in range(4):
        for quad in range(2):
            out = None
            for k in range(4):
                part = roll(layers[4 * quad + k], 32 * (k - chunk), 1)
                out = part if k == 0 else jnp.where(lanes >= 32 * k, part, out)
            scratch[chunk, quad] = out
    for chip in range(4):
        chunk = z_block(chip, gz)
        for quad in range(2):
            for odd in range(2):
                part = scratch[chunk, quad, pl.ds(odd, 8, stride=2), :]
                packed[2 * chip, quad, 8 * odd : 8 * odd + 8] = part
                packed[2 * chip + 1, quad, 8 * odd : 8 * odd + 8] = part


def make_rhs(density, xf, yf, zf):
    return pl.pallas_call(
        rhs_kernel,
        out_shape=(
            jax.ShapeDtypeStruct((BX, BY, BZ), jnp.float32),
            jax.ShapeDtypeStruct((8, 2, BY, BZ), jnp.float32),
        ),
        in_specs=[HBM] * 4,
        out_specs=(VMEM, VMEM),
        scratch_shapes=[pltpu.VMEM((4, 2, BY, BZ), jnp.float32)]
        + [pltpu.VMEM(a.shape, a.dtype) for a in (density, xf, yf, zf)]
        + [pltpu.SemaphoreType.DMA((4,))],
        compiler_params=pltpu.CompilerParams(vmem_limit_bytes=60 * 1024 * 1024),
    )(density, xf, yf, zf)


def join_kernel(*refs):
    out = refs[-1]
    for b, ref in enumerate(refs[:-1]):
        for i in range(16):
            out[i, BY * b : BY * b + BY] = ref[i]


def join(*blocks):
    return pl.pallas_call(
        join_kernel,
        out_shape=jax.ShapeDtypeStruct((16, 4 * BY, 128), jnp.float32),
        in_specs=[VMEM] * 4,
        out_specs=VMEM,
        compiler_params=small(),
    )(*blocks)


def unpack_kernel(*refs):
    pl.when(lax.axis_index("gx_1") == 0)(lambda: unpack_on_core(*refs))


def unpack_on_core(own, left, right, rows_, out):
    lanes = lane_index((8, LANES))
    even = lanes // 32 % 2 == 0
    for i in range(16):
        for odd in range(2):
            for b in range(4):
                c = rows_[i, pl.ds(BY * b + 8 * odd, 8)]
                for k in range(4):
                    out[4 * i + k, odd, pl.ds(8 * (b + b // 2), 8)] = roll(c, 32 - 32 * k, 1)
            part = pl.ds(8 * odd, 8)
            a, c, d = left[i, part], own[i, part], right[i, part]
            low = jnp.where(lanes < 64, a, roll(d, 64, 1))
            high = jnp.where(lanes < 64, roll(a, 64, 1), d)
            out[4 * i, odd, 16:24] = jnp.where(even, low, roll(c, 32, 1))
            out[4 * i + 1, odd, 16:24] = jnp.where(even, roll(low, -32, 1), c)
            out[4 * i + 2, odd, 16:24] = jnp.where(even, high, roll(c, -32, 1))
            out[4 * i + 3, odd, 16:24] = jnp.where(even, roll(high, -32, 1), roll(c, 64, 1))


def unpack(own, left, right, rows):
    return pl.pallas_call(
        unpack_kernel,
        out_shape=jax.ShapeDtypeStruct((NX, 2, 40, LANES), jnp.float32),
        in_specs=[VMEM] * 4,
        out_specs=VMEM,
        compiler_params=small(),
    )(own, left, right, rows)


def at(row, step=0):
    return pl.ds(8 + row + step, 8)


def every_other(row, step=0):
    return pl.ds(8 + 2 * row + step, 8, stride=2)


def sides(x, step):
    return roll(x, step, 1) + roll(x, -step, 1)


def third(x):
    return x * (1.0 / 3.0)


def chunks(count, size, body):
    size, unroll = size if isinstance(size, tuple) else (size, 1)
    if size == count:
        body(0)
    elif size * unroll == count:
        for i in range(unroll):
            body(i * size)
    else:
        lax.fori_loop(0, count // size, lambda i, _: body(i * size) or 0, 0, unroll=unroll)


def cycle_down(src, mask, mask2, fold, sum1, part1, f1, f2, rows1, rows2, size, nb):
    def gather(first, size=size):
        for r in rows1:
            layers = [2 * first + k for k in range(2 * size + 2)]
            cells = [src[x, 0, at(r)] + src[x, 1, at(r)] for x in layers]
            beyond = [src[x, 1, at(r, -1)] + src[x, 0, at(r, 1)] for x in layers[1:-1]]
            for i in range(size):
                before, a, b, after = cells[2 * i : 2 * i + 4]
                u = a + b
                y = beyond[2 * i] + beyond[2 * i + 1]
                sum1[first + i + 1, at(r)] = u
                part1[first + i + 1, at(r)] = third(u) + relax * (((u + u) + (before + after)) + y)

    chunks(NX // 2, size, gather)

    def across(first):
        for r in rows1:
            for x in [first + k for k in range(1, 32 + 1)]:
                f1[x, at(r)] = part1[x, at(r)] + relax * sides(sum1[x, at(r)], 1)

    chunks(NX // 2, 32, across)

    def level1(first):
        for r in rows1:
            m = mask[at(r)]
            for x in [first + k for k in range(1, 16 + 1)]:
                f1[x, at(r)] = fold(f1[x, at(r)], 1) * m

    chunks(NX // 2, 16, level1)

    def level2(first):
        for r in rows2:
            m = mask2[at(r)]
            layers = [2 * first + k for k in range(2 * nb + 2)]
            cells = [f1[x, every_other(r), :] + f1[x, every_other(r, 1), :] for x in layers]
            beyond = [f1[x, every_other(r, -1), :] + f1[x, every_other(r, 2), :] for x in layers[1:-1]]
            for i in range(nb):
                before, a, b, after = cells[2 * i : 2 * i + 4]
                u = a + b
                y = beyond[2 * i] + beyond[2 * i + 1]
                s = third(u) + relax * (((u + u) + (before + after)) + (y + sides(u, 2)))
                f2[first + i + 1, at(r)] = fold(s, 2) * m

    chunks(NX // 4, nb, level2)


def cycle_coarse(mask2, f2, t2, e2, rows, last):
    def around(ref, x, r):
        return (ref[x - 1, at(r)] + ref[x + 1, at(r)]) + (ref[x, at(r, -1)] + ref[x, at(r, 1)])

    def sweep1(first):
        for r in rows:
            m = mask2[at(r)]
            for x in range(1, 17):
                v = f2[first + x, at(r)]
                s = (4.0 / 3.0) * v + relax * (around(f2, first + x, r) + sides(v, 4))
                t2[first + x, at(r)] = (relax * s) * m

    chunks(NX // 4, 16, sweep1)

    def sweep2(first):
        for r in last:
            m = mask2[at(r)]
            for x in range(1, 17):
                v = t2[first + x, at(r)]
                s = (third(v) + relax * (f2[first + x, at(r)] + (around(t2, first + x, r) + sides(v, 4)))) * m
                e2[first + x, every_other(r), :] = s
                e2[first + x, every_other(r, 1), :] = s

    chunks(NX // 4, 16, sweep2)


def cycle_up(src, mask, f1, e2, v1, e1, v0, out, rows1, last1, rows0, last0, nd, ne):
    def correct1(first):
        for r in rows1:
            for i in range(4):
                e = e2[first + i + 1, at(r)]
                for k in (1, 2):
                    x = 2 * first + 2 * i + k
                    v1[x, at(r)] = relax * f1[x, at(r)] + e

    chunks(NX // 4, 4, correct1)

    def smooth1(first):
        for r in last1:
            m = mask[at(r)]
            for x in [first + k for k in range(1, nd + 1)]:
                v = v1[x, at(r)]
                y = v1[x, at(r, -1)] + v1[x, at(r, 1)]
                s = third(v) + relax * ((f1[x, at(r)] + (v1[x - 1, at(r)] + v1[x + 1, at(r)])) + (y + sides(v, 2)))
                e1[x, at(r)] = s * m

    chunks(NX // 2, nd, smooth1)

    def correct0(first):
        for odd in range(2):
            for r in rows0[odd]:
                for i in range(1, 33):
                    e = e1[first + i, at(r)]
                    for k in (-1, 0):
                        x = 2 * first + 2 * i + k
                        v0[x, odd, at(r)] = relax * src[x, odd, at(r)] + e

    chunks(NX // 2, 32, correct0)

    def smooth0(first):
        for odd in range(2):
            for r in last0[odd]:
                m = mask[at(r)]
                layers = [v0[first + k, odd, at(r)] for k in range(ne + 2)]
                for k in range(1, ne + 1):
                    x = first + k
                    v = layers[k]
                    y = v0[x, 1 - odd, at(r, odd - 1)] + v0[x, 1 - odd, at(r, odd)]
                    s = third(v) + relax * ((src[x, odd, at(r)] + (layers[k - 1] + layers[k + 1])) + (y + sides(v, 1)))
                    out[x, odd, at(r)] = s * m

    chunks(NX, ne, smooth0)


def images(src, first, odd, r, count):
    layers = [src[first + k, odd, at(r)] for k in range(count + 2)]
    result = []
    for k in range(1, count + 1):
        v = layers[k]
        y = src[first + k, 1 - odd, at(r, odd - 1)] + src[first + k, 1 - odd, at(r, odd)]
        result.append((v, 6.0 * v - ((layers[k - 1] + layers[k + 1]) + (y + sides(v, 1)))))
    return result


def cycles_kernel(*refs):
    pl.when(lax.axis_index("gx_1") == 0)(lambda: cycles_on_core(*refs))


def cycles_on_core(known, up, down, out, other, r0, z0, q0, w, v0, f1, v1, e1, e2, f2, t2, mask, mask2):
    gx0, _, gy, gz = place()

    def inside(count, height):
        rows, lanes = row_index((count, LANES)) - 8, lane_index((count, LANES))
        y = gy * BY - HY + height * rows
        z = (gz * 4 + z_block(gx0, gz)) * CZ - HZ + lanes
        return jnp.where((y >= 0) & (y < NY) & (z >= 0) & (z < NZ), 1.0, 0.0)

    mask[...] = inside(56, 2)
    mask2[...] = inside(40, 4)
    for ref, count in ((r0, NX), (z0, NX), (q0, NX), (w, NX), (v0, NX), (f1, NX // 2), (v1, NX // 2), (f2, NX // 4), (t2, NX // 4)):
        ref[0] = jnp.zeros(ref.shape[1:], jnp.float32)
        ref[count + 1] = jnp.zeros(ref.shape[1:], jnp.float32)
    lanes = lane_index((8, LANES))
    between = (lanes >= HZ) & (lanes < HZ + CZ)

    def corners_in(i, _):
        for odd in range(2):
            for b in range(5):
                if b == 2:
                    corners = (None,) * 4
                else:
                    part = pl.ds(BY * (b - b // 3) + 8 * odd, 8)
                    a, d = up[i, part], down[i, part]
                    one = jnp.where(lanes < 64, a, roll(d, 64, 1))
                    two = jnp.where(lanes < 64, roll(a, 64, 1), d)
                    corners = (one, roll(one, -32, 1), two, roll(two, -32, 1))
                for k, corner in enumerate(corners):
                    value = known[4 * i + k, odd, pl.ds(8 * b, 8)]
                    r0[4 * i + k + 1, odd, at(8 * b)] = value if corner is None else jnp.where(between, value, corner)
        return 0

    lax.fori_loop(0, 16, corners_in, 0, unroll=4)
    low = {step: lanes & step == 0 for step in (1, 2)}

    def fold(x, step):
        return 0.5 * (x + jnp.where(low[step], roll(x, -step, 1), roll(x, step, 1)))

    middle = (8, 16, 24)
    cycle_down(r0, mask, mask2, fold, v1, e1, f1, f2, (0, 8, 16, 24, 32), (0, 8, 12), 4, 8)
    cycle_coarse(mask2, f2, t2, e2, (0, 8, 12), (1, 9))
    cycle_up(r0, mask, f1, e2, v1, e1, v0, z0, (6, 14, 22, 26), (7, 15, 23, 25), ((8, 16, 24, 25), (7, 15, 23, 24)), (middle, middle), 32, 64)

    def image(first):
        for odd in range(2):
            for r in middle:
                m = mask[at(r)]
                for k, (_, value) in enumerate(images(z0, first, odd, r, 64)):
                    q0[first + k + 1, odd, at(r)] = value * m

    chunks(NX, 64, image)
    cycle_down(q0, mask, mask2, fold, v1, e1, f1, f2, middle, (5, 7), 8, 16)
    cycle_coarse(mask2, f2, t2, e2, (6,), (6,))
    cycle_up(q0, mask, f1, e2, v1, e1, v0, w, (14, 18), (15, 17), ((15, 17), (15, 17)), ((16, 17), (15, 16)), 32, 64)

    def sums(i, acc):
        acc = list(acc)
        for odd in range(2):
            for k, (ww, s) in enumerate(images(w, 64 * i, odd, 16, 64)):
                x = 64 * i + k + 1
                r, zz, q = r0[x, odd, at(16)], z0[x, odd, at(16)], q0[x, odd, at(16)]
                for n, term in enumerate((r * zz, zz * q, r * ww, q * ww, ww * s)):
                    acc[n] = acc[n] + term
                v0[x, odd, at(16)] = s
        return tuple(acc)

    acc = lax.fori_loop(0, NX // 64, sums, (jnp.zeros((8, LANES), jnp.float32),) * 5)

    for odd_slab, ref in enumerate((out, other)):
        for t in range(4):
            for k in range(BX):
                x = BX * (2 * t + odd_slab) + k + 1
                for odd in range(2):
                    zz, q, ww, s = (field[x, odd, at(16)] for field in (z0, q0, w, v0))
                    ref[t, pl.ds(k * BY + 8 * odd, 8)] = jnp.where(
                        lanes < 32, roll(zz, -32, 1), jnp.where(lanes < 64, q, jnp.where(lanes < 96, roll(ww, 32, 1), roll(s, 64, 1)))
                    )
    home = (lanes >= HZ) & (lanes < HZ + CZ)
    row = jnp.zeros((8, LANES), jnp.float32)
    for k, a in enumerate(acc):
        row = jnp.where(lanes == k, jnp.sum(jnp.where(home, a, 0.0)), row)
    for t in range(4):
        out[t, BX * BY : BX * BY + 8] = row
        other[t, BX * BY : BX * BY + 8] = row


def cycles(*blocks):
    fine = pltpu.VMEM((NX + 2, 2, 56, LANES), jnp.float32)
    level1 = pltpu.VMEM((NX // 2 + 2, 56, LANES), jnp.float32)
    level2 = pltpu.VMEM((NX // 4 + 2, 40, LANES), jnp.float32)
    return pl.pallas_call(
        cycles_kernel,
        out_shape=(jax.ShapeDtypeStruct((4, BX * BY + 8, LANES), jnp.float32),) * 2,
        in_specs=[VMEM] * 3,
        out_specs=(VMEM, VMEM),
        scratch_shapes=[fine] * 5
        + [level1] * 3
        + [pltpu.VMEM((NX // 4 + 2, 56, LANES), jnp.float32), level2, level2, pltpu.VMEM((56, LANES), jnp.float32), pltpu.VMEM((40, LANES), jnp.float32)],
        compiler_params=pltpu.CompilerParams(vmem_limit_bytes=30 * 1024 * 1024),
    )(*blocks)


def finish_kernel(rhs, fields, sums, solution, residual):
    total = jnp.sum(sums[...], axis=0, keepdims=True)
    lanes = lane_index(total.shape)

    def pick(k):
        return jnp.sum(jnp.where(lanes == k, total, 0.0), axis=1, keepdims=True)

    rz, zq, rw, qw, ws = (pick(k) for k in range(5))
    step0 = rz / zq
    rz1 = rz - step0 * (rw + zq) + step0 * step0 * qw
    growth = rz1 / rz
    image1 = (zq - 2.0 * step0 * qw + step0 * step0 * ws) + 2.0 * growth * (zq - step0 * qw) + growth * growth * zq
    step1 = rz1 / image1
    on_z = step0 + step1 * (1.0 + growth)
    on_w = -step1 * step0
    wide = lane_index((BY, LANES))
    gz = lax.axis_index("gz")
    for x in range(BX):
        parts = [fields[z_block(c, gz), x * BY : (x + 1) * BY] for c in range(4)]

        def field(f):
            value = None
            for c in range(4):
                part = roll(parts[c], 32 * (c - f), 1)
                value = part if c == 0 else jnp.where(wide >= 32 * c, part, value)
            return value

        z0, q0, w, s = (field(f) for f in range(4))
        u = on_z * z0 + on_w * w
        v = on_z * q0 + on_w * s
        for odd in range(2):
            rows = pl.ds(odd, 8, stride=2)
            solution[x, rows, :] = u[8 * odd : 8 * odd + 8]
            residual[x, rows, :] = rhs[x, rows, :] - v[8 * odd : 8 * odd + 8]


def finish(rhs, fields, sums):
    shape = jax.ShapeDtypeStruct((BX, BY, BZ), jnp.float32)
    return pl.pallas_call(finish_kernel, out_shape=(shape, shape), in_specs=[VMEM] * 3, out_specs=(VMEM, VMEM), compiler_params=small())(rhs, fields, sums)


def y_pairs(step):
    return [(a, 16 + a + step) for a in range(16) if 0 <= a + step < 16]


def z_pairs(step):
    def number(core, block):
        gz, at = block // 4, block % 4
        return ((at if gz % 2 == 0 else 3 - at) * 2 + core) * 8 + gz

    return [(number(1, a), number(0, a + step)) for a in range(32) if 0 <= a + step < 32]


Z_AXES = ("gx_0", "gx_1", "gz")


def local(density, x_faces, y_faces, z_faces):
    rhs, packed = make_rhs(density, x_faces, y_faces, z_faces)
    own = lax.all_to_all(packed, GX, 0, 0, tiled=True).reshape(16, BY, 128)
    moved = []
    for step in (2, -2, 1, -1):
        moved.append(lax.ppermute(own, ("gx_1", "gy"), y_pairs(step)))
    left = lax.ppermute(own, Z_AXES, z_pairs(1))
    right = lax.ppermute(own, Z_AXES, z_pairs(-1))
    rows = join(moved[0], moved[2], moved[3], moved[1])
    up = lax.ppermute(rows, Z_AXES, z_pairs(1))
    down = lax.ppermute(rows, Z_AXES, z_pairs(-1))
    rows = lax.ppermute(rows, "gx_1", [(1, 0)])
    known = unpack(own, left, right, rows)
    packed, other = cycles(known, up, down)
    other = lax.ppermute(other, "gx_1", [(0, 1)])
    packed = jnp.where(lax.axis_index("gx_1") == 1, other, packed)
    fields = lax.all_to_all(packed, "gx_0", 0, 0, tiled=True)
    sums = jnp.sum(fields[:, BX * BY, :], axis=0)
    sums = lax.all_to_all(jnp.broadcast_to(sums, (128, 1, 128)), ("gy", "gz"), 0, 0, tiled=True)
    return finish(rhs, fields, sums.reshape(128, 128))


def solution(mesh):
    torus = Mesh(mesh.devices.reshape(4, 2, mesh.shape["gy"], mesh.shape["gz"]), AXES)
    in_specs = (P(GX, "gy", "gz"), P(None, "gy", "gz"), P(None, GX, "gz"), P(None, GX, "gy"))
    out_specs = (P(GX, "gy", "gz"), P(GX, "gy", "gz"))
    return jax.shard_map(local, mesh=torus, in_specs=in_specs, out_specs=out_specs, check_vma=False)
```

```python
import jax
import jax.numpy as jnp
from jax import lax
from jax.experimental import pallas as pl
from jax.experimental.pallas import tpu as pltpu
from jax.sharding import Mesh
from jax.sharding import PartitionSpec as P


AXES = ("gx_0", "gx_1", "gy", "gz")
GX = ("gx_0", "gx_1")
NX, NY, NZ = 64, 256, 1024
BX, BY, BZ = 8, 16, 128
CZ = 32
HY, HZ = 32, 32
LANES = 128
relax = 1.0 / 9.0
coupling = 0.5
VMEM = pl.BlockSpec(memory_space=pltpu.VMEM)
HBM = pl.BlockSpec(memory_space=pltpu.MemorySpace.HBM)


def roll(x, shift, axis):
    return pltpu.roll(x, shift % x.shape[axis], axis)


def place():
    return tuple(lax.axis_index(axis) for axis in AXES)


def z_block(gx0, gz):
    return jnp.where(gz % 2 == 0, gx0, 3 - gx0)


def small(**more):
    return pltpu.CompilerParams(vmem_limit_bytes=4 * 1024 * 1024, **more)


def lane_index(shape):
    return lax.broadcasted_iota(jnp.int32, shape, 1)


def row_index(shape):
    return lax.broadcasted_iota(jnp.int32, shape, 0)


def rhs_kernel(density_in, xf_in, yf_in, zf_in, rhs, packed, scratch, density, xf, yf, zf, arrived):
    copies = [pltpu.make_async_copy(a, b, arrived.at[i]) for i, (a, b) in enumerate(((density_in, density), (xf_in, xf), (yf_in, yf), (zf_in, zf)))]
    for copy in copies:
        copy.start()
    gx0, core, gy, gz = place()
    gx = 2 * gx0 + core
    rows, lanes = row_index((BY, BZ)), lane_index((BY, BZ))
    eye = row_index((BY, BY)) == lane_index((BY, BY))
    low_y = (rows == 0) & (gy == 0)
    high_y = (rows == BY - 1) & (gy == NY // BY - 1)
    low_z = (lanes == 0) & (gz == 0)
    high_z = (lanes == BZ - 1) & (gz == NZ // BZ - 1)

    def column(row):
        return jnp.sum(jnp.where(eye, row, 0.0), axis=1, keepdims=True)

    for copy in copies:
        copy.wait()
    layers = []
    for x in range(BX):
        value = -coupling * density[x]
        if x == 0:
            value = value + jnp.where(gx == 0, xf[0], 0.0)
        if x == BX - 1:
            value = value + jnp.where(gx == NX // BX - 1, xf[1], 0.0)
        value = value + jnp.where(low_y, yf[0, x : x + 1, :], 0.0)
        value = value + jnp.where(high_y, yf[1, x : x + 1, :], 0.0)
        value = value + jnp.where(low_z, column(zf[0, x : x + 1, :]), 0.0)
        value = value + jnp.where(high_z, column(zf[1, x : x + 1, :]), 0.0)
        rhs[x] = value
        layers.append(value)
    for chunk in range(4):
        for quad in range(2):
            out = None
            for k in range(4):
                part = roll(layers[4 * quad + k], 32 * (k - chunk), 1)
                out = part if k == 0 else jnp.where(lanes >= 32 * k, part, out)
            scratch[chunk, quad] = out
    for chip in range(4):
        chunk = z_block(chip, gz)
        for quad in range(2):
            for odd in range(2):
                part = scratch[chunk, quad, pl.ds(odd, 8, stride=2), :]
                packed[2 * chip, quad, 8 * odd : 8 * odd + 8] = part
                packed[2 * chip + 1, quad, 8 * odd : 8 * odd + 8] = part


def make_rhs(density, xf, yf, zf):
    return pl.pallas_call(
        rhs_kernel,
        out_shape=(
            jax.ShapeDtypeStruct((BX, BY, BZ), jnp.float32),
            jax.ShapeDtypeStruct((8, 2, BY, BZ), jnp.float32),
        ),
        in_specs=[HBM] * 4,
        out_specs=(VMEM, VMEM),
        scratch_shapes=[pltpu.VMEM((4, 2, BY, BZ), jnp.float32)]
        + [pltpu.VMEM(a.shape, a.dtype) for a in (density, xf, yf, zf)]
        + [pltpu.SemaphoreType.DMA((4,))],
        compiler_params=pltpu.CompilerParams(vmem_limit_bytes=60 * 1024 * 1024),
    )(density, xf, yf, zf)


def join_kernel(*refs):
    out = refs[-1]
    for b, ref in enumerate(refs[:-1]):
        for i in range(16):
            out[i, BY * b : BY * b + BY] = ref[i]


def join(*blocks):
    return pl.pallas_call(
        join_kernel,
        out_shape=jax.ShapeDtypeStruct((16, 4 * BY, 128), jnp.float32),
        in_specs=[VMEM] * 4,
        out_specs=VMEM,
        compiler_params=small(),
    )(*blocks)


def unpack_kernel(*refs):
    pl.when(lax.axis_index("gx_1") == 0)(lambda: unpack_on_core(*refs))


def unpack_on_core(own, left, right, rows_, out):
    lanes = lane_index((8, LANES))
    even = lanes // 32 % 2 == 0
    for i in range(16):
        for odd in range(2):
            for b in range(4):
                c = rows_[i, pl.ds(BY * b + 8 * odd, 8)]
                for k in range(4):
                    out[4 * i + k, odd, pl.ds(8 * (b + b // 2), 8)] = roll(c, 32 - 32 * k, 1)
            part = pl.ds(8 * odd, 8)
            a, c, d = left[i, part], own[i, part], right[i, part]
            low = jnp.where(lanes < 64, a, roll(d, 64, 1))
            high = jnp.where(lanes < 64, roll(a, 64, 1), d)
            out[4 * i, odd, 16:24] = jnp.where(even, low, roll(c, 32, 1))
            out[4 * i + 1, odd, 16:24] = jnp.where(even, roll(low, -32, 1), c)
            out[4 * i + 2, odd, 16:24] = jnp.where(even, high, roll(c, -32, 1))
            out[4 * i + 3, odd, 16:24] = jnp.where(even, roll(high, -32, 1), roll(c, 64, 1))


def unpack(own, left, right, rows):
    return pl.pallas_call(
        unpack_kernel,
        out_shape=jax.ShapeDtypeStruct((NX, 2, 40, LANES), jnp.float32),
        in_specs=[VMEM] * 4,
        out_specs=VMEM,
        compiler_params=small(),
    )(own, left, right, rows)


def at(row, step=0):
    return pl.ds(8 + row + step, 8)


def every_other(row, step=0):
    return pl.ds(8 + 2 * row + step, 8, stride=2)


def sides(x, step):
    return roll(x, step, 1) + roll(x, -step, 1)


def third(x):
    return x * (1.0 / 3.0)


def chunks(count, size, body):
    size, unroll = size if isinstance(size, tuple) else (size, 1)
    if size == count:
        body(0)
    elif size * unroll == count:
        for i in range(unroll):
            body(i * size)
    else:
        lax.fori_loop(0, count // size, lambda i, _: body(i * size) or 0, 0, unroll=unroll)


def cycle_down(src, mask, mask2, fold, outer, sum1, part1, f1, f2, rows1, rows2, size, nb):
    def gather(first, size=size):
        for r in rows1:
            layers = [2 * first + k for k in range(2 * size + 2)]
            cells = [src[x, 0, at(r)] + src[x, 1, at(r)] for x in layers]
            beyond = [src[x, 1, at(r, -1)] + src[x, 0, at(r, 1)] for x in layers[1:-1]]
            for i in range(size):
                before, a, b, after = cells[2 * i : 2 * i + 4]
                u = a + b
                y = beyond[2 * i] + beyond[2 * i + 1]
                sum1[first + i + 1, at(r)] = u
                part1[first + i + 1, at(r)] = third(u) + relax * (((u + u) + (before + after)) + y)

    chunks(NX // 2, size, gather)

    def across(first):
        for r in rows1:
            for x in [first + k for k in range(1, 32 + 1)]:
                f1[x, at(r)] = part1[x, at(r)] + relax * (sum1[x, at(r)] + outer(sum1[x, at(r)], 1))

    chunks(NX // 2, 32, across)

    def level1(first):
        for r in rows1:
            m = mask[at(r)]
            for x in [first + k for k in range(1, 16 + 1)]:
                f1[x, at(r)] = fold(f1[x, at(r)], 1) * m

    chunks(NX // 2, 16, level1)

    def level2(first):
        for r in rows2:
            m = mask2[at(r)]
            layers = [2 * first + k for k in range(2 * nb + 2)]
            cells = [f1[x, every_other(r), :] + f1[x, every_other(r, 1), :] for x in layers]
            beyond = [f1[x, every_other(r, -1), :] + f1[x, every_other(r, 2), :] for x in layers[1:-1]]
            for i in range(nb):
                before, a, b, after = cells[2 * i : 2 * i + 4]
                u = a + b
                y = beyond[2 * i] + beyond[2 * i + 1]
                s = third(u) + relax * (((u + u) + (before + after)) + (y + (u + outer(u, 2))))
                f2[first + i + 1, at(r)] = fold(s, 2) * m

    chunks(NX // 4, nb, level2)


def cycle_coarse(mask2, f2, t2, e2, rows, last):
    def around(ref, x, r):
        return (ref[x - 1, at(r)] + ref[x + 1, at(r)]) + (ref[x, at(r, -1)] + ref[x, at(r, 1)])

    def sweep1(first):
        for r in rows:
            m = mask2[at(r)]
            for x in range(1, 17):
                v = f2[first + x, at(r)]
                s = (4.0 / 3.0) * v + relax * (around(f2, first + x, r) + sides(v, 4))
                t2[first + x, at(r)] = (relax * s) * m

    chunks(NX // 4, 16, sweep1)

    def sweep2(first):
        for r in last:
            m = mask2[at(r)]
            for x in range(1, 17):
                v = t2[first + x, at(r)]
                s = (third(v) + relax * (f2[first + x, at(r)] + (around(t2, first + x, r) + sides(v, 4)))) * m
                e2[first + x, every_other(r), :] = s
                e2[first + x, every_other(r, 1), :] = s

    chunks(NX // 4, 16, sweep2)


def cycle_up(src, mask, f1, e2, v1, e1, v0, out, rows1, last1, rows0, last0, nd, ne):
    def correct1(first):
        for r in rows1:
            for i in range(4):
                e = e2[first + i + 1, at(r)]
                for k in (1, 2):
                    x = 2 * first + 2 * i + k
                    v1[x, at(r)] = relax * f1[x, at(r)] + e

    chunks(NX // 4, 4, correct1)

    def smooth1(first):
        for r in last1:
            m = mask[at(r)]
            for x in [first + k for k in range(1, nd + 1)]:
                v = v1[x, at(r)]
                y = v1[x, at(r, -1)] + v1[x, at(r, 1)]
                s = third(v) + relax * ((f1[x, at(r)] + (v1[x - 1, at(r)] + v1[x + 1, at(r)])) + (y + sides(v, 2)))
                e1[x, at(r)] = s * m

    chunks(NX // 2, nd, smooth1)

    def correct0(first):
        for odd in range(2):
            for r in rows0[odd]:
                for i in range(1, 33):
                    e = e1[first + i, at(r)]
                    for k in (-1, 0):
                        x = 2 * first + 2 * i + k
                        v0[x, odd, at(r)] = relax * src[x, odd, at(r)] + e

    chunks(NX // 2, 32, correct0)

    def smooth0(first):
        for odd in range(2):
            for r in last0[odd]:
                m = mask[at(r)]
                layers = [v0[first + k, odd, at(r)] for k in range(ne + 2)]
                for k in range(1, ne + 1):
                    x = first + k
                    v = layers[k]
                    y = v0[x, 1 - odd, at(r, odd - 1)] + v0[x, 1 - odd, at(r, odd)]
                    s = third(v) + relax * ((src[x, odd, at(r)] + (layers[k - 1] + layers[k + 1])) + (y + sides(v, 1)))
                    out[x, odd, at(r)] = s * m

    chunks(NX, ne, smooth0)


def images(src, first, odd, r, count):
    layers = [src[first + k, odd, at(r)] for k in range(count + 2)]
    result = []
    for k in range(1, count + 1):
        v = layers[k]
        y = src[first + k, 1 - odd, at(r, odd - 1)] + src[first + k, 1 - odd, at(r, odd)]
        result.append((v, 6.0 * v - ((layers[k - 1] + layers[k + 1]) + (y + sides(v, 1)))))
    return result


def cycles_kernel(*refs):
    pl.when(lax.axis_index("gx_1") == 0)(lambda: cycles_on_core(*refs))


def cycles_on_core(known, up, down, out, other, r0, z0, q0, w, v0, f1, v1, e1, e2, f2, t2, mask, mask2):
    gx0, _, gy, gz = place()

    def inside(count, height):
        rows, lanes = row_index((count, LANES)) - 8, lane_index((count, LANES))
        y = gy * BY - HY + height * rows
        z = (gz * 4 + z_block(gx0, gz)) * CZ - HZ + lanes
        return jnp.where((y >= 0) & (y < NY) & (z >= 0) & (z < NZ), 1.0, 0.0)

    mask[...] = inside(56, 2)
    mask2[...] = inside(40, 4)
    for ref, count in ((r0, NX), (z0, NX), (q0, NX), (w, NX), (v0, NX), (f1, NX // 2), (v1, NX // 2), (f2, NX // 4), (t2, NX // 4)):
        ref[0] = jnp.zeros(ref.shape[1:], jnp.float32)
        ref[count + 1] = jnp.zeros(ref.shape[1:], jnp.float32)
    lanes = lane_index((8, LANES))
    between = (lanes >= HZ) & (lanes < HZ + CZ)

    def corners_in(i, _):
        for odd in range(2):
            for b in range(5):
                if b == 2:
                    corners = (None,) * 4
                else:
                    part = pl.ds(BY * (b - b // 3) + 8 * odd, 8)
                    a, d = up[i, part], down[i, part]
                    one = jnp.where(lanes < 64, a, roll(d, 64, 1))
                    two = jnp.where(lanes < 64, roll(a, 64, 1), d)
                    corners = (one, roll(one, -32, 1), two, roll(two, -32, 1))
                for k, corner in enumerate(corners):
                    value = known[4 * i + k, odd, pl.ds(8 * b, 8)]
                    r0[4 * i + k + 1, odd, at(8 * b)] = value if corner is None else jnp.where(between, value, corner)
        return 0

    lax.fori_loop(0, 16, corners_in, 0, unroll=4)
    partner = {step: lanes ^ step for step in (1, 2)}
    outside = {step: (lanes + jnp.where(lanes & step == 0, -step, step)) & 127 for step in (1, 2)}

    def fold(x, step):
        return 0.5 * (x + jnp.take_along_axis(x, partner[step], axis=1))

    def outer(x, step):
        return jnp.take_along_axis(x, outside[step], axis=1)

    middle = (8, 16, 24)
    cycle_down(r0, mask, mask2, fold, outer, v1, e1, f1, f2, (0, 8, 16, 24, 32), (0, 8, 12), 4, 8)
    cycle_coarse(mask2, f2, t2, e2, (0, 8, 12), (1, 9))
    cycle_up(r0, mask, f1, e2, v1, e1, v0, z0, (6, 14, 22, 26), (7, 15, 23, 25), ((8, 16, 24, 25), (7, 15, 23, 24)), (middle, middle), 32, 64)

    def image(first):
        for odd in range(2):
            for r in middle:
                m = mask[at(r)]
                for k, (_, value) in enumerate(images(z0, first, odd, r, 64)):
                    q0[first + k + 1, odd, at(r)] = value * m

    chunks(NX, 64, image)
    cycle_down(q0, mask, mask2, fold, outer, v1, e1, f1, f2, middle, (5, 7), 8, 16)
    cycle_coarse(mask2, f2, t2, e2, (6,), (6,))
    cycle_up(q0, mask, f1, e2, v1, e1, v0, w, (14, 18), (15, 17), ((15, 17), (15, 17)), ((16, 17), (15, 16)), 32, 64)

    def sums(i, acc):
        acc = list(acc)
        for odd in range(2):
            for k, (ww, s) in enumerate(images(w, 64 * i, odd, 16, 64)):
                x = 64 * i + k + 1
                r, zz, q = r0[x, odd, at(16)], z0[x, odd, at(16)], q0[x, odd, at(16)]
                for n, term in enumerate((r * zz, zz * q, r * ww, q * ww, ww * s)):
                    acc[n] = acc[n] + term
                v0[x, odd, at(16)] = s
        return tuple(acc)

    acc = lax.fori_loop(0, NX // 64, sums, (jnp.zeros((8, LANES), jnp.float32),) * 5)

    for odd_slab, ref in enumerate((out, other)):
        for t in range(4):
            for k in range(BX):
                x = BX * (2 * t + odd_slab) + k + 1
                for odd in range(2):
                    zz, q, ww, s = (field[x, odd, at(16)] for field in (z0, q0, w, v0))
                    ref[t, pl.ds(k * BY + 8 * odd, 8)] = jnp.where(
                        lanes < 32, roll(zz, -32, 1), jnp.where(lanes < 64, q, jnp.where(lanes < 96, roll(ww, 32, 1), roll(s, 64, 1)))
                    )
    home = (lanes >= HZ) & (lanes < HZ + CZ)
    row = jnp.zeros((8, LANES), jnp.float32)
    for k, a in enumerate(acc):
        row = jnp.where(lanes == k, jnp.sum(jnp.where(home, a, 0.0)), row)
    for t in range(4):
        out[t, BX * BY : BX * BY + 8] = row
        other[t, BX * BY : BX * BY + 8] = row


def cycles(*blocks):
    fine = pltpu.VMEM((NX + 2, 2, 56, LANES), jnp.float32)
    level1 = pltpu.VMEM((NX // 2 + 2, 56, LANES), jnp.float32)
    level2 = pltpu.VMEM((NX // 4 + 2, 40, LANES), jnp.float32)
    return pl.pallas_call(
        cycles_kernel,
        out_shape=(jax.ShapeDtypeStruct((4, BX * BY + 8, LANES), jnp.float32),) * 2,
        in_specs=[VMEM] * 3,
        out_specs=(VMEM, VMEM),
        scratch_shapes=[fine] * 5
        + [level1] * 3
        + [pltpu.VMEM((NX // 4 + 2, 56, LANES), jnp.float32), level2, level2, pltpu.VMEM((56, LANES), jnp.float32), pltpu.VMEM((40, LANES), jnp.float32)],
        compiler_params=pltpu.CompilerParams(vmem_limit_bytes=30 * 1024 * 1024),
    )(*blocks)


def finish_kernel(rhs, fields, sums, solution, residual):
    total = jnp.sum(sums[...], axis=0, keepdims=True)
    lanes = lane_index(total.shape)

    def pick(k):
        return jnp.sum(jnp.where(lanes == k, total, 0.0), axis=1, keepdims=True)

    rz, zq, rw, qw, ws = (pick(k) for k in range(5))
    step0 = rz / zq
    rz1 = rz - step0 * (rw + zq) + step0 * step0 * qw
    growth = rz1 / rz
    image1 = (zq - 2.0 * step0 * qw + step0 * step0 * ws) + 2.0 * growth * (zq - step0 * qw) + growth * growth * zq
    step1 = rz1 / image1
    on_z = step0 + step1 * (1.0 + growth)
    on_w = -step1 * step0
    wide = lane_index((BY, LANES))
    gz = lax.axis_index("gz")
    for x in range(BX):
        parts = [fields[z_block(c, gz), x * BY : (x + 1) * BY] for c in range(4)]

        def field(f):
            value = None
            for c in range(4):
                part = roll(parts[c], 32 * (c - f), 1)
                value = part if c == 0 else jnp.where(wide >= 32 * c, part, value)
            return value

        z0, q0, w, s = (field(f) for f in range(4))
        u = on_z * z0 + on_w * w
        v = on_z * q0 + on_w * s
        for odd in range(2):
            rows = pl.ds(odd, 8, stride=2)
            solution[x, rows, :] = u[8 * odd : 8 * odd + 8]
            residual[x, rows, :] = rhs[x, rows, :] - v[8 * odd : 8 * odd + 8]


def finish(rhs, fields, sums):
    shape = jax.ShapeDtypeStruct((BX, BY, BZ), jnp.float32)
    return pl.pallas_call(finish_kernel, out_shape=(shape, shape), in_specs=[VMEM] * 3, out_specs=(VMEM, VMEM), compiler_params=small())(rhs, fields, sums)


def y_pairs(step):
    return [(a, 16 + a + step) for a in range(16) if 0 <= a + step < 16]


def z_pairs(step):
    def number(core, block):
        gz, at = block // 4, block % 4
        return ((at if gz % 2 == 0 else 3 - at) * 2 + core) * 8 + gz

    return [(number(1, a), number(0, a + step)) for a in range(32) if 0 <= a + step < 32]


Z_AXES = ("gx_0", "gx_1", "gz")


def local(density, x_faces, y_faces, z_faces):
    rhs, packed = make_rhs(density, x_faces, y_faces, z_faces)
    own = lax.all_to_all(packed, GX, 0, 0, tiled=True).reshape(16, BY, 128)
    moved = []
    for step in (2, -2, 1, -1):
        moved.append(lax.ppermute(own, ("gx_1", "gy"), y_pairs(step)))
    left = lax.ppermute(own, Z_AXES, z_pairs(1))
    right = lax.ppermute(own, Z_AXES, z_pairs(-1))
    rows = join(moved[0], moved[2], moved[3], moved[1])
    up = lax.ppermute(rows, Z_AXES, z_pairs(1))
    down = lax.ppermute(rows, Z_AXES, z_pairs(-1))
    rows = lax.ppermute(rows, "gx_1", [(1, 0)])
    known = unpack(own, left, right, rows)
    packed, other = cycles(known, up, down)
    other = lax.all_gather(other, "gx_1")
    packed = jnp.where(lax.axis_index("gx_1") == 1, other[0], packed)
    fields = lax.all_to_all(packed, "gx_0", 0, 0, tiled=True)
    sums = jnp.sum(fields[:, BX * BY, :], axis=0)
    sums = lax.all_to_all(jnp.broadcast_to(sums, (128, 1, 128)), ("gy", "gz"), 0, 0, tiled=True)
    return finish(rhs, fields, sums.reshape(128, 128))


def solution(mesh):
    torus = Mesh(mesh.devices.reshape(4, 2, mesh.shape["gy"], mesh.shape["gz"]), AXES)
    in_specs = (P(GX, "gy", "gz"), P(None, "gy", "gz"), P(None, GX, "gz"), P(None, GX, "gy"))
    out_specs = (P(GX, "gy", "gz"), P(GX, "gy", "gz"))
    return jax.shard_map(local, mesh=torus, in_specs=in_specs, out_specs=out_specs, check_vma=False)
```

```python
import jax
import jax.numpy as jnp
from jax import lax
from jax.experimental import pallas as pl
from jax.experimental.pallas import tpu as pltpu
from jax.sharding import Mesh
from jax.sharding import PartitionSpec as P


AXES = ("gx_0", "gx_1", "gy", "gz")
GX = ("gx_0", "gx_1")
NX, NY, NZ = 64, 256, 1024
BX, BY, BZ = 8, 16, 128
CZ = 32
HY, HZ = 32, 32
LANES = 128
relax = 1.0 / 9.0
coupling = 0.5
VMEM = pl.BlockSpec(memory_space=pltpu.VMEM)
HBM = pl.BlockSpec(memory_space=pltpu.MemorySpace.HBM)


def roll(x, shift, axis):
    return pltpu.roll(x, shift % x.shape[axis], axis)


def place():
    return tuple(lax.axis_index(axis) for axis in AXES)


def z_block(gx0, gz):
    return jnp.where(gz % 2 == 0, gx0, 3 - gx0)


def small(**more):
    return pltpu.CompilerParams(vmem_limit_bytes=4 * 1024 * 1024, **more)


def lane_index(shape):
    return lax.broadcasted_iota(jnp.int32, shape, 1)


def row_index(shape):
    return lax.broadcasted_iota(jnp.int32, shape, 0)


def rhs_kernel(density_in, xf_in, yf_in, zf_in, rhs, packed, scratch, density, xf, yf, zf, arrived):
    copies = [pltpu.make_async_copy(a, b, arrived.at[i]) for i, (a, b) in enumerate(((density_in, density), (xf_in, xf), (yf_in, yf), (zf_in, zf)))]
    for copy in copies:
        copy.start()
    gx0, core, gy, gz = place()
    gx = 2 * gx0 + core
    rows, lanes = row_index((BY, BZ)), lane_index((BY, BZ))
    eye = row_index((BY, BY)) == lane_index((BY, BY))
    low_y = (rows == 0) & (gy == 0)
    high_y = (rows == BY - 1) & (gy == NY // BY - 1)
    low_z = (lanes == 0) & (gz == 0)
    high_z = (lanes == BZ - 1) & (gz == NZ // BZ - 1)

    def column(row):
        return jnp.sum(jnp.where(eye, row, 0.0), axis=1, keepdims=True)

    for copy in copies:
        copy.wait()
    layers = []
    for x in range(BX):
        value = -coupling * density[x]
        if x == 0:
            value = value + jnp.where(gx == 0, xf[0], 0.0)
        if x == BX - 1:
            value = value + jnp.where(gx == NX // BX - 1, xf[1], 0.0)
        value = value + jnp.where(low_y, yf[0, x : x + 1, :], 0.0)
        value = value + jnp.where(high_y, yf[1, x : x + 1, :], 0.0)
        value = value + jnp.where(low_z, column(zf[0, x : x + 1, :]), 0.0)
        value = value + jnp.where(high_z, column(zf[1, x : x + 1, :]), 0.0)
        rhs[x] = value
        layers.append(value)
    for chunk in range(4):
        for quad in range(2):
            out = None
            for k in range(4):
                part = roll(layers[4 * quad + k], 32 * (k - chunk), 1)
                out = part if k == 0 else jnp.where(lanes >= 32 * k, part, out)
            scratch[chunk, quad] = out
    for chip in range(4):
        chunk = z_block(chip, gz)
        for quad in range(2):
            for odd in range(2):
                part = scratch[chunk, quad, pl.ds(odd, 8, stride=2), :]
                packed[2 * chip, quad, 8 * odd : 8 * odd + 8] = part
                packed[2 * chip + 1, quad, 8 * odd : 8 * odd + 8] = part


def make_rhs(density, xf, yf, zf):
    return pl.pallas_call(
        rhs_kernel,
        out_shape=(
            jax.ShapeDtypeStruct((BX, BY, BZ), jnp.float32),
            jax.ShapeDtypeStruct((8, 2, BY, BZ), jnp.float32),
        ),
        in_specs=[HBM] * 4,
        out_specs=(VMEM, VMEM),
        scratch_shapes=[pltpu.VMEM((4, 2, BY, BZ), jnp.float32)]
        + [pltpu.VMEM(a.shape, a.dtype) for a in (density, xf, yf, zf)]
        + [pltpu.SemaphoreType.DMA((4,))],
        compiler_params=pltpu.CompilerParams(vmem_limit_bytes=60 * 1024 * 1024),
    )(density, xf, yf, zf)


def join_kernel(*refs):
    out = refs[-1]
    for b, ref in enumerate(refs[:-1]):
        for i in range(16):
            out[i, BY * b : BY * b + BY] = ref[i]


def join(*blocks):
    return pl.pallas_call(
        join_kernel,
        out_shape=jax.ShapeDtypeStruct((16, 4 * BY, 128), jnp.float32),
        in_specs=[VMEM] * 4,
        out_specs=VMEM,
        compiler_params=small(),
    )(*blocks)


def unpack_kernel(*refs):
    pl.when(lax.axis_index("gx_1") == 0)(lambda: unpack_on_core(*refs))


def unpack_on_core(own, left, right, rows_, out):
    lanes = lane_index((8, LANES))
    even = lanes // 32 % 2 == 0
    for i in range(16):
        for odd in range(2):
            for b in range(4):
                c = rows_[i, pl.ds(BY * b + 8 * odd, 8)]
                for k in range(4):
                    out[4 * i + k, odd, pl.ds(8 * (b + b // 2), 8)] = roll(c, 32 - 32 * k, 1)
            part = pl.ds(8 * odd, 8)
            a, c, d = left[i, part], own[i, part], right[i, part]
            low = jnp.where(lanes < 64, a, roll(d, 64, 1))
            high = jnp.where(lanes < 64, roll(a, 64, 1), d)
            out[4 * i, odd, 16:24] = jnp.where(even, low, roll(c, 32, 1))
            out[4 * i + 1, odd, 16:24] = jnp.where(even, roll(low, -32, 1), c)
            out[4 * i + 2, odd, 16:24] = jnp.where(even, high, roll(c, -32, 1))
            out[4 * i + 3, odd, 16:24] = jnp.where(even, roll(high, -32, 1), roll(c, 64, 1))


def unpack(own, left, right, rows):
    return pl.pallas_call(
        unpack_kernel,
        out_shape=jax.ShapeDtypeStruct((NX, 2, 40, LANES), jnp.float32),
        in_specs=[VMEM] * 4,
        out_specs=VMEM,
        compiler_params=small(),
    )(own, left, right, rows)


def at(row, step=0):
    return pl.ds(8 + row + step, 8)


def every_other(row, step=0):
    return pl.ds(8 + 2 * row + step, 8, stride=2)


def sides(x, step):
    return roll(x, step, 1) + roll(x, -step, 1)


def third(x):
    return x * (1.0 / 3.0)


def chunks(count, size, body):
    size, unroll = size if isinstance(size, tuple) else (size, 1)
    if size == count:
        body(0)
    elif size * unroll == count:
        for i in range(unroll):
            body(i * size)
    else:
        lax.fori_loop(0, count // size, lambda i, _: body(i * size) or 0, 0, unroll=unroll)


def cycle_down(src, mask, mask2, fold, outer, sum1, part1, f1, f2, rows1, rows2, size, nb):
    def gather(first, size=size):
        for r in rows1:
            layers = [2 * first + k for k in range(2 * size + 2)]
            cells = [src[x, 0, at(r)] + src[x, 1, at(r)] for x in layers]
            beyond = [src[x, 1, at(r, -1)] + src[x, 0, at(r, 1)] for x in layers[1:-1]]
            for i in range(size):
                before, a, b, after = cells[2 * i : 2 * i + 4]
                u = a + b
                y = beyond[2 * i] + beyond[2 * i + 1]
                sum1[first + i + 1, at(r)] = u
                part1[first + i + 1, at(r)] = third(u) + relax * (((u + u) + (before + after)) + y)

    chunks(NX // 2, size, gather)

    def across(first):
        for r in rows1:
            for x in [first + k for k in range(1, 32 + 1)]:
                f1[x, at(r)] = part1[x, at(r)] + relax * (sum1[x, at(r)] + outer(sum1[x, at(r)], 1))

    chunks(NX // 2, 32, across)

    def level1(first):
        for r in rows1:
            m = mask[at(r)]
            for x in [first + k for k in range(1, 32 + 1)]:
                f1[x, at(r)] = fold(f1[x, at(r)], 1) * m

    chunks(NX // 2, 32, level1)

    def level2(first):
        for r in rows2:
            m = mask2[at(r)]
            layers = [2 * first + k for k in range(2 * nb + 2)]
            cells = [f1[x, every_other(r), :] + f1[x, every_other(r, 1), :] for x in layers]
            beyond = [f1[x, every_other(r, -1), :] + f1[x, every_other(r, 2), :] for x in layers[1:-1]]
            for i in range(nb):
                before, a, b, after = cells[2 * i : 2 * i + 4]
                u = a + b
                y = beyond[2 * i] + beyond[2 * i + 1]
                s = third(u) + relax * (((u + u) + (before + after)) + (y + (u + outer(u, 2))))
                f2[first + i + 1, at(r)] = fold(s, 2) * m

    chunks(NX // 4, nb, level2)


def cycle_coarse(mask2, f2, t2, e2, rows, last):
    def around(ref, x, r):
        return (ref[x - 1, at(r)] + ref[x + 1, at(r)]) + (ref[x, at(r, -1)] + ref[x, at(r, 1)])

    def sweep1(first):
        for r in rows:
            m = mask2[at(r)]
            for x in range(1, 17):
                v = f2[first + x, at(r)]
                s = (4.0 / 3.0) * v + relax * (around(f2, first + x, r) + sides(v, 4))
                t2[first + x, at(r)] = (relax * s) * m

    chunks(NX // 4, 16, sweep1)

    def sweep2(first):
        for r in last:
            m = mask2[at(r)]
            for x in range(1, 17):
                v = t2[first + x, at(r)]
                s = (third(v) + relax * (f2[first + x, at(r)] + (around(t2, first + x, r) + sides(v, 4)))) * m
                e2[first + x, every_other(r), :] = s
                e2[first + x, every_other(r, 1), :] = s

    chunks(NX // 4, 16, sweep2)


def cycle_up(src, mask, f1, e2, v1, e1, v0, out, rows1, last1, rows0, last0, nd, ne):
    def correct1(first):
        for r in rows1:
            for i in range(4):
                e = e2[first + i + 1, at(r)]
                for k in (1, 2):
                    x = 2 * first + 2 * i + k
                    v1[x, at(r)] = relax * f1[x, at(r)] + e

    chunks(NX // 4, 4, correct1)

    def smooth1(first):
        for r in last1:
            m = mask[at(r)]
            for x in [first + k for k in range(1, nd + 1)]:
                v = v1[x, at(r)]
                y = v1[x, at(r, -1)] + v1[x, at(r, 1)]
                s = third(v) + relax * ((f1[x, at(r)] + (v1[x - 1, at(r)] + v1[x + 1, at(r)])) + (y + sides(v, 2)))
                e1[x, at(r)] = s * m

    chunks(NX // 2, nd, smooth1)

    def correct0(first):
        for odd in range(2):
            for r in rows0[odd]:
                for i in range(1, 33):
                    e = e1[first + i, at(r)]
                    for k in (-1, 0):
                        x = 2 * first + 2 * i + k
                        v0[x, odd, at(r)] = relax * src[x, odd, at(r)] + e

    chunks(NX // 2, 32, correct0)

    def smooth0(first):
        for odd in range(2):
            for r in last0[odd]:
                m = mask[at(r)]
                layers = [v0[first + k, odd, at(r)] for k in range(ne + 2)]
                for k in range(1, ne + 1):
                    x = first + k
                    v = layers[k]
                    y = v0[x, 1 - odd, at(r, odd - 1)] + v0[x, 1 - odd, at(r, odd)]
                    s = third(v) + relax * ((src[x, odd, at(r)] + (layers[k - 1] + layers[k + 1])) + (y + sides(v, 1)))
                    out[x, odd, at(r)] = s * m

    chunks(NX, ne, smooth0)


def images(src, first, odd, r, count):
    layers = [src[first + k, odd, at(r)] for k in range(count + 2)]
    result = []
    for k in range(1, count + 1):
        v = layers[k]
        y = src[first + k, 1 - odd, at(r, odd - 1)] + src[first + k, 1 - odd, at(r, odd)]
        result.append((v, 6.0 * v - ((layers[k - 1] + layers[k + 1]) + (y + sides(v, 1)))))
    return result


def cycles_kernel(*refs):
    pl.when(lax.axis_index("gx_1") == 0)(lambda: cycles_on_core(*refs))


def cycles_on_core(known, up, down, out, other, r0, z0, q0, w, v0, f1, v1, e1, e2, f2, t2, mask, mask2):
    gx0, _, gy, gz = place()

    def inside(count, height):
        rows, lanes = row_index((count, LANES)) - 8, lane_index((count, LANES))
        y = gy * BY - HY + height * rows
        z = (gz * 4 + z_block(gx0, gz)) * CZ - HZ + lanes
        return jnp.where((y >= 0) & (y < NY) & (z >= 0) & (z < NZ), 1.0, 0.0)

    mask[...] = inside(56, 2)
    mask2[...] = inside(40, 4)
    for ref, count in ((r0, NX), (z0, NX), (q0, NX), (w, NX), (v0, NX), (f1, NX // 2), (v1, NX // 2), (f2, NX // 4), (t2, NX // 4)):
        ref[0] = jnp.zeros(ref.shape[1:], jnp.float32)
        ref[count + 1] = jnp.zeros(ref.shape[1:], jnp.float32)
    lanes = lane_index((8, LANES))
    between = (lanes >= HZ) & (lanes < HZ + CZ)

    def corners_in(i, _):
        for odd in range(2):
            for b in range(5):
                if b == 2:
                    corners = (None,) * 4
                else:
                    part = pl.ds(BY * (b - b // 3) + 8 * odd, 8)
                    a, d = up[i, part], down[i, part]
                    one = jnp.where(lanes < 64, a, roll(d, 64, 1))
                    two = jnp.where(lanes < 64, roll(a, 64, 1), d)
                    corners = (one, roll(one, -32, 1), two, roll(two, -32, 1))
                for k, corner in enumerate(corners):
                    value = known[4 * i + k, odd, pl.ds(8 * b, 8)]
                    r0[4 * i + k + 1, odd, at(8 * b)] = value if corner is None else jnp.where(between, value, corner)
        return 0

    lax.fori_loop(0, 16, corners_in, 0, unroll=4)
    partner = {step: lanes ^ step for step in (1, 2)}
    outside = {step: (lanes + jnp.where(lanes & step == 0, -step, step)) & 127 for step in (1, 2)}

    def fold(x, step):
        return 0.5 * (x + jnp.take_along_axis(x, partner[step], axis=1))

    def outer(x, step):
        return jnp.take_along_axis(x, outside[step], axis=1)

    middle = (8, 16, 24)
    cycle_down(r0, mask, mask2, fold, outer, v1, e1, f1, f2, (0, 8, 16, 24, 32), (0, 8, 12), 8, 8)
    cycle_coarse(mask2, f2, t2, e2, (0, 8, 12), (1, 9))
    cycle_up(r0, mask, f1, e2, v1, e1, v0, z0, (6, 14, 22, 26), (7, 15, 23, 25), ((8, 16, 24, 25), (7, 15, 23, 24)), (middle, middle), 32, 64)

    def image(first):
        for odd in range(2):
            for r in middle:
                m = mask[at(r)]
                for k, (_, value) in enumerate(images(z0, first, odd, r, 64)):
                    q0[first + k + 1, odd, at(r)] = value * m

    chunks(NX, 64, image)
    cycle_down(q0, mask, mask2, fold, outer, v1, e1, f1, f2, middle, (5, 7), 8, 16)
    cycle_coarse(mask2, f2, t2, e2, (6,), (6,))
    cycle_up(q0, mask, f1, e2, v1, e1, v0, w, (14, 18), (15, 17), ((15, 17), (15, 17)), ((16, 17), (15, 16)), 32, 64)

    def sums(i, acc):
        acc = list(acc)
        for odd in range(2):
            for k, (ww, s) in enumerate(images(w, 64 * i, odd, 16, 64)):
                x = 64 * i + k + 1
                r, zz, q = r0[x, odd, at(16)], z0[x, odd, at(16)], q0[x, odd, at(16)]
                for n, term in enumerate((r * zz, zz * q, r * ww, q * ww, ww * s)):
                    acc[n] = acc[n] + term
                v0[x, odd, at(16)] = s
        return tuple(acc)

    acc = lax.fori_loop(0, NX // 64, sums, (jnp.zeros((8, LANES), jnp.float32),) * 5)

    for odd_slab, ref in enumerate((out, other)):
        for t in range(4):
            for k in range(BX):
                x = BX * (2 * t + odd_slab) + k + 1
                for odd in range(2):
                    zz, q, ww, s = (field[x, odd, at(16)] for field in (z0, q0, w, v0))
                    ref[t, pl.ds(k * BY + 8 * odd, 8)] = jnp.where(
                        lanes < 32, roll(zz, -32, 1), jnp.where(lanes < 64, q, jnp.where(lanes < 96, roll(ww, 32, 1), roll(s, 64, 1)))
                    )
    home = (lanes >= HZ) & (lanes < HZ + CZ)
    row = jnp.zeros((8, LANES), jnp.float32)
    for k, a in enumerate(acc):
        row = jnp.where(lanes == k, jnp.sum(jnp.where(home, a, 0.0)), row)
    for t in range(4):
        out[t, BX * BY : BX * BY + 8] = row
        other[t, BX * BY : BX * BY + 8] = row


def cycles(*blocks):
    fine = pltpu.VMEM((NX + 2, 2, 56, LANES), jnp.float32)
    level1 = pltpu.VMEM((NX // 2 + 2, 56, LANES), jnp.float32)
    level2 = pltpu.VMEM((NX // 4 + 2, 40, LANES), jnp.float32)
    return pl.pallas_call(
        cycles_kernel,
        out_shape=(jax.ShapeDtypeStruct((4, BX * BY + 8, LANES), jnp.float32),) * 2,
        in_specs=[VMEM] * 3,
        out_specs=(VMEM, VMEM),
        scratch_shapes=[fine] * 5
        + [level1] * 3
        + [pltpu.VMEM((NX // 4 + 2, 56, LANES), jnp.float32), level2, level2, pltpu.VMEM((56, LANES), jnp.float32), pltpu.VMEM((40, LANES), jnp.float32)],
        compiler_params=pltpu.CompilerParams(vmem_limit_bytes=30 * 1024 * 1024),
    )(*blocks)


def finish_kernel(rhs, fields, sums, solution, residual):
    total = jnp.sum(sums[...], axis=0, keepdims=True)
    lanes = lane_index(total.shape)

    def pick(k):
        return jnp.sum(jnp.where(lanes == k, total, 0.0), axis=1, keepdims=True)

    rz, zq, rw, qw, ws = (pick(k) for k in range(5))
    step0 = rz / zq
    rz1 = rz - step0 * (rw + zq) + step0 * step0 * qw
    growth = rz1 / rz
    image1 = (zq - 2.0 * step0 * qw + step0 * step0 * ws) + 2.0 * growth * (zq - step0 * qw) + growth * growth * zq
    step1 = rz1 / image1
    on_z = step0 + step1 * (1.0 + growth)
    on_w = -step1 * step0
    wide = lane_index((BY, LANES))
    gz = lax.axis_index("gz")
    for x in range(BX):
        parts = [fields[z_block(c, gz), x * BY : (x + 1) * BY] for c in range(4)]

        def field(f):
            value = None
            for c in range(4):
                part = roll(parts[c], 32 * (c - f), 1)
                value = part if c == 0 else jnp.where(wide >= 32 * c, part, value)
            return value

        z0, q0, w, s = (field(f) for f in range(4))
        u = on_z * z0 + on_w * w
        v = on_z * q0 + on_w * s
        for odd in range(2):
            rows = pl.ds(odd, 8, stride=2)
            solution[x, rows, :] = u[8 * odd : 8 * odd + 8]
            residual[x, rows, :] = rhs[x, rows, :] - v[8 * odd : 8 * odd + 8]


def finish(rhs, fields, sums):
    shape = jax.ShapeDtypeStruct((BX, BY, BZ), jnp.float32)
    return pl.pallas_call(finish_kernel, out_shape=(shape, shape), in_specs=[VMEM] * 3, out_specs=(VMEM, VMEM), compiler_params=small())(rhs, fields, sums)


def y_pairs(step):
    return [(a, 16 + a + step) for a in range(16) if 0 <= a + step < 16]


def z_pairs(step):
    def number(core, block):
        gz, at = block // 4, block % 4
        return ((at if gz % 2 == 0 else 3 - at) * 2 + core) * 8 + gz

    return [(number(1, a), number(0, a + step)) for a in range(32) if 0 <= a + step < 32]


Z_AXES = ("gx_0", "gx_1", "gz")


def local(density, x_faces, y_faces, z_faces):
    rhs, packed = make_rhs(density, x_faces, y_faces, z_faces)
    own = lax.all_to_all(packed, GX, 0, 0, tiled=True).reshape(16, BY, 128)
    moved = []
    for step in (2, -2, 1, -1):
        moved.append(lax.ppermute(own, ("gx_1", "gy"), y_pairs(step)))
    left = lax.ppermute(own, Z_AXES, z_pairs(1))
    right = lax.ppermute(own, Z_AXES, z_pairs(-1))
    rows = join(moved[0], moved[2], moved[3], moved[1])
    up = lax.ppermute(rows, Z_AXES, z_pairs(1))
    down = lax.ppermute(rows, Z_AXES, z_pairs(-1))
    rows = lax.ppermute(rows, "gx_1", [(1, 0)])
    known = unpack(own, left, right, rows)
    packed, other = cycles(known, up, down)
    other = lax.all_gather(other, "gx_1")
    packed = jnp.where(lax.axis_index("gx_1") == 1, other[0], packed)
    fields = lax.all_to_all(packed, "gx_0", 0, 0, tiled=True)
    sums = jnp.sum(fields[:, BX * BY, :], axis=0)
    sums = lax.all_to_all(jnp.broadcast_to(sums, (128, 1, 128)), ("gy", "gz"), 0, 0, tiled=True)
    return finish(rhs, fields, sums.reshape(128, 128))


def solution(mesh):
    torus = Mesh(mesh.devices.reshape(4, 2, mesh.shape["gy"], mesh.shape["gz"]), AXES)
    in_specs = (P(GX, "gy", "gz"), P(None, "gy", "gz"), P(None, GX, "gz"), P(None, GX, "gy"))
    out_specs = (P(GX, "gy", "gz"), P(GX, "gy", "gz"))
    return jax.shard_map(local, mesh=torus, in_specs=in_specs, out_specs=out_specs, check_vma=False)
```

```python
import jax
import jax.numpy as jnp
from jax import lax
from jax.experimental import pallas as pl
from jax.experimental.pallas import tpu as pltpu
from jax.sharding import Mesh
from jax.sharding import PartitionSpec as P


AXES = ("gx_0", "gx_1", "gy", "gz")
GX = ("gx_0", "gx_1")
NX, NY, NZ = 64, 256, 1024
BX, BY, BZ = 8, 16, 128
CZ = 32
HY, HZ = 32, 32
LANES = 128
relax = 1.0 / 9.0
coupling = 0.5
VMEM = pl.BlockSpec(memory_space=pltpu.VMEM)
HBM = pl.BlockSpec(memory_space=pltpu.MemorySpace.HBM)


def roll(x, shift, axis):
    return pltpu.roll(x, shift % x.shape[axis], axis)


def place():
    return tuple(lax.axis_index(axis) for axis in AXES)


def z_block(gx0, gz):
    return jnp.where(gz % 2 == 0, gx0, 3 - gx0)


def small(**more):
    return pltpu.CompilerParams(vmem_limit_bytes=4 * 1024 * 1024, **more)


def lane_index(shape):
    return lax.broadcasted_iota(jnp.int32, shape, 1)


def row_index(shape):
    return lax.broadcasted_iota(jnp.int32, shape, 0)


def rhs_kernel(density_in, xf_in, yf_in, zf_in, rhs, packed, scratch, density, xf, yf, zf, arrived):
    copies = [pltpu.make_async_copy(a, b, arrived.at[i]) for i, (a, b) in enumerate(((density_in, density), (xf_in, xf), (yf_in, yf), (zf_in, zf)))]
    for copy in copies:
        copy.start()
    gx0, core, gy, gz = place()
    gx = 2 * gx0 + core
    rows, lanes = row_index((BY, BZ)), lane_index((BY, BZ))
    eye = row_index((BY, BY)) == lane_index((BY, BY))
    low_y = (rows == 0) & (gy == 0)
    high_y = (rows == BY - 1) & (gy == NY // BY - 1)
    low_z = (lanes == 0) & (gz == 0)
    high_z = (lanes == BZ - 1) & (gz == NZ // BZ - 1)

    def column(row):
        return jnp.sum(jnp.where(eye, row, 0.0), axis=1, keepdims=True)

    for copy in copies:
        copy.wait()
    for x in range(BX):
        value = -coupling * density[x]
        if x == 0:
            value = value + jnp.where(gx == 0, xf[0], 0.0)
        if x == BX - 1:
            value = value + jnp.where(gx == NX // BX - 1, xf[1], 0.0)
        value = value + jnp.where(low_y, yf[0, x : x + 1, :], 0.0)
        rhs[x] = value + jnp.where(high_y, yf[1, x : x + 1, :], 0.0)

    @pl.when((gz == 0) | (gz == NZ // BZ - 1))
    def _():
        for x in range(BX):
            value = rhs[x] + jnp.where(low_z, column(zf[0, x : x + 1, :]), 0.0)
            rhs[x] = value + jnp.where(high_z, column(zf[1, x : x + 1, :]), 0.0)

    layers = [rhs[x] for x in range(BX)]
    for chunk in range(4):
        for quad in range(2):
            out = None
            for k in range(4):
                part = roll(layers[4 * quad + k], 32 * (k - chunk), 1)
                out = part if k == 0 else jnp.where(lanes >= 32 * k, part, out)
            scratch[chunk, quad] = out
    for chip in range(4):
        chunk = z_block(chip, gz)
        for quad in range(2):
            for odd in range(2):
                part = scratch[chunk, quad, pl.ds(odd, 8, stride=2), :]
                packed[2 * chip, quad, 8 * odd : 8 * odd + 8] = part
                packed[2 * chip + 1, quad, 8 * odd : 8 * odd + 8] = part


def make_rhs(density, xf, yf, zf):
    return pl.pallas_call(
        rhs_kernel,
        out_shape=(
            jax.ShapeDtypeStruct((BX, BY, BZ), jnp.float32),
            jax.ShapeDtypeStruct((8, 2, BY, BZ), jnp.float32),
        ),
        in_specs=[HBM] * 4,
        out_specs=(VMEM, VMEM),
        scratch_shapes=[pltpu.VMEM((4, 2, BY, BZ), jnp.float32)]
        + [pltpu.VMEM(a.shape, a.dtype) for a in (density, xf, yf, zf)]
        + [pltpu.SemaphoreType.DMA((4,))],
        compiler_params=pltpu.CompilerParams(vmem_limit_bytes=60 * 1024 * 1024),
    )(density, xf, yf, zf)


def join_kernel(*refs):
    out = refs[-1]
    for b, ref in enumerate(refs[:-1]):
        for i in range(16):
            out[i, BY * b : BY * b + BY] = ref[i]


def join(*blocks):
    return pl.pallas_call(
        join_kernel,
        out_shape=jax.ShapeDtypeStruct((16, 4 * BY, 128), jnp.float32),
        in_specs=[VMEM] * 4,
        out_specs=VMEM,
        compiler_params=small(),
    )(*blocks)


def unpack_kernel(*refs):
    pl.when(lax.axis_index("gx_1") == 0)(lambda: unpack_on_core(*refs))


def unpack_on_core(own, left, right, rows_, out):
    lanes = lane_index((8, LANES))
    even = lanes // 32 % 2 == 0
    for i in range(16):
        for odd in range(2):
            for b in range(4):
                c = rows_[i, pl.ds(BY * b + 8 * odd, 8)]
                for k in range(4):
                    out[4 * i + k, odd, pl.ds(8 * (b + b // 2), 8)] = roll(c, 32 - 32 * k, 1)
            part = pl.ds(8 * odd, 8)
            a, c, d = left[i, part], own[i, part], right[i, part]
            low = jnp.where(lanes < 64, a, roll(d, 64, 1))
            high = jnp.where(lanes < 64, roll(a, 64, 1), d)
            out[4 * i, odd, 16:24] = jnp.where(even, low, roll(c, 32, 1))
            out[4 * i + 1, odd, 16:24] = jnp.where(even, roll(low, -32, 1), c)
            out[4 * i + 2, odd, 16:24] = jnp.where(even, high, roll(c, -32, 1))
            out[4 * i + 3, odd, 16:24] = jnp.where(even, roll(high, -32, 1), roll(c, 64, 1))


def unpack(own, left, right, rows):
    return pl.pallas_call(
        unpack_kernel,
        out_shape=jax.ShapeDtypeStruct((NX, 2, 40, LANES), jnp.float32),
        in_specs=[VMEM] * 4,
        out_specs=VMEM,
        compiler_params=small(),
    )(own, left, right, rows)


def at(row, step=0):
    return pl.ds(8 + row + step, 8)


def every_other(row, step=0):
    return pl.ds(8 + 2 * row + step, 8, stride=2)


def sides(x, step):
    return roll(x, step, 1) + roll(x, -step, 1)


def third(x):
    return x * (1.0 / 3.0)


def chunks(count, size, body):
    size, unroll = size if isinstance(size, tuple) else (size, 1)
    if size == count:
        body(0)
    elif size * unroll == count:
        for i in range(unroll):
            body(i * size)
    else:
        lax.fori_loop(0, count // size, lambda i, _: body(i * size) or 0, 0, unroll=unroll)


def cycle_down(src, mask, mask2, fold, outer, sum1, part1, f1, f2, rows1, rows2, size, nb):
    def gather(first, size=size):
        for r in rows1:
            layers = [2 * first + k for k in range(2 * size + 2)]
            cells = [src[x, 0, at(r)] + src[x, 1, at(r)] for x in layers]
            beyond = [src[x, 1, at(r, -1)] + src[x, 0, at(r, 1)] for x in layers[1:-1]]
            for i in range(size):
                before, a, b, after = cells[2 * i : 2 * i + 4]
                u = a + b
                y = beyond[2 * i] + beyond[2 * i + 1]
                sum1[first + i + 1, at(r)] = u
                part1[first + i + 1, at(r)] = third(u) + relax * (((u + u) + (before + after)) + y)

    chunks(NX // 2, size, gather)

    def across(first):
        for r in rows1:
            for x in [first + k for k in range(1, 32 + 1)]:
                f1[x, at(r)] = part1[x, at(r)] + relax * (sum1[x, at(r)] + outer(sum1[x, at(r)], 1))

    chunks(NX // 2, 32, across)

    def level1(first):
        for r in rows1:
            m = mask[at(r)]
            for x in [first + k for k in range(1, 32 + 1)]:
                f1[x, at(r)] = fold(f1[x, at(r)], 1) * m

    chunks(NX // 2, 32, level1)

    def level2(first):
        for r in rows2:
            m = mask2[at(r)]
            layers = [2 * first + k for k in range(2 * nb + 2)]
            cells = [f1[x, every_other(r), :] + f1[x, every_other(r, 1), :] for x in layers]
            beyond = [f1[x, every_other(r, -1), :] + f1[x, every_other(r, 2), :] for x in layers[1:-1]]
            for i in range(nb):
                before, a, b, after = cells[2 * i : 2 * i + 4]
                u = a + b
                y = beyond[2 * i] + beyond[2 * i + 1]
                s = third(u) + relax * (((u + u) + (before + after)) + (y + (u + outer(u, 2))))
                f2[first + i + 1, at(r)] = fold(s, 2) * m

    chunks(NX // 4, nb, level2)


def cycle_coarse(mask2, f2, t2, e2, rows, last):
    def around(ref, x, r):
        return (ref[x - 1, at(r)] + ref[x + 1, at(r)]) + (ref[x, at(r, -1)] + ref[x, at(r, 1)])

    def sweep1(first):
        for r in rows:
            m = mask2[at(r)]
            for x in range(1, 17):
                v = f2[first + x, at(r)]
                s = (4.0 / 3.0) * v + relax * (around(f2, first + x, r) + sides(v, 4))
                t2[first + x, at(r)] = (relax * s) * m

    chunks(NX // 4, 16, sweep1)

    def sweep2(first):
        for r in last:
            m = mask2[at(r)]
            for x in range(1, 17):
                v = t2[first + x, at(r)]
                s = (third(v) + relax * (f2[first + x, at(r)] + (around(t2, first + x, r) + sides(v, 4)))) * m
                e2[first + x, every_other(r), :] = s
                e2[first + x, every_other(r, 1), :] = s

    chunks(NX // 4, 16, sweep2)


def cycle_up(src, mask, f1, e2, v1, e1, v0, out, rows1, last1, rows0, last0, nd, ne):
    def correct1(first):
        for r in rows1:
            for i in range(4):
                e = e2[first + i + 1, at(r)]
                for k in (1, 2):
                    x = 2 * first + 2 * i + k
                    v1[x, at(r)] = relax * f1[x, at(r)] + e

    chunks(NX // 4, 4, correct1)

    def smooth1(first):
        for r in last1:
            m = mask[at(r)]
            for x in [first + k for k in range(1, nd + 1)]:
                v = v1[x, at(r)]
                y = v1[x, at(r, -1)] + v1[x, at(r, 1)]
                s = third(v) + relax * ((f1[x, at(r)] + (v1[x - 1, at(r)] + v1[x + 1, at(r)])) + (y + sides(v, 2)))
                e1[x, at(r)] = s * m

    chunks(NX // 2, nd, smooth1)

    def correct0(first):
        for odd in range(2):
            for r in rows0[odd]:
                for i in range(1, 33):
                    e = e1[first + i, at(r)]
                    for k in (-1, 0):
                        x = 2 * first + 2 * i + k
                        v0[x, odd, at(r)] = relax * src[x, odd, at(r)] + e

    chunks(NX // 2, 32, correct0)

    def smooth0(first):
        for odd in range(2):
            for r in last0[odd]:
                m = mask[at(r)]
                layers = [v0[first + k, odd, at(r)] for k in range(ne + 2)]
                for k in range(1, ne + 1):
                    x = first + k
                    v = layers[k]
                    y = v0[x, 1 - odd, at(r, odd - 1)] + v0[x, 1 - odd, at(r, odd)]
                    s = third(v) + relax * ((src[x, odd, at(r)] + (layers[k - 1] + layers[k + 1])) + (y + sides(v, 1)))
                    out[x, odd, at(r)] = s * m

    chunks(NX, ne, smooth0)


def images(src, first, odd, r, count):
    layers = [src[first + k, odd, at(r)] for k in range(count + 2)]
    result = []
    for k in range(1, count + 1):
        v = layers[k]
        y = src[first + k, 1 - odd, at(r, odd - 1)] + src[first + k, 1 - odd, at(r, odd)]
        result.append((v, 6.0 * v - ((layers[k - 1] + layers[k + 1]) + (y + sides(v, 1)))))
    return result


def cycles_kernel(*refs):
    pl.when(lax.axis_index("gx_1") == 0)(lambda: cycles_on_core(*refs))


def cycles_on_core(known, up, down, out, other, r0, z0, q0, w, v0, f1, v1, e1, e2, f2, t2, mask, mask2):
    gx0, _, gy, gz = place()

    def inside(count, height):
        rows, lanes = row_index((count, LANES)) - 8, lane_index((count, LANES))
        y = gy * BY - HY + height * rows
        z = (gz * 4 + z_block(gx0, gz)) * CZ - HZ + lanes
        return jnp.where((y >= 0) & (y < NY) & (z >= 0) & (z < NZ), 1.0, 0.0)

    mask[...] = inside(56, 2)
    mask2[...] = inside(40, 4)
    for ref, count in ((r0, NX), (z0, NX), (q0, NX), (w, NX), (v0, NX), (f1, NX // 2), (v1, NX // 2), (f2, NX // 4), (t2, NX // 4)):
        ref[0] = jnp.zeros(ref.shape[1:], jnp.float32)
        ref[count + 1] = jnp.zeros(ref.shape[1:], jnp.float32)
    lanes = lane_index((8, LANES))
    between = (lanes >= HZ) & (lanes < HZ + CZ)

    def corners_in(i, _):
        for odd in range(2):
            for b in range(5):
                if b == 2:
                    corners = (None,) * 4
                else:
                    part = pl.ds(BY * (b - b // 3) + 8 * odd, 8)
                    a, d = up[i, part], down[i, part]
                    one = jnp.where(lanes < 64, a, roll(d, 64, 1))
                    two = jnp.where(lanes < 64, roll(a, 64, 1), d)
                    corners = (one, roll(one, -32, 1), two, roll(two, -32, 1))
                for k, corner in enumerate(corners):
                    value = known[4 * i + k, odd, pl.ds(8 * b, 8)]
                    r0[4 * i + k + 1, odd, at(8 * b)] = value if corner is None else jnp.where(between, value, corner)
        return 0

    lax.fori_loop(0, 16, corners_in, 0, unroll=4)
    partner = {step: lanes ^ step for step in (1, 2)}
    outside = {step: (lanes + jnp.where(lanes & step == 0, -step, step)) & 127 for step in (1, 2)}

    def fold(x, step):
        return 0.5 * (x + jnp.take_along_axis(x, partner[step], axis=1))

    def outer(x, step):
        return jnp.take_along_axis(x, outside[step], axis=1)

    middle = (8, 16, 24)
    cycle_down(r0, mask, mask2, fold, outer, v1, e1, f1, f2, (0, 8, 16, 24, 32), (0, 8, 12), 8, 8)
    cycle_coarse(mask2, f2, t2, e2, (0, 8, 12), (1, 9))
    cycle_up(r0, mask, f1, e2, v1, e1, v0, z0, (6, 14, 22, 26), (7, 15, 23, 25), ((8, 16, 24, 25), (7, 15, 23, 24)), (middle, middle), 32, 64)

    def image(first):
        for odd in range(2):
            for r in middle:
                m = mask[at(r)]
                for k, (_, value) in enumerate(images(z0, first, odd, r, 64)):
                    q0[first + k + 1, odd, at(r)] = value * m

    chunks(NX, 64, image)
    cycle_down(q0, mask, mask2, fold, outer, v1, e1, f1, f2, middle, (5, 7), 8, 16)
    cycle_coarse(mask2, f2, t2, e2, (6,), (6,))
    cycle_up(q0, mask, f1, e2, v1, e1, v0, w, (14, 18), (15, 17), ((15, 17), (15, 17)), ((16, 17), (15, 16)), 32, 64)

    def sums(i, acc):
        acc = list(acc)
        for odd in range(2):
            for k, (ww, s) in enumerate(images(w, 64 * i, odd, 16, 64)):
                x = 64 * i + k + 1
                r, zz, q = r0[x, odd, at(16)], z0[x, odd, at(16)], q0[x, odd, at(16)]
                for n, term in enumerate((r * zz, zz * q, r * ww, q * ww, ww * s)):
                    acc[n] = acc[n] + term
                v0[x, odd, at(16)] = s
        return tuple(acc)

    acc = lax.fori_loop(0, NX // 64, sums, (jnp.zeros((8, LANES), jnp.float32),) * 5)

    for odd_slab, ref in enumerate((out, other)):
        for t in range(4):
            for k in range(BX):
                x = BX * (2 * t + odd_slab) + k + 1
                for odd in range(2):
                    zz, q, ww, s = (field[x, odd, at(16)] for field in (z0, q0, w, v0))
                    ref[t, pl.ds(k * BY + 8 * odd, 8)] = jnp.where(
                        lanes < 32, roll(zz, -32, 1), jnp.where(lanes < 64, q, jnp.where(lanes < 96, roll(ww, 32, 1), roll(s, 64, 1)))
                    )
    home = (lanes >= HZ) & (lanes < HZ + CZ)
    row = jnp.zeros((8, LANES), jnp.float32)
    for k, a in enumerate(acc):
        row = jnp.where(lanes == k, jnp.sum(jnp.where(home, a, 0.0)), row)
    for t in range(4):
        out[t, BX * BY : BX * BY + 8] = row
        other[t, BX * BY : BX * BY + 8] = row


def cycles(*blocks):
    fine = pltpu.VMEM((NX + 2, 2, 56, LANES), jnp.float32)
    level1 = pltpu.VMEM((NX // 2 + 2, 56, LANES), jnp.float32)
    level2 = pltpu.VMEM((NX // 4 + 2, 40, LANES), jnp.float32)
    return pl.pallas_call(
        cycles_kernel,
        out_shape=(jax.ShapeDtypeStruct((4, BX * BY + 8, LANES), jnp.float32),) * 2,
        in_specs=[VMEM] * 3,
        out_specs=(VMEM, VMEM),
        scratch_shapes=[fine] * 5
        + [level1] * 3
        + [pltpu.VMEM((NX // 4 + 2, 56, LANES), jnp.float32), level2, level2, pltpu.VMEM((56, LANES), jnp.float32), pltpu.VMEM((40, LANES), jnp.float32)],
        compiler_params=pltpu.CompilerParams(vmem_limit_bytes=30 * 1024 * 1024),
    )(*blocks)


def finish_kernel(rhs, fields, sums, solution, residual):
    total = jnp.sum(sums[...], axis=0, keepdims=True)
    lanes = lane_index(total.shape)

    def pick(k):
        return jnp.sum(jnp.where(lanes == k, total, 0.0), axis=1, keepdims=True)

    rz, zq, rw, qw, ws = (pick(k) for k in range(5))
    step0 = rz / zq
    rz1 = rz - step0 * (rw + zq) + step0 * step0 * qw
    growth = rz1 / rz
    image1 = (zq - 2.0 * step0 * qw + step0 * step0 * ws) + 2.0 * growth * (zq - step0 * qw) + growth * growth * zq
    step1 = rz1 / image1
    on_z = step0 + step1 * (1.0 + growth)
    on_w = -step1 * step0
    wide = lane_index((BY, LANES))
    even = wide // 32 % 2 == 0
    scale = jnp.where(wide < 64, on_z, on_w)
    gz = lax.axis_index("gz")

    def pair(a, b):
        return jnp.where(wide < 64, a, b) + roll(jnp.where(wide < 64, b, a), 64, 1)

    for x in range(BX):
        parts = [scale * fields[z_block(c, gz), x * BY : (x + 1) * BY] for c in range(4)]
        one, two = pair(parts[0], parts[2]), pair(parts[1], parts[3])
        u = jnp.where(even, one, roll(two, 32, 1))
        v = jnp.where(even, roll(one, -32, 1), two)
        for odd in range(2):
            rows = pl.ds(odd, 8, stride=2)
            solution[x, rows, :] = u[8 * odd : 8 * odd + 8]
            residual[x, rows, :] = rhs[x, rows, :] - v[8 * odd : 8 * odd + 8]


def finish(rhs, fields, sums):
    shape = jax.ShapeDtypeStruct((BX, BY, BZ), jnp.float32)
    return pl.pallas_call(finish_kernel, out_shape=(shape, shape), in_specs=[VMEM] * 3, out_specs=(VMEM, VMEM), compiler_params=small())(rhs, fields, sums)


def y_pairs(step):
    return [(a, 16 + a + step) for a in range(16) if 0 <= a + step < 16]


def z_pairs(step):
    def number(core, block):
        gz, at = block // 4, block % 4
        return ((at if gz % 2 == 0 else 3 - at) * 2 + core) * 8 + gz

    return [(number(1, a), number(0, a + step)) for a in range(32) if 0 <= a + step < 32]


Z_AXES = ("gx_0", "gx_1", "gz")


def local(density, x_faces, y_faces, z_faces):
    rhs, packed = make_rhs(density, x_faces, y_faces, z_faces)
    own = lax.all_to_all(packed, GX, 0, 0, tiled=True).reshape(16, BY, 128)
    moved = []
    for step in (2, -2, 1, -1):
        moved.append(lax.ppermute(own, ("gx_1", "gy"), y_pairs(step)))
    left = lax.ppermute(own, Z_AXES, z_pairs(1))
    right = lax.ppermute(own, Z_AXES, z_pairs(-1))
    rows = join(moved[0], moved[2], moved[3], moved[1])
    up = lax.ppermute(rows, Z_AXES, z_pairs(1))
    down = lax.ppermute(rows, Z_AXES, z_pairs(-1))
    rows = lax.ppermute(rows, "gx_1", [(1, 0)])
    known = unpack(own, left, right, rows)
    packed, other = cycles(known, up, down)
    other = lax.all_gather(other, "gx_1")
    packed = jnp.where(lax.axis_index("gx_1") == 1, other[0], packed)
    fields = lax.all_to_all(packed, "gx_0", 0, 0, tiled=True)
    sums = jnp.sum(fields[:, BX * BY, :], axis=0)
    sums = lax.all_to_all(jnp.broadcast_to(sums, (128, 1, 128)), ("gy", "gz"), 0, 0, tiled=True)
    return finish(rhs, fields, sums.reshape(128, 128))


def solution(mesh):
    torus = Mesh(mesh.devices.reshape(4, 2, mesh.shape["gy"], mesh.shape["gz"]), AXES)
    in_specs = (P(GX, "gy", "gz"), P(None, "gy", "gz"), P(None, GX, "gz"), P(None, GX, "gy"))
    out_specs = (P(GX, "gy", "gz"), P(GX, "gy", "gz"))
    return jax.shard_map(local, mesh=torus, in_specs=in_specs, out_specs=out_specs, check_vma=False)
```

```python
import jax
import jax.numpy as jnp
from jax import lax
from jax.experimental import pallas as pl
from jax.experimental.pallas import tpu as pltpu
from jax.sharding import Mesh
from jax.sharding import PartitionSpec as P


AXES = ("gx_0", "gx_1", "gy", "gz")
GX = ("gx_0", "gx_1")
NX, NY, NZ = 64, 256, 1024
BX, BY, BZ = 8, 16, 128
CZ = 32
HY, HZ = 32, 32
LANES = 128
relax = 1.0 / 9.0
coupling = 0.5
VMEM = pl.BlockSpec(memory_space=pltpu.VMEM)
HBM = pl.BlockSpec(memory_space=pltpu.MemorySpace.HBM)


def roll(x, shift, axis):
    return pltpu.roll(x, shift % x.shape[axis], axis)


def place():
    return tuple(lax.axis_index(axis) for axis in AXES)


def z_block(gx0, gz):
    return jnp.where(gz % 2 == 0, gx0, 3 - gx0)


def small(**more):
    return pltpu.CompilerParams(vmem_limit_bytes=4 * 1024 * 1024, **more)


def lane_index(shape):
    return lax.broadcasted_iota(jnp.int32, shape, 1)


def row_index(shape):
    return lax.broadcasted_iota(jnp.int32, shape, 0)


def rhs_kernel(density_in, xf_in, yf_in, zf_in, rhs, packed, scratch, density, xf, yf, zf, arrived):
    copies = [pltpu.make_async_copy(a, b, arrived.at[i]) for i, (a, b) in enumerate(((density_in, density), (xf_in, xf), (yf_in, yf), (zf_in, zf)))]
    for copy in copies:
        copy.start()
    gx0, core, gy, gz = place()
    gx = 2 * gx0 + core
    rows, lanes = row_index((BY, BZ)), lane_index((BY, BZ))
    eye = row_index((BY, BY)) == lane_index((BY, BY))
    low_y = (rows == 0) & (gy == 0)
    high_y = (rows == BY - 1) & (gy == NY // BY - 1)
    low_z = (lanes == 0) & (gz == 0)
    high_z = (lanes == BZ - 1) & (gz == NZ // BZ - 1)

    def column(row):
        return jnp.sum(jnp.where(eye, row, 0.0), axis=1, keepdims=True)

    for copy in copies:
        copy.wait()
    for x in range(BX):
        value = -coupling * density[x]
        if x == 0:
            value = value + jnp.where(gx == 0, xf[0], 0.0)
        if x == BX - 1:
            value = value + jnp.where(gx == NX // BX - 1, xf[1], 0.0)
        value = value + jnp.where(low_y, yf[0, x : x + 1, :], 0.0)
        rhs[x] = value + jnp.where(high_y, yf[1, x : x + 1, :], 0.0)

    @pl.when((gz == 0) | (gz == NZ // BZ - 1))
    def _():
        for x in range(BX):
            value = rhs[x] + jnp.where(low_z, column(zf[0, x : x + 1, :]), 0.0)
            rhs[x] = value + jnp.where(high_z, column(zf[1, x : x + 1, :]), 0.0)

    layers = [rhs[x] for x in range(BX)]
    for chunk in range(4):
        for quad in range(2):
            out = None
            for k in range(4):
                part = roll(layers[4 * quad + k], 32 * (k - chunk), 1)
                out = part if k == 0 else jnp.where(lanes >= 32 * k, part, out)
            scratch[chunk, quad] = out
    for chip in range(4):
        chunk = z_block(chip, gz)
        for quad in range(2):
            for odd in range(2):
                part = scratch[chunk, quad, pl.ds(odd, 8, stride=2), :]
                packed[2 * chip, quad, 8 * odd : 8 * odd + 8] = part
                packed[2 * chip + 1, quad, 8 * odd : 8 * odd + 8] = part


def make_rhs(density, xf, yf, zf):
    return pl.pallas_call(
        rhs_kernel,
        out_shape=(
            jax.ShapeDtypeStruct((BX, BY, BZ), jnp.float32),
            jax.ShapeDtypeStruct((8, 2, BY, BZ), jnp.float32),
        ),
        in_specs=[HBM] * 4,
        out_specs=(VMEM, VMEM),
        scratch_shapes=[pltpu.VMEM((4, 2, BY, BZ), jnp.float32)]
        + [pltpu.VMEM(a.shape, a.dtype) for a in (density, xf, yf, zf)]
        + [pltpu.SemaphoreType.DMA((4,))],
        compiler_params=pltpu.CompilerParams(vmem_limit_bytes=60 * 1024 * 1024),
    )(density, xf, yf, zf)


def join_kernel(*refs):
    out = refs[-1]
    for b, ref in enumerate(refs[:-1]):
        for i in range(16):
            out[i, BY * b : BY * b + BY] = ref[i]


def join(*blocks):
    return pl.pallas_call(
        join_kernel,
        out_shape=jax.ShapeDtypeStruct((16, 4 * BY, 128), jnp.float32),
        in_specs=[VMEM] * 4,
        out_specs=VMEM,
        compiler_params=small(),
    )(*blocks)


def unpack_kernel(*refs):
    pl.when(lax.axis_index("gx_1") == 0)(lambda: unpack_on_core(*refs))


def unpack_on_core(own, left, right, rows_, out):
    lanes = lane_index((8, LANES))
    even = lanes // 32 % 2 == 0
    for i in range(16):
        for odd in range(2):
            for b in range(4):
                c = rows_[i, pl.ds(BY * b + 8 * odd, 8)]
                for k in range(4):
                    out[4 * i + k, odd, pl.ds(8 * (b + b // 2), 8)] = roll(c, 32 - 32 * k, 1)
            part = pl.ds(8 * odd, 8)
            a, c, d = left[i, part], own[i, part], right[i, part]
            low = jnp.where(lanes < 64, a, roll(d, 64, 1))
            high = jnp.where(lanes < 64, roll(a, 64, 1), d)
            out[4 * i, odd, 16:24] = jnp.where(even, low, roll(c, 32, 1))
            out[4 * i + 1, odd, 16:24] = jnp.where(even, roll(low, -32, 1), c)
            out[4 * i + 2, odd, 16:24] = jnp.where(even, high, roll(c, -32, 1))
            out[4 * i + 3, odd, 16:24] = jnp.where(even, roll(high, -32, 1), roll(c, 64, 1))


def unpack(own, left, right, rows):
    return pl.pallas_call(
        unpack_kernel,
        out_shape=jax.ShapeDtypeStruct((NX, 2, 40, LANES), jnp.float32),
        in_specs=[VMEM] * 4,
        out_specs=VMEM,
        compiler_params=small(),
    )(own, left, right, rows)


def at(row, step=0):
    return pl.ds(8 + row + step, 8)


def every_other(row, step=0):
    return pl.ds(8 + 2 * row + step, 8, stride=2)


def sides(x, step):
    return roll(x, step, 1) + roll(x, -step, 1)


def third(x):
    return x * (1.0 / 3.0)


def chunks(count, size, body):
    size, unroll = size if isinstance(size, tuple) else (size, 1)
    if size == count:
        body(0)
    elif size * unroll == count:
        for i in range(unroll):
            body(i * size)
    else:
        lax.fori_loop(0, count // size, lambda i, _: body(i * size) or 0, 0, unroll=unroll)


def cycle_down(src, mask, mask2, fold, outer, sum1, part1, f1, f2, rows1, rows2, size, nb):
    def gather(first, size=size):
        for r in rows1:
            layers = [2 * first + k for k in range(2 * size + 2)]
            cells = [src[x, 0, at(r)] + src[x, 1, at(r)] for x in layers]
            beyond = [src[x, 1, at(r, -1)] + src[x, 0, at(r, 1)] for x in layers[1:-1]]
            for i in range(size):
                before, a, b, after = cells[2 * i : 2 * i + 4]
                u = a + b
                y = beyond[2 * i] + beyond[2 * i + 1]
                sum1[first + i + 1, at(r)] = u
                part1[first + i + 1, at(r)] = third(u) + relax * (((u + u) + (before + after)) + y)

    chunks(NX // 2, size, gather)

    def across(first):
        for r in rows1:
            for x in [first + k for k in range(1, 32 + 1)]:
                f1[x, at(r)] = part1[x, at(r)] + relax * (sum1[x, at(r)] + outer(sum1[x, at(r)], 1))

    chunks(NX // 2, 32, across)

    def level1(first):
        for r in rows1:
            m = mask[at(r)]
            for x in [first + k for k in range(1, 32 + 1)]:
                f1[x, at(r)] = fold(f1[x, at(r)], 1) * m

    chunks(NX // 2, 32, level1)

    def level2(first):
        for r in rows2:
            m = mask2[at(r)]
            layers = [2 * first + k for k in range(2 * nb + 2)]
            cells = [f1[x, every_other(r), :] + f1[x, every_other(r, 1), :] for x in layers]
            beyond = [f1[x, every_other(r, -1), :] + f1[x, every_other(r, 2), :] for x in layers[1:-1]]
            for i in range(nb):
                before, a, b, after = cells[2 * i : 2 * i + 4]
                u = a + b
                y = beyond[2 * i] + beyond[2 * i + 1]
                s = third(u) + relax * (((u + u) + (before + after)) + (y + (u + outer(u, 2))))
                f2[first + i + 1, at(r)] = fold(s, 2) * m

    chunks(NX // 4, nb, level2)


def cycle_coarse(mask2, f2, t2, e2, rows, last):
    def around(ref, x, r):
        return (ref[x - 1, at(r)] + ref[x + 1, at(r)]) + (ref[x, at(r, -1)] + ref[x, at(r, 1)])

    def sweep1(first):
        for r in rows:
            m = mask2[at(r)]
            for x in range(1, 17):
                v = f2[first + x, at(r)]
                s = (4.0 / 3.0) * v + relax * (around(f2, first + x, r) + sides(v, 4))
                t2[first + x, at(r)] = (relax * s) * m

    chunks(NX // 4, 16, sweep1)

    def sweep2(first):
        for r in last:
            m = mask2[at(r)]
            for x in range(1, 17):
                v = t2[first + x, at(r)]
                s = (third(v) + relax * (f2[first + x, at(r)] + (around(t2, first + x, r) + sides(v, 4)))) * m
                e2[first + x, every_other(r), :] = s
                e2[first + x, every_other(r, 1), :] = s

    chunks(NX // 4, 16, sweep2)


def cycle_up(src, mask, f1, e2, v1, e1, v0, out, rows1, last1, rows0, last0, nd, ne):
    def correct1(first):
        for r in rows1:
            for i in range(4):
                e = e2[first + i + 1, at(r)]
                for k in (1, 2):
                    x = 2 * first + 2 * i + k
                    v1[x, at(r)] = relax * f1[x, at(r)] + e

    chunks(NX // 4, 4, correct1)

    def smooth1(first):
        for r in last1:
            m = mask[at(r)]
            for x in [first + k for k in range(1, nd + 1)]:
                v = v1[x, at(r)]
                y = v1[x, at(r, -1)] + v1[x, at(r, 1)]
                s = third(v) + relax * ((f1[x, at(r)] + (v1[x - 1, at(r)] + v1[x + 1, at(r)])) + (y + sides(v, 2)))
                e1[x, at(r)] = s * m

    chunks(NX // 2, nd, smooth1)

    def correct0(first):
        for odd in range(2):
            for r in rows0[odd]:
                for i in range(1, 33):
                    e = e1[first + i, at(r)]
                    for k in (-1, 0):
                        x = 2 * first + 2 * i + k
                        v0[x, odd, at(r)] = relax * src[x, odd, at(r)] + e

    chunks(NX // 2, 32, correct0)

    def smooth0(first):
        for odd in range(2):
            for r in last0[odd]:
                m = mask[at(r)]
                layers = [v0[first + k, odd, at(r)] for k in range(ne + 2)]
                for k in range(1, ne + 1):
                    x = first + k
                    v = layers[k]
                    y = v0[x, 1 - odd, at(r, odd - 1)] + v0[x, 1 - odd, at(r, odd)]
                    s = third(v) + relax * ((src[x, odd, at(r)] + (layers[k - 1] + layers[k + 1])) + (y + sides(v, 1)))
                    out[x, odd, at(r)] = s * m

    chunks(NX, ne, smooth0)


def smooth_row(src, mask, v0, out, odd, row):
    def layers(parity, at_row, x):
        return pl.ds((2 * x + parity) * 56 + 8 + at_row, 8, stride=112)

    source, before, target = (ref.reshape((NX + 2) * 112, LANES) for ref in (src, v0, out))
    m = mask[8 + row : 9 + row]
    for x in range(1, NX + 1, 8):
        v = before[layers(odd, row, x), :]
        y = before[layers(1 - odd, row + odd - 1, x), :] + before[layers(1 - odd, row + odd, x), :]
        across = before[layers(odd, row, x - 1), :] + before[layers(odd, row, x + 1), :]
        s = third(v) + relax * ((source[layers(odd, row, x), :] + across) + (y + sides(v, 1)))
        target[layers(odd, row, x), :] = s * m


def images(src, first, odd, r, count):
    layers = [src[first + k, odd, at(r)] for k in range(count + 2)]
    result = []
    for k in range(1, count + 1):
        v = layers[k]
        y = src[first + k, 1 - odd, at(r, odd - 1)] + src[first + k, 1 - odd, at(r, odd)]
        result.append((v, 6.0 * v - ((layers[k - 1] + layers[k + 1]) + (y + sides(v, 1)))))
    return result


def cycles_kernel(*refs):
    pl.when(lax.axis_index("gx_1") == 0)(lambda: cycles_on_core(*refs))


def cycles_on_core(known, up, down, out, other, r0, z0, q0, w, v0, f1, v1, e1, e2, f2, t2, mask, mask2):
    gx0, _, gy, gz = place()

    def inside(count, height):
        rows, lanes = row_index((count, LANES)) - 8, lane_index((count, LANES))
        y = gy * BY - HY + height * rows
        z = (gz * 4 + z_block(gx0, gz)) * CZ - HZ + lanes
        return jnp.where((y >= 0) & (y < NY) & (z >= 0) & (z < NZ), 1.0, 0.0)

    mask[...] = inside(56, 2)
    mask2[...] = inside(40, 4)
    for ref, count in ((r0, NX), (z0, NX), (q0, NX), (w, NX), (v0, NX), (f1, NX // 2), (v1, NX // 2), (f2, NX // 4), (t2, NX // 4)):
        ref[0] = jnp.zeros(ref.shape[1:], jnp.float32)
        ref[count + 1] = jnp.zeros(ref.shape[1:], jnp.float32)
    lanes = lane_index((8, LANES))
    between = (lanes >= HZ) & (lanes < HZ + CZ)

    def corners_in(i, _):
        for odd in range(2):
            for b in range(5):
                if b == 2:
                    corners = (None,) * 4
                else:
                    part = pl.ds(BY * (b - b // 3) + 8 * odd, 8)
                    a, d = up[i, part], down[i, part]
                    one = jnp.where(lanes < 64, a, roll(d, 64, 1))
                    two = jnp.where(lanes < 64, roll(a, 64, 1), d)
                    corners = (one, roll(one, -32, 1), two, roll(two, -32, 1))
                for k, corner in enumerate(corners):
                    value = known[4 * i + k, odd, pl.ds(8 * b, 8)]
                    r0[4 * i + k + 1, odd, at(8 * b)] = value if corner is None else jnp.where(between, value, corner)
        return 0

    lax.fori_loop(0, 16, corners_in, 0, unroll=4)
    partner = {step: lanes ^ step for step in (1, 2)}
    outside = {step: (lanes + jnp.where(lanes & step == 0, -step, step)) & 127 for step in (1, 2)}

    def fold(x, step):
        return 0.5 * (x + jnp.take_along_axis(x, partner[step], axis=1))

    def outer(x, step):
        return jnp.take_along_axis(x, outside[step], axis=1)

    middle = (8, 16, 24)
    cycle_down(r0, mask, mask2, fold, outer, v1, e1, f1, f2, (0, 8, 16, 24, 32), (0, 8, 12), 8, 8)
    cycle_coarse(mask2, f2, t2, e2, (0, 8, 12), (1, 9))
    cycle_up(r0, mask, f1, e2, v1, e1, v0, z0, (6, 14, 22, 26), (7, 15, 23, 25), ((8, 16, 24, 25), (7, 15, 23, 24)), (middle, middle), 32, 64)

    def image(first):
        for odd in range(2):
            for r in middle:
                m = mask[at(r)]
                for k, (_, value) in enumerate(images(z0, first, odd, r, 64)):
                    q0[first + k + 1, odd, at(r)] = value * m

    chunks(NX, 64, image)
    cycle_down(q0, mask, mask2, fold, outer, v1, e1, f1, f2, middle, (5, 7), 8, 16)
    cycle_coarse(mask2, f2, t2, e2, (6,), (6,))
    cycle_up(q0, mask, f1, e2, v1, e1, v0, w, (14, 18), (15, 17), ((15, 17), (15, 17)), ((16,), (16,)), 32, 64)
    smooth_row(q0, mask, v0, w, 0, 24)
    smooth_row(q0, mask, v0, w, 1, 15)

    def sums(i, acc):
        acc = list(acc)
        for odd in range(2):
            for k, (ww, s) in enumerate(images(w, 64 * i, odd, 16, 64)):
                x = 64 * i + k + 1
                r, zz, q = r0[x, odd, at(16)], z0[x, odd, at(16)], q0[x, odd, at(16)]
                for n, term in enumerate((r * zz, zz * q, r * ww, q * ww, ww * s)):
                    acc[n] = acc[n] + term
                v0[x, odd, at(16)] = s
        return tuple(acc)

    acc = lax.fori_loop(0, NX // 64, sums, (jnp.zeros((8, LANES), jnp.float32),) * 5)

    for odd_slab, ref in enumerate((out, other)):
        for t in range(4):
            for k in range(BX):
                x = BX * (2 * t + odd_slab) + k + 1
                for odd in range(2):
                    zz, q, ww, s = (field[x, odd, at(16)] for field in (z0, q0, w, v0))
                    ref[t, pl.ds(k * BY + 8 * odd, 8)] = jnp.where(
                        lanes < 32, roll(zz, -32, 1), jnp.where(lanes < 64, q, jnp.where(lanes < 96, roll(ww, 32, 1), roll(s, 64, 1)))
                    )
    home = (lanes >= HZ) & (lanes < HZ + CZ)
    row = jnp.zeros((8, LANES), jnp.float32)
    for k, a in enumerate(acc):
        row = jnp.where(lanes == k, jnp.sum(jnp.where(home, a, 0.0)), row)
    for t in range(4):
        out[t, BX * BY : BX * BY + 8] = row
        other[t, BX * BY : BX * BY + 8] = row


def cycles(*blocks):
    fine = pltpu.VMEM((NX + 2, 2, 56, LANES), jnp.float32)
    level1 = pltpu.VMEM((NX // 2 + 2, 56, LANES), jnp.float32)
    level2 = pltpu.VMEM((NX // 4 + 2, 40, LANES), jnp.float32)
    return pl.pallas_call(
        cycles_kernel,
        out_shape=(jax.ShapeDtypeStruct((4, BX * BY + 8, LANES), jnp.float32),) * 2,
        in_specs=[VMEM] * 3,
        out_specs=(VMEM, VMEM),
        scratch_shapes=[fine] * 5
        + [level1] * 3
        + [pltpu.VMEM((NX // 4 + 2, 56, LANES), jnp.float32), level2, level2, pltpu.VMEM((56, LANES), jnp.float32), pltpu.VMEM((40, LANES), jnp.float32)],
        compiler_params=pltpu.CompilerParams(vmem_limit_bytes=30 * 1024 * 1024),
    )(*blocks)


def finish_kernel(rhs, fields, sums, solution, residual):
    total = jnp.sum(sums[...], axis=0, keepdims=True)
    lanes = lane_index(total.shape)

    def pick(k):
        return jnp.sum(jnp.where(lanes == k, total, 0.0), axis=1, keepdims=True)

    rz, zq, rw, qw, ws = (pick(k) for k in range(5))
    step0 = rz / zq
    rz1 = rz - step0 * (rw + zq) + step0 * step0 * qw
    growth = rz1 / rz
    image1 = (zq - 2.0 * step0 * qw + step0 * step0 * ws) + 2.0 * growth * (zq - step0 * qw) + growth * growth * zq
    step1 = rz1 / image1
    on_z = step0 + step1 * (1.0 + growth)
    on_w = -step1 * step0
    wide = lane_index((BY, LANES))
    even = wide // 32 % 2 == 0
    scale = jnp.where(wide < 64, on_z, on_w)
    gz = lax.axis_index("gz")

    def pair(a, b):
        return jnp.where(wide < 64, a, b) + roll(jnp.where(wide < 64, b, a), 64, 1)

    for x in range(BX):
        parts = [scale * fields[z_block(c, gz), x * BY : (x + 1) * BY] for c in range(4)]
        one, two = pair(parts[0], parts[2]), pair(parts[1], parts[3])
        u = jnp.where(even, one, roll(two, 32, 1))
        v = jnp.where(even, roll(one, -32, 1), two)
        for odd in range(2):
            rows = pl.ds(odd, 8, stride=2)
            solution[x, rows, :] = u[8 * odd : 8 * odd + 8]
            residual[x, rows, :] = rhs[x, rows, :] - v[8 * odd : 8 * odd + 8]


def finish(rhs, fields, sums):
    shape = jax.ShapeDtypeStruct((BX, BY, BZ), jnp.float32)
    return pl.pallas_call(finish_kernel, out_shape=(shape, shape), in_specs=[VMEM] * 3, out_specs=(VMEM, VMEM), compiler_params=small())(rhs, fields, sums)


def y_pairs(step):
    return [(a, 16 + a + step) for a in range(16) if 0 <= a + step < 16]


def z_pairs(step):
    def number(core, block):
        gz, at = block // 4, block % 4
        return ((at if gz % 2 == 0 else 3 - at) * 2 + core) * 8 + gz

    return [(number(1, a), number(0, a + step)) for a in range(32) if 0 <= a + step < 32]


Z_AXES = ("gx_0", "gx_1", "gz")


def local(density, x_faces, y_faces, z_faces):
    rhs, packed = make_rhs(density, x_faces, y_faces, z_faces)
    own = lax.all_to_all(packed, GX, 0, 0, tiled=True).reshape(16, BY, 128)
    moved = []
    for step in (2, -2, 1, -1):
        moved.append(lax.ppermute(own, ("gx_1", "gy"), y_pairs(step)))
    left = lax.ppermute(own, Z_AXES, z_pairs(1))
    right = lax.ppermute(own, Z_AXES, z_pairs(-1))
    rows = join(moved[0], moved[2], moved[3], moved[1])
    up = lax.ppermute(rows, Z_AXES, z_pairs(1))
    down = lax.ppermute(rows, Z_AXES, z_pairs(-1))
    rows = lax.ppermute(rows, "gx_1", [(1, 0)])
    known = unpack(own, left, right, rows)
    packed, other = cycles(known, up, down)
    other = lax.all_gather(other, "gx_1")
    packed = jnp.where(lax.axis_index("gx_1") == 1, other[0], packed)
    fields = lax.all_to_all(packed, "gx_0", 0, 0, tiled=True)
    sums = jnp.sum(fields[:, BX * BY, :], axis=0)
    sums = lax.all_to_all(jnp.broadcast_to(sums, (128, 1, 128)), ("gy", "gz"), 0, 0, tiled=True)
    return finish(rhs, fields, sums.reshape(128, 128))


def solution(mesh):
    torus = Mesh(mesh.devices.reshape(4, 2, mesh.shape["gy"], mesh.shape["gz"]), AXES)
    in_specs = (P(GX, "gy", "gz"), P(None, "gy", "gz"), P(None, GX, "gz"), P(None, GX, "gy"))
    out_specs = (P(GX, "gy", "gz"), P(GX, "gy", "gz"))
    return jax.shard_map(local, mesh=torus, in_specs=in_specs, out_specs=out_specs, check_vma=False)
```

```python
import jax
import jax.numpy as jnp
from jax import lax
from jax.experimental import pallas as pl
from jax.experimental.pallas import tpu as pltpu
from jax.sharding import Mesh
from jax.sharding import PartitionSpec as P


AXES = ("gx_0", "gx_1", "gy", "gz")
GX = ("gx_0", "gx_1")
NX, NY, NZ = 64, 256, 1024
BX, BY, BZ = 8, 16, 128
CZ = 32
HY, HZ = 32, 32
LANES = 128
relax = 1.0 / 9.0
coupling = 0.5
VMEM = pl.BlockSpec(memory_space=pltpu.VMEM)
HBM = pl.BlockSpec(memory_space=pltpu.MemorySpace.HBM)


def roll(x, shift, axis):
    return pltpu.roll(x, shift % x.shape[axis], axis)


def place():
    return tuple(lax.axis_index(axis) for axis in AXES)


def z_block(gx0, gz):
    return jnp.where(gz % 2 == 0, gx0, 3 - gx0)


def small(**more):
    return pltpu.CompilerParams(vmem_limit_bytes=4 * 1024 * 1024, **more)


def lane_index(shape):
    return lax.broadcasted_iota(jnp.int32, shape, 1)


def row_index(shape):
    return lax.broadcasted_iota(jnp.int32, shape, 0)


def rhs_kernel(density_in, xf_in, yf_in, zf_in, rhs, packed, scratch, density, xf, yf, zf, arrived):
    copies = [pltpu.make_async_copy(a, b, arrived.at[i]) for i, (a, b) in enumerate(((density_in, density), (xf_in, xf), (yf_in, yf), (zf_in, zf)))]
    for copy in copies:
        copy.start()
    gx0, core, gy, gz = place()
    gx = 2 * gx0 + core
    rows, lanes = row_index((BY, BZ)), lane_index((BY, BZ))
    eye = row_index((BY, BY)) == lane_index((BY, BY))
    low_y = (rows == 0) & (gy == 0)
    high_y = (rows == BY - 1) & (gy == NY // BY - 1)
    low_z = (lanes == 0) & (gz == 0)
    high_z = (lanes == BZ - 1) & (gz == NZ // BZ - 1)

    def column(row):
        return jnp.sum(jnp.where(eye, row, 0.0), axis=1, keepdims=True)

    for copy in copies:
        copy.wait()
    for x in range(BX):
        value = -coupling * density[x]
        if x == 0:
            value = value + jnp.where(gx == 0, xf[0], 0.0)
        if x == BX - 1:
            value = value + jnp.where(gx == NX // BX - 1, xf[1], 0.0)
        value = value + jnp.where(low_y, yf[0, x : x + 1, :], 0.0)
        rhs[x] = value + jnp.where(high_y, yf[1, x : x + 1, :], 0.0)

    @pl.when((gz == 0) | (gz == NZ // BZ - 1))
    def _():
        for x in range(BX):
            value = rhs[x] + jnp.where(low_z, column(zf[0, x : x + 1, :]), 0.0)
            rhs[x] = value + jnp.where(high_z, column(zf[1, x : x + 1, :]), 0.0)

    layers = [rhs[x] for x in range(BX)]
    for chunk in range(4):
        for quad in range(2):
            out = None
            for k in range(4):
                part = roll(layers[4 * quad + k], 32 * (k - chunk), 1)
                out = part if k == 0 else jnp.where(lanes >= 32 * k, part, out)
            scratch[chunk, quad] = out
    for chip in range(4):
        chunk = z_block(chip, gz)
        for quad in range(2):
            for odd in range(2):
                part = scratch[chunk, quad, pl.ds(odd, 8, stride=2), :]
                packed[2 * chip, quad, 8 * odd : 8 * odd + 8] = part
                packed[2 * chip + 1, quad, 8 * odd : 8 * odd + 8] = part


def make_rhs(density, xf, yf, zf):
    return pl.pallas_call(
        rhs_kernel,
        out_shape=(
            jax.ShapeDtypeStruct((BX, BY, BZ), jnp.float32),
            jax.ShapeDtypeStruct((8, 2, BY, BZ), jnp.float32),
        ),
        in_specs=[HBM] * 4,
        out_specs=(VMEM, VMEM),
        scratch_shapes=[pltpu.VMEM((4, 2, BY, BZ), jnp.float32)]
        + [pltpu.VMEM(a.shape, a.dtype) for a in (density, xf, yf, zf)]
        + [pltpu.SemaphoreType.DMA((4,))],
        compiler_params=pltpu.CompilerParams(vmem_limit_bytes=60 * 1024 * 1024),
    )(density, xf, yf, zf)


def join_kernel(*refs):
    out = refs[-1]
    for b, ref in enumerate(refs[:-1]):
        for i in range(16):
            out[i, BY * b : BY * b + BY] = ref[i]


def join(*blocks):
    return pl.pallas_call(
        join_kernel,
        out_shape=jax.ShapeDtypeStruct((16, 4 * BY, 128), jnp.float32),
        in_specs=[VMEM] * 4,
        out_specs=VMEM,
        compiler_params=small(),
    )(*blocks)


def unpack_kernel(*refs):
    pl.when(lax.axis_index("gx_1") == 0)(lambda: unpack_on_core(*refs))


def unpack_on_core(own, left, right, rows_, out):
    lanes = lane_index((8, LANES))
    even = lanes // 32 % 2 == 0
    for i in range(16):
        for odd in range(2):
            for b in range(4):
                c = rows_[i, pl.ds(BY * b + 8 * odd, 8)]
                for k in range(4):
                    out[4 * i + k, odd, pl.ds(8 * (b + b // 2), 8)] = roll(c, 32 - 32 * k, 1)
            part = pl.ds(8 * odd, 8)
            a, c, d = left[i, part], own[i, part], right[i, part]
            low = jnp.where(lanes < 64, a, roll(d, 64, 1))
            high = jnp.where(lanes < 64, roll(a, 64, 1), d)
            out[4 * i, odd, 16:24] = jnp.where(even, low, roll(c, 32, 1))
            out[4 * i + 1, odd, 16:24] = jnp.where(even, roll(low, -32, 1), c)
            out[4 * i + 2, odd, 16:24] = jnp.where(even, high, roll(c, -32, 1))
            out[4 * i + 3, odd, 16:24] = jnp.where(even, roll(high, -32, 1), roll(c, 64, 1))


def unpack(own, left, right, rows):
    return pl.pallas_call(
        unpack_kernel,
        out_shape=jax.ShapeDtypeStruct((NX, 2, 40, LANES), jnp.float32),
        in_specs=[VMEM] * 4,
        out_specs=VMEM,
        compiler_params=small(),
    )(own, left, right, rows)


def at(row, step=0):
    return pl.ds(8 + row + step, 8)


def every_other(row, step=0):
    return pl.ds(8 + 2 * row + step, 8, stride=2)


def sides(x, step):
    return roll(x, step, 1) + roll(x, -step, 1)


def third(x):
    return x * (1.0 / 3.0)


def chunks(count, size, body):
    size, unroll = size if isinstance(size, tuple) else (size, 1)
    if size == count:
        body(0)
    elif size * unroll == count:
        for i in range(unroll):
            body(i * size)
    else:
        lax.fori_loop(0, count // size, lambda i, _: body(i * size) or 0, 0, unroll=unroll)


def cycle_down(src, mask, mask2, fold, outer, sum1, part1, f1, f2, rows1, rows2, size, nb):
    def gather(first, size=size):
        for r in rows1:
            layers = [2 * first + k for k in range(2 * size + 2)]
            cells = [src[x, 0, at(r)] + src[x, 1, at(r)] for x in layers]
            beyond = [src[x, 1, at(r, -1)] + src[x, 0, at(r, 1)] for x in layers[1:-1]]
            for i in range(size):
                before, a, b, after = cells[2 * i : 2 * i + 4]
                u = a + b
                y = beyond[2 * i] + beyond[2 * i + 1]
                sum1[first + i + 1, at(r)] = u
                part1[first + i + 1, at(r)] = third(u) + relax * (((u + u) + (before + after)) + y)

    chunks(NX // 2, size, gather)

    def across(first):
        for r in rows1:
            for x in [first + k for k in range(1, 32 + 1)]:
                f1[x, at(r)] = part1[x, at(r)] + relax * (sum1[x, at(r)] + outer(sum1[x, at(r)], 1))

    chunks(NX // 2, 32, across)

    def level1(first):
        for r in rows1:
            m = mask[at(r)]
            for x in [first + k for k in range(1, 32 + 1)]:
                f1[x, at(r)] = fold(f1[x, at(r)], 1) * m

    chunks(NX // 2, 32, level1)

    def level2(first):
        for r in rows2:
            m = mask2[at(r)]
            layers = [2 * first + k for k in range(2 * nb + 2)]
            cells = [f1[x, every_other(r), :] + f1[x, every_other(r, 1), :] for x in layers]
            beyond = [f1[x, every_other(r, -1), :] + f1[x, every_other(r, 2), :] for x in layers[1:-1]]
            for i in range(nb):
                before, a, b, after = cells[2 * i : 2 * i + 4]
                u = a + b
                y = beyond[2 * i] + beyond[2 * i + 1]
                s = third(u) + relax * (((u + u) + (before + after)) + (y + (u + outer(u, 2))))
                f2[first + i + 1, at(r)] = fold(s, 2) * m

    chunks(NX // 4, nb, level2)


def cycle_coarse(mask2, f2, t2, e2, rows, last):
    def around(ref, x, r):
        return (ref[x - 1, at(r)] + ref[x + 1, at(r)]) + (ref[x, at(r, -1)] + ref[x, at(r, 1)])

    def sweep1(first):
        for r in rows:
            m = mask2[at(r)]
            for x in range(1, 17):
                v = f2[first + x, at(r)]
                s = (4.0 / 3.0) * v + relax * (around(f2, first + x, r) + sides(v, 4))
                t2[first + x, at(r)] = (relax * s) * m

    chunks(NX // 4, 16, sweep1)

    def sweep2(first):
        for r in last:
            m = mask2[at(r)]
            for x in range(1, 17):
                v = t2[first + x, at(r)]
                s = (third(v) + relax * (f2[first + x, at(r)] + (around(t2, first + x, r) + sides(v, 4)))) * m
                e2[first + x, every_other(r), :] = s
                e2[first + x, every_other(r, 1), :] = s

    chunks(NX // 4, 16, sweep2)


def cycle_up(src, mask, f1, e2, v1, e1, v0, out, rows1, last1, rows0, last0, nd, ne):
    def correct1(first):
        for r in rows1:
            for i in range(4):
                e = e2[first + i + 1, at(r)]
                for k in (1, 2):
                    x = 2 * first + 2 * i + k
                    v1[x, at(r)] = relax * f1[x, at(r)] + e

    chunks(NX // 4, 4, correct1)

    def smooth1(first):
        for r in last1:
            m = mask[at(r)]
            for x in [first + k for k in range(1, nd + 1)]:
                v = v1[x, at(r)]
                y = v1[x, at(r, -1)] + v1[x, at(r, 1)]
                s = third(v) + relax * ((f1[x, at(r)] + (v1[x - 1, at(r)] + v1[x + 1, at(r)])) + (y + sides(v, 2)))
                e1[x, at(r)] = s * m

    chunks(NX // 2, nd, smooth1)
    right, before, target = (ref.reshape((NX // 2 + 2) * 56, LANES) for ref in (f1, v1, e1))
    for row in (last1[-1] + 8, last1[-1] + 9):
        for x in range(1, NX // 2 + 1, 8):
            here, under, over, prior, later = (pl.ds((x + i) * 56 + 8 + row + j, 8, stride=56) for i, j in ((0, 0), (0, -1), (0, 1), (-1, 0), (1, 0)))
            v = before[here, :]
            y = before[under, :] + before[over, :]
            s = third(v) + relax * ((right[here, :] + (before[prior, :] + before[later, :])) + (y + sides(v, 2)))
            target[here, :] = s * mask[8 + row : 9 + row]

    def correct0(first):
        for odd in range(2):
            for r in rows0[odd]:
                for i in range(1, 33):
                    e = e1[first + i, at(r)]
                    for k in (-1, 0):
                        x = 2 * first + 2 * i + k
                        v0[x, odd, at(r)] = relax * src[x, odd, at(r)] + e

    chunks(NX // 2, 32, correct0)

    def smooth0(first):
        for odd in range(2):
            for r in last0[odd]:
                m = mask[at(r)]
                layers = [v0[first + k, odd, at(r)] for k in range(ne + 2)]
                for k in range(1, ne + 1):
                    x = first + k
                    v = layers[k]
                    y = v0[x, 1 - odd, at(r, odd - 1)] + v0[x, 1 - odd, at(r, odd)]
                    s = third(v) + relax * ((src[x, odd, at(r)] + (layers[k - 1] + layers[k + 1])) + (y + sides(v, 1)))
                    out[x, odd, at(r)] = s * m

    chunks(NX, ne, smooth0)


def smooth_row(src, mask, v0, out, odd, row):
    def layers(parity, at_row, x):
        return pl.ds((2 * x + parity) * 56 + 8 + at_row, 8, stride=112)

    source, before, target = (ref.reshape((NX + 2) * 112, LANES) for ref in (src, v0, out))
    m = mask[8 + row : 9 + row]
    for x in range(1, NX + 1, 8):
        v = before[layers(odd, row, x), :]
        y = before[layers(1 - odd, row + odd - 1, x), :] + before[layers(1 - odd, row + odd, x), :]
        across = before[layers(odd, row, x - 1), :] + before[layers(odd, row, x + 1), :]
        s = third(v) + relax * ((source[layers(odd, row, x), :] + across) + (y + sides(v, 1)))
        target[layers(odd, row, x), :] = s * m


def images(src, first, odd, r, count):
    layers = [src[first + k, odd, at(r)] for k in range(count + 2)]
    result = []
    for k in range(1, count + 1):
        v = layers[k]
        y = src[first + k, 1 - odd, at(r, odd - 1)] + src[first + k, 1 - odd, at(r, odd)]
        result.append((v, 6.0 * v - ((layers[k - 1] + layers[k + 1]) + (y + sides(v, 1)))))
    return result


def cycles_kernel(*refs):
    pl.when(lax.axis_index("gx_1") == 0)(lambda: cycles_on_core(*refs))


def cycles_on_core(known, up, down, out, other, r0, z0, q0, w, v0, f1, v1, e1, e2, f2, t2, mask, mask2):
    gx0, _, gy, gz = place()

    def inside(count, height):
        rows, lanes = row_index((count, LANES)) - 8, lane_index((count, LANES))
        y = gy * BY - HY + height * rows
        z = (gz * 4 + z_block(gx0, gz)) * CZ - HZ + lanes
        return jnp.where((y >= 0) & (y < NY) & (z >= 0) & (z < NZ), 1.0, 0.0)

    mask[...] = inside(56, 2)
    mask2[...] = inside(40, 4)
    for ref, count in ((r0, NX), (z0, NX), (q0, NX), (w, NX), (v0, NX), (f1, NX // 2), (v1, NX // 2), (f2, NX // 4), (t2, NX // 4)):
        ref[0] = jnp.zeros(ref.shape[1:], jnp.float32)
        ref[count + 1] = jnp.zeros(ref.shape[1:], jnp.float32)
    lanes = lane_index((8, LANES))
    between = (lanes >= HZ) & (lanes < HZ + CZ)

    def corners_in(i, _):
        for odd in range(2):
            for b in range(5):
                if b == 2:
                    corners = (None,) * 4
                else:
                    part = pl.ds(BY * (b - b // 3) + 8 * odd, 8)
                    a, d = up[i, part], down[i, part]
                    one = jnp.where(lanes < 64, a, roll(d, 64, 1))
                    two = jnp.where(lanes < 64, roll(a, 64, 1), d)
                    corners = (one, roll(one, -32, 1), two, roll(two, -32, 1))
                for k, corner in enumerate(corners):
                    value = known[4 * i + k, odd, pl.ds(8 * b, 8)]
                    r0[4 * i + k + 1, odd, at(8 * b)] = value if corner is None else jnp.where(between, value, corner)
        return 0

    lax.fori_loop(0, 16, corners_in, 0, unroll=4)
    partner = {step: lanes ^ step for step in (1, 2)}
    outside = {step: (lanes + jnp.where(lanes & step == 0, -step, step)) & 127 for step in (1, 2)}

    def fold(x, step):
        return 0.5 * (x + jnp.take_along_axis(x, partner[step], axis=1))

    def outer(x, step):
        return jnp.take_along_axis(x, outside[step], axis=1)

    middle = (8, 16, 24)
    cycle_down(r0, mask, mask2, fold, outer, v1, e1, f1, f2, (0, 8, 16, 24, 32), (0, 8, 12), 8, 8)
    cycle_coarse(mask2, f2, t2, e2, (0, 8, 12), (1, 9))
    cycle_up(r0, mask, f1, e2, v1, e1, v0, z0, (6, 14, 22, 26), (7, 15, 23), ((8, 16, 24, 25), (7, 15, 23, 24)), (middle, middle), 32, 64)

    def image(first):
        for odd in range(2):
            for r in middle:
                m = mask[at(r)]
                for k, (_, value) in enumerate(images(z0, first, odd, r, 64)):
                    q0[first + k + 1, odd, at(r)] = value * m

    chunks(NX, 64, image)
    cycle_down(q0, mask, mask2, fold, outer, v1, e1, f1, f2, middle, (5, 7), 8, 16)
    cycle_coarse(mask2, f2, t2, e2, (6,), (6,))
    cycle_up(q0, mask, f1, e2, v1, e1, v0, w, (14, 18), (15,), ((15, 17), (15, 17)), ((16,), (16,)), 32, 64)
    smooth_row(q0, mask, v0, w, 0, 24)
    smooth_row(q0, mask, v0, w, 1, 15)

    def sums(i, acc):
        acc = list(acc)
        for odd in range(2):
            for k, (ww, s) in enumerate(images(w, 64 * i, odd, 16, 64)):
                x = 64 * i + k + 1
                r, zz, q = r0[x, odd, at(16)], z0[x, odd, at(16)], q0[x, odd, at(16)]
                for n, term in enumerate((r * zz, zz * q, r * ww, q * ww, ww * s)):
                    acc[n] = acc[n] + term
                v0[x, odd, at(16)] = s
        return tuple(acc)

    acc = lax.fori_loop(0, NX // 64, sums, (jnp.zeros((8, LANES), jnp.float32),) * 5)

    for odd_slab, ref in enumerate((out, other)):
        for t in range(4):
            for k in range(BX):
                x = BX * (2 * t + odd_slab) + k + 1
                for odd in range(2):
                    zz, q, ww, s = (field[x, odd, at(16)] for field in (z0, q0, w, v0))
                    ref[t, pl.ds(k * BY + 8 * odd, 8)] = jnp.where(
                        lanes < 32, roll(zz, -32, 1), jnp.where(lanes < 64, q, jnp.where(lanes < 96, roll(ww, 32, 1), roll(s, 64, 1)))
                    )
    home = (lanes >= HZ) & (lanes < HZ + CZ)
    row = jnp.zeros((8, LANES), jnp.float32)
    for k, a in enumerate(acc):
        row = jnp.where(lanes == k, jnp.sum(jnp.where(home, a, 0.0)), row)
    for t in range(4):
        out[t, BX * BY : BX * BY + 8] = row
        other[t, BX * BY : BX * BY + 8] = row


def cycles(*blocks):
    fine = pltpu.VMEM((NX + 2, 2, 56, LANES), jnp.float32)
    level1 = pltpu.VMEM((NX // 2 + 2, 56, LANES), jnp.float32)
    level2 = pltpu.VMEM((NX // 4 + 2, 40, LANES), jnp.float32)
    return pl.pallas_call(
        cycles_kernel,
        out_shape=(jax.ShapeDtypeStruct((4, BX * BY + 8, LANES), jnp.float32),) * 2,
        in_specs=[VMEM] * 3,
        out_specs=(VMEM, VMEM),
        scratch_shapes=[fine] * 5
        + [level1] * 3
        + [pltpu.VMEM((NX // 4 + 2, 56, LANES), jnp.float32), level2, level2, pltpu.VMEM((56, LANES), jnp.float32), pltpu.VMEM((40, LANES), jnp.float32)],
        compiler_params=pltpu.CompilerParams(vmem_limit_bytes=30 * 1024 * 1024),
    )(*blocks)


def finish_kernel(rhs, fields, sums, solution, residual):
    total = jnp.sum(sums[...], axis=0, keepdims=True)
    lanes = lane_index(total.shape)

    def pick(k):
        return jnp.sum(jnp.where(lanes == k, total, 0.0), axis=1, keepdims=True)

    rz, zq, rw, qw, ws = (pick(k) for k in range(5))
    step0 = rz / zq
    rz1 = rz - step0 * (rw + zq) + step0 * step0 * qw
    growth = rz1 / rz
    image1 = (zq - 2.0 * step0 * qw + step0 * step0 * ws) + 2.0 * growth * (zq - step0 * qw) + growth * growth * zq
    step1 = rz1 / image1
    on_z = step0 + step1 * (1.0 + growth)
    on_w = -step1 * step0
    wide = lane_index((BY, LANES))
    even = wide // 32 % 2 == 0
    scale = jnp.where(wide < 64, on_z, on_w)
    gz = lax.axis_index("gz")

    def pair(a, b):
        return jnp.where(wide < 64, a, b) + roll(jnp.where(wide < 64, b, a), 64, 1)

    for x in range(BX):
        parts = [scale * fields[z_block(c, gz), x * BY : (x + 1) * BY] for c in range(4)]
        one, two = pair(parts[0], parts[2]), pair(parts[1], parts[3])
        u = jnp.where(even, one, roll(two, 32, 1))
        v = jnp.where(even, roll(one, -32, 1), two)
        for odd in range(2):
            rows = pl.ds(odd, 8, stride=2)
            solution[x, rows, :] = u[8 * odd : 8 * odd + 8]
            residual[x, rows, :] = rhs[x, rows, :] - v[8 * odd : 8 * odd + 8]


def finish(rhs, fields, sums):
    shape = jax.ShapeDtypeStruct((BX, BY, BZ), jnp.float32)
    return pl.pallas_call(finish_kernel, out_shape=(shape, shape), in_specs=[VMEM] * 3, out_specs=(VMEM, VMEM), compiler_params=small())(rhs, fields, sums)


def y_pairs(step):
    return [(a, 16 + a + step) for a in range(16) if 0 <= a + step < 16]


def z_pairs(step):
    def number(core, block):
        gz, at = block // 4, block % 4
        return ((at if gz % 2 == 0 else 3 - at) * 2 + core) * 8 + gz

    return [(number(1, a), number(0, a + step)) for a in range(32) if 0 <= a + step < 32]


Z_AXES = ("gx_0", "gx_1", "gz")


def local(density, x_faces, y_faces, z_faces):
    rhs, packed = make_rhs(density, x_faces, y_faces, z_faces)
    own = lax.all_to_all(packed, GX, 0, 0, tiled=True).reshape(16, BY, 128)
    moved = []
    for step in (2, -2, 1, -1):
        moved.append(lax.ppermute(own, ("gx_1", "gy"), y_pairs(step)))
    left = lax.ppermute(own, Z_AXES, z_pairs(1))
    right = lax.ppermute(own, Z_AXES, z_pairs(-1))
    rows = join(moved[0], moved[2], moved[3], moved[1])
    up = lax.ppermute(rows, Z_AXES, z_pairs(1))
    down = lax.ppermute(rows, Z_AXES, z_pairs(-1))
    rows = lax.ppermute(rows, "gx_1", [(1, 0)])
    known = unpack(own, left, right, rows)
    packed, other = cycles(known, up, down)
    other = lax.all_gather(other, "gx_1")
    packed = jnp.where(lax.axis_index("gx_1") == 1, other[0], packed)
    fields = lax.all_to_all(packed, "gx_0", 0, 0, tiled=True)
    sums = jnp.sum(fields[:, BX * BY, :], axis=0)
    sums = lax.all_to_all(jnp.broadcast_to(sums, (128, 1, 128)), ("gy", "gz"), 0, 0, tiled=True)
    return finish(rhs, fields, sums.reshape(128, 128))


def solution(mesh):
    torus = Mesh(mesh.devices.reshape(4, 2, mesh.shape["gy"], mesh.shape["gz"]), AXES)
    in_specs = (P(GX, "gy", "gz"), P(None, "gy", "gz"), P(None, GX, "gz"), P(None, GX, "gy"))
    out_specs = (P(GX, "gy", "gz"), P(GX, "gy", "gz"))
    return jax.shard_map(local, mesh=torus, in_specs=in_specs, out_specs=out_specs, check_vma=False)
```
